256 devices in a mesh: rep: 2 (over y), seq: 128 (over z, x, core).
Axes of the slice: x: 4, y: 2, z: 16, core: 2. Of those that a mesh axis runs over, the one named last changes fastest.
The devices are a block of a 4x16x16 slice.
Arguments:
- latents: bfloat16 [16, 196608], P(None, ('rep', 'seq')), parts along dimension 1, may hold values from -6 to 6
- layout: int32 [256, 768], P('rep'), parts along dimension 0, may hold values from 0 to 98303, as said below
- assign: int32 [16], P('rep'), parts along dimension 0, may hold values from 0 to 7, as said below
- counts: int32 [16], P('rep'), parts along dimension 0, may hold values from 1 to 3
- latent_cache: bfloat16 [2, 1024, 1024], P(None, ('rep', 'seq')), parts along dimension 1, may hold values from -6 to 6
- feature_cache: bfloat16 [2, 1024, 64, 384], P(None, ('rep', 'seq')), parts along dimension 1, may hold values from -4 to 4
- first_weight: bfloat16 [3, 3, 3, 16, 384], replicated, may hold values from -0.3125 to 0.3125
- first_bias: float32 [384], replicated, may hold values from -3 to 3
- norm_gain: float32 [384], replicated, may hold values from 0.25 to 1.75
- second_weight: bfloat16 [3, 3, 3, 384, 192], replicated, may hold values from -0.0625 to 0.0625
- second_bias: float32 [192], replicated, may hold values from -3 to 3
Outputs:
- decoded_frames: bfloat16 [3, 2048, 128, 192], P(None, ('rep', 'seq')), parts along dimension 1
- latent_cache_next: bfloat16 [2, 1024, 1024], P(None, ('rep', 'seq')), parts along dimension 1
- feature_cache_next: bfloat16 [2, 1024, 64, 384], P(None, ('rep', 'seq')), parts along dimension 1
The draws below stay inside these ranges and needn't reach their ends.
There are 2 independent parts, one for each index of `rep`. The reference program is written for one: setup_inputs(seed, part) draws one part's arguments, and reference() takes and returns one part's arrays. A program takes and returns all parts, laid end to end along the dimension named above; an argument that names none is the same for every part. Nothing has to cross between parts.
Inputs may be any that keep to these rules, and one draw needn't show every extreme that they name: assign is a permutation of 0 to 7. layout is a permutation of 0 to 98303. Call the cells of request assign[g], rows k * 4 to (k + 1) * 4 - 1, all frames and columns, the tile of seq index (g * 16 + k - 8) mod 128; every row of layout holds exactly 6 cells of every tile.
All inputs are finite; a program needn't handle non-finite values.
Results may differ from the reference program's by a relative error of at most 0.0034.
Values may be sent and summed in bfloat16 or wider, within the bound.
A program may use at most 128 MiB of HBM per device.

```python
import jax
import jax.numpy as jnp
from jax import lax

LAT_CH = 16
MID_CH = 384
OUT_CH = 192
REQS = 8
FMAX = 3
ROWS_DEV = 4
W = 64
GROUP = 16
SHIFT = 8
HEIGHT = 64
CELLS = 768
PEER = 6
TOTAL_CELLS = 98304
ROWS_ALL = 512
N_SEQ = 128


def pairing(key):
    return jax.random.permutation(jax.random.fold_in(key, 11), REQS).astype(jnp.int32)


def one_permutation(subkey):
    return jax.random.permutation(subkey, CELLS).astype(jnp.int32)


def draw_assign(key, part):
    return pairing(key)


def draw_layout(key, part):
    assign = pairing(key)
    spread_keys = jax.random.split(jax.random.fold_in(key, 23), N_SEQ)
    within = jax.vmap(one_permutation)(spread_keys)
    numbers = jnp.arange(N_SEQ, dtype=jnp.int32)[:, None] * CELLS + within
    numbers = jnp.transpose(numbers.reshape(N_SEQ, N_SEQ, PEER), (1, 0, 2)).reshape(N_SEQ, CELLS)
    slot_keys = jax.random.split(jax.random.fold_in(key, 37), N_SEQ)
    mixing = jax.vmap(one_permutation)(slot_keys)
    numbers = jnp.take_along_axis(numbers, mixing, axis=1)
    target = numbers // CELLS
    inside = numbers % CELLS
    frame_index = inside // (ROWS_DEV * W)
    tile_row = inside // W % ROWS_DEV
    column = inside % W
    place = (target + SHIFT) % N_SEQ
    group_index = place // GROUP
    position = place % GROUP
    request = jnp.take(assign, group_index)
    image_row = position * ROWS_DEV + tile_row
    return (((request * FMAX + frame_index) * HEIGHT + image_row) * W + column).astype(jnp.int32)


def plant(entries, key, smallest, top_value):
    spot = [jax.random.randint(jax.random.fold_in(key, axis), (), 0, length) for axis, length in enumerate(entries.shape)]
    longest = entries.shape.index(max(entries.shape))
    neighbour = spot[:longest] + [(spot[longest] + 1) % entries.shape[longest]] + spot[longest + 1:]
    return entries.at[tuple(spot)].set(smallest).at[tuple(neighbour)].set(top_value)


def levels(rng, extent, cuts, low, largest):
    factor_of = 1.0
    for axis_at, blocks in cuts:
        draws = jax.random.uniform(jax.random.fold_in(jax.random.fold_in(rng, 6), axis_at), (blocks,), jnp.float32, low / len(cuts), largest / len(cuts))
        factor_of = factor_of * jnp.repeat(jnp.exp(draws), extent[axis_at] // blocks).reshape((-1,) + (1,) * (len(extent) - 1 - axis_at))
    return factor_of


def scatter_about(key, shape, deviation, bound, pieces=(), kind=jnp.bfloat16):
    values = jax.random.normal(key, shape, jnp.float32) * deviation
    if len(pieces) > 0:
        values = levels(key, shape, pieces, -0.22, 0.18) * values
    return jnp.clip(values, min=-bound, max=bound).astype(kind)


def setup_inputs(seed: int = 0, part: int = 0) -> dict:
    key_of = jax.random.split(jax.random.key(seed), 12)
    part_keys = jax.random.split(jax.random.fold_in(key_of[11], part), 12)
    return {
        "latents": scatter_about(part_keys[0], (LAT_CH, TOTAL_CELLS), 1.0, 6.0, ((1, 128),)),
        "layout": draw_layout(jax.random.fold_in(jax.random.fold_in(key_of[11], part), 71), part),
        "assign": draw_assign(jax.random.fold_in(jax.random.fold_in(key_of[11], part), 71), part),
        "counts": plant(jax.random.randint(part_keys[3], (REQS,), 1, FMAX + 1), jax.random.fold_in(part_keys[3], 1), 1, FMAX).astype(jnp.int32),
        "latent_cache": scatter_about(part_keys[4], (2, ROWS_ALL, W * LAT_CH), 1.0, 6.0, ((1, 128),)),
        "feature_cache": scatter_about(part_keys[5], (2, ROWS_ALL, W, MID_CH), 0.6, 4.0, ((1, 128),)),
        "first_weight": scatter_about(key_of[6], (3, 3, 3, LAT_CH, MID_CH), (27 * LAT_CH) ** -0.5, 0.3125),
        "first_bias": scatter_about(key_of[7], (MID_CH,), 0.5, 3.0, (), jnp.float32),
        "norm_gain": jnp.clip(1.0 + 0.15 * jax.random.normal(key_of[8], (MID_CH,), jnp.float32), 0.25, 1.75),
        "second_weight": scatter_about(key_of[9], (3, 3, 3, MID_CH, OUT_CH), (27 * MID_CH) ** -0.5, 0.0625),
        "second_bias": scatter_about(key_of[10], (OUT_CH,), 0.5, 3.0, (), jnp.float32),
    }


def causal_conv(values, weight, offset):
    result = lax.conv_general_dilated(values[None], weight, (1, 1, 1), ((0, 0), (1, 1), (1, 1)), dimension_numbers=('NDHWC', 'DHWIO', 'NDHWC'), preferred_element_type=jnp.float32)
    return result[0] + offset

def activate(linear, norm_gain):
    inverse = lax.rsqrt(lax.optimization_barrier(jnp.mean(linear * linear, axis=-1, keepdims=True)) + 1e-06)
    return jax.nn.silu(linear * inverse * norm_gain).astype(jnp.bfloat16)

def reference(latents, layout, assign, counts, latent_cache, feature_cache, first_weight, first_bias, norm_gain, second_weight, second_bias):
    positions = jnp.argsort(layout.reshape(-1)).astype(jnp.int32)
    ordered = jnp.take(latents, positions, axis=1).reshape(LAT_CH, REQS, FMAX, HEIGHT, W)
    ordered = jnp.transpose(ordered, (1, 2, 3, 4, 0))
    latent_prev = jnp.roll(latent_cache, SHIFT * ROWS_DEV, axis=1).reshape(2, REQS, HEIGHT, W, LAT_CH)
    feature_prev = jnp.roll(feature_cache, SHIFT * ROWS_DEV, axis=1).reshape(2, REQS, HEIGHT, W, MID_CH)
    frame_index = jnp.arange(FMAX, dtype=jnp.int32)[:, None, None, None]
    decoded_list = []
    latent_list = []
    feature_list = []
    for group_index in range(REQS):
        request = assign[group_index].astype(jnp.int32)
        live_frames = counts[request].astype(jnp.int32)
        window = lax.dynamic_index_in_dim(ordered, request, 0, keepdims=False)
        first_input = jnp.concatenate([latent_prev[:, group_index], window], axis=0)
        features = activate(causal_conv(first_input, first_weight, first_bias), norm_gain)
        second_input = jnp.concatenate([feature_prev[:, group_index], features], axis=0)
        doubled = jnp.repeat(jnp.repeat(second_input, 2, axis=1), 2, axis=2)
        decoded = causal_conv(doubled, second_weight, second_bias)
        decoded = jnp.where(frame_index < live_frames, decoded, 0.0).astype(jnp.bfloat16)
        decoded_list.append(decoded)
        latent_list.append(lax.dynamic_slice_in_dim(first_input, live_frames, 2, 0))
        feature_list.append(lax.dynamic_slice_in_dim(second_input, live_frames, 2, 0))
    decoded_frames = jnp.roll(jnp.concatenate(decoded_list, axis=1), -2 * SHIFT * ROWS_DEV, axis=1)
    latent_cache_next = jnp.roll(jnp.concatenate(latent_list, axis=1), -SHIFT * ROWS_DEV, axis=1).reshape(2, ROWS_ALL, W * LAT_CH)
    feature_cache_next = jnp.roll(jnp.concatenate(feature_list, axis=1), -SHIFT * ROWS_DEV, axis=1)
    return (decoded_frames, latent_cache_next, feature_cache_next)
```

```python
import jax
import jax.numpy as jnp
from jax import lax
from jax.experimental import pallas as pl
from jax.experimental.pallas import tpu as pltpu
from jax.sharding import PartitionSpec as P

LAT_CH = 16
REQS = 8
FMAX = 3
ROWS_DEV = 4
W = 64
MID_CH = 384
OUT_CH = 192


def padded_2(array, sides, width):
    for axis, dim in sides:
        devices, length = (lax.axis_size(axis), array.shape[dim])
        up = [(i, (i + 1) % devices) for i in range(devices)]
        down = [(j, i) for i, j in up]
        last = lax.slice_in_dim(array, length - width, length, axis=dim)
        first = lax.slice_in_dim(array, 0, width, axis=dim)
        before = lax.ppermute(last, axis, up)
        after = lax.ppermute(first, axis, down)
        array = jnp.concatenate([before, array, after], axis=dim)
    return array


def tile_numbers(layout, assign, per_group, devices):
    height = ROWS_DEV * per_group
    offset = per_group // 2
    tile_cells = FMAX * ROWS_DEV * W
    column = layout % W
    remain = layout // W
    image_row = remain % height
    remain = remain // height
    frame_index = remain % FMAX
    request = remain // FMAX
    group_ranks = jnp.arange(REQS, dtype=jnp.int32)
    group_index = jnp.sum(jnp.where(assign == request[..., None], group_ranks, 0), axis=-1)
    place = group_index * per_group + image_row // ROWS_DEV
    target = (place - offset + devices) % devices
    within = (frame_index * ROWS_DEV + image_row % ROWS_DEV) * W + column
    return target * tile_cells + within


def keep_rows(values, rim_width, position, height):
    row_index = position * ROWS_DEV - rim_width + jnp.arange(values.shape[1], dtype=jnp.int32)
    inside = (row_index >= 0) & (row_index < height)
    return jnp.where(inside[None, :, None, None], values, jnp.zeros((), values.dtype))


def decode_kernel(
    live_ref, place_ref, xt_ref, w1_ref, b1_ref, gain_ref, fc_ref, top_ref, bot_ref, w2_hbm, b2_ref,
    out_ref, fn_ref, w2_ref, wc_ref, xs_ref, h_ref, ob_ref, sem,
):
    live = live_ref[0]
    place = place_ref[0]
    last = place_ref[1]
    load = pltpu.make_async_copy(w2_hbm, w2_ref, sem)
    load.start()
    f32, bf16 = jnp.float32, jnp.bfloat16
    rows, mid = ROWS_DEV + 2, MID_CH
    xt = xt_ref[...].astype(f32)
    lanes = xt.shape[1]
    column = lax.broadcasted_iota(jnp.int32, xt.shape, 1) % W
    shifted = (
        jnp.where(column == 0, 0.0, pltpu.roll(xt, 1, 1)),
        xt,
        jnp.where(column == W - 1, 0.0, pltpu.roll(xt, lanes - 1, 1)),
    )
    per_frame = (ROWS_DEV + 4) * W
    for e in range(3):
        odd = pltpu.roll(shifted[e], lanes - W, 1).astype(bf16)
        even = shifted[e].astype(bf16)
        for b in range(3):
            source, start = ((even, 0), (odd, 0), (even, 2 * W))[b]
            for a in range(3):
                k = ((a * 3 + b) * 3 + e) * LAT_CH
                for t in range(FMAX):
                    at = (t + a) * per_frame + start
                    xs_ref[k : k + LAT_CH, t * rows * W : (t + 1) * rows * W] = source[:, at : at + rows * W]
    cells = rows * W
    row = lax.broadcasted_iota(jnp.int32, (cells, mid), 0)
    first_column = (row % W) == 0
    last_column = (row % W) == W - 1
    outside = jnp.logical_or(
        jnp.logical_and(row < W, place == 0),
        jnp.logical_and(row >= cells - W, place == last),
    )

    def spread(frame, values):
        before = jnp.where(first_column, 0.0, pltpu.roll(values, 1, 0)).astype(bf16)
        after = jnp.where(last_column, 0.0, pltpu.roll(values, cells - 1, 0)).astype(bf16)
        here = values.astype(bf16)
        h_ref[0, frame, :, 0:mid] = before
        h_ref[0, frame, :, mid : 2 * mid] = here
        h_ref[1, frame, :, 0:mid] = here
        h_ref[1, frame, :, mid : 2 * mid] = after

    for frame in range(2):
        values = jnp.concatenate(
            [top_ref[frame], fc_ref[frame], bot_ref[frame]], axis=0
        ).astype(f32)
        spread(frame, jnp.where(outside, 0.0, values))
    bias = b1_ref[...]
    gain = gain_ref[...]
    for t in range(FMAX):
        pre = lax.dot_general(
            xs_ref[:, t * cells : (t + 1) * cells],
            w1_ref[...],
            (((0,), (0,)), ((), ())),
            preferred_element_type=f32,
        ) + bias
        inverse = lax.rsqrt(jnp.mean(pre * pre, axis=1, keepdims=True) + 1e-06)
        v = pre * inverse * gain
        half = 0.5 * v
        spread(2 + t, jnp.where(outside, 0.0, half + half * jnp.tanh(half)))
    own = slice(W, W + ROWS_DEV * W)
    for j in range(2):
        one = h_ref[1, 1 + j, own, 0:mid]
        two = h_ref[1, 2 + j, own, 0:mid]
        three = h_ref[1, 3 + j, own, 0:mid]
        fn_ref[j] = jnp.where(live == 1, one.astype(f32), jnp.where(live == 2, two.astype(f32), three.astype(f32))).astype(bf16)
    load.wait()
    near = (((0,), (1, 2)), ((0, 1), (2,)))

    @pl.loop(0, 3)
    def _(a):
        base = a * 9
        tap = [[w2_ref[base + b * 3 + e].astype(f32) for e in range(3)] for b in range(3)]
        for py in range(2):
            for dy in range(2):
                taps = [sum(tap[b][e] for b in near[py][dy]) for e in range(3)]
                for px in range(2):
                    for dx in range(2):
                        total = sum(taps[e] for e in near[px][dx])
                        wc_ref[py * 2 + px, a * 2 + dy, dx * mid : (dx + 1) * mid, 0:OUT_CH] = total.astype(bf16)

    bias2 = b2_ref[...]
    block = ROWS_DEV * W
    for py in range(2):
        for px in range(2):
            total = None
            for a in range(3):
                for dy in range(2):
                    at = (py + dy) * W
                    left = h_ref[px, a : a + FMAX, at : at + block, :].reshape(FMAX * block, 2 * mid)
                    part = jnp.dot(left, wc_ref[py * 2 + px, a * 2 + dy], preferred_element_type=f32)
                    total = part if total is None else total + part
            total = (total + bias2).reshape(FMAX, ROWS_DEV, W, 256)
            for t in range(FMAX):
                kept = jnp.where(t < live, total[t], 0.0)
                for part in range(2):
                    ob_ref[part, t, :, pl.ds(px, W, stride=2), :] = kept[:, :, part * 128 : (part + 1) * 128]
        for t in range(FMAX):
            for y in range(ROWS_DEV):
                out_ref[t, 2 * y + py, :, 0:128] = ob_ref[0, t, y].astype(bf16)
                out_ref[t, 2 * y + py, :, 128:OUT_CH] = ob_ref[1, t, y, :, 0 : OUT_CH - 128].astype(bf16)


def decode(live, place, last, window, first_weight, first_bias, norm_gain, feature_cache, above, below, second_weight, second_bias):
    rows = ROWS_DEV + 2
    vm = pl.BlockSpec(memory_space=pltpu.VMEM)
    sm = pl.BlockSpec(memory_space=pltpu.SMEM)
    f32, bf16 = jnp.float32, jnp.bfloat16
    return pl.pallas_call(
        decode_kernel,
        out_shape=(
            jax.ShapeDtypeStruct((FMAX, 2 * ROWS_DEV, 2 * W, OUT_CH), bf16),
            jax.ShapeDtypeStruct((2, ROWS_DEV * W, MID_CH), bf16),
        ),
        in_specs=[sm, sm, vm, vm, vm, vm, vm, vm, vm, pl.BlockSpec(memory_space=pl.ANY), vm],
        out_specs=(vm, vm),
        scratch_shapes=[
            pltpu.VMEM((27, MID_CH, OUT_CH), bf16),
            pltpu.VMEM((4, 6, 2 * MID_CH, 256), bf16),
            pltpu.VMEM((27 * LAT_CH, FMAX * rows * W), bf16),
            pltpu.VMEM((2, 5, rows * W, 2 * MID_CH), bf16),
            pltpu.VMEM((2, FMAX, ROWS_DEV, 2 * W, 128), f32),
            pltpu.SemaphoreType.DMA,
        ],
        compiler_params=pltpu.CompilerParams(vmem_limit_bytes=60 * 1024 * 1024),
        cost_estimate=pl.CostEstimate(flops=6_200_000_000, bytes_accessed=7_000_000, transcendentals=442368),
    )(
        jnp.reshape(live, (1,)).astype(jnp.int32),
        jnp.stack([place, last]).astype(jnp.int32),
        window,
        first_weight.reshape(27 * LAT_CH, MID_CH),
        first_bias.reshape(1, MID_CH),
        norm_gain.reshape(1, MID_CH),
        feature_cache.reshape(2, ROWS_DEV * W, MID_CH),
        above.reshape(2, W, MID_CH),
        below.reshape(2, W, MID_CH),
        second_weight.reshape(27, MID_CH, OUT_CH),
        jnp.pad(second_bias, (0, 256 - OUT_CH)).reshape(1, 256),
    )


def body(
    latents,
    layout,
    assign,
    counts,
    latent_cache,
    feature_cache,
    first_weight,
    first_bias,
    norm_gain,
    second_weight,
    second_bias,
):
    devices = lax.axis_size("seq")
    myself = lax.axis_index("seq")
    per_group = devices // REQS
    offset = per_group // 2
    height = ROWS_DEV * per_group
    tile_cells = FMAX * ROWS_DEV * W
    per_peer = tile_cells // devices
    numbers = tile_numbers(layout, assign, per_group, devices)
    own_numbers = lax.dynamic_index_in_dim(numbers, myself, 0, keepdims=False)
    sending_order = jnp.argsort(own_numbers)
    outgoing = jnp.take(latents, sending_order, axis=1).reshape(LAT_CH, devices, per_peer)
    incoming = lax.all_to_all(outgoing, "seq", split_axis=1, concat_axis=1, tiled=True)
    arrived = lax.dynamic_slice_in_dim(jnp.sort(numbers, axis=1), myself * per_peer, per_peer, 1)
    placing = jnp.argsort((arrived - myself * tile_cells).reshape(-1))
    arranged = jnp.take(incoming.reshape(LAT_CH, tile_cells), placing, axis=1)
    window = jnp.transpose(arranged.reshape(LAT_CH, FMAX, ROWS_DEV, W), (1, 2, 3, 0))
    place = (myself + offset) % devices
    position = place % per_group
    request = jnp.take(assign, place // per_group)
    live_frames = jnp.take(counts, request)
    first_input = jnp.concatenate([latent_cache.reshape(2, ROWS_DEV, W, LAT_CH), window], axis=0)
    padded = keep_rows(padded_2(first_input, (("seq", 1),), 2), 2, position, height)
    ring = lax.axis_size("seq")
    up = [(i, (i + 1) % ring) for i in range(ring)]
    above = lax.ppermute(feature_cache[:, -1], "seq", up)
    below = lax.ppermute(feature_cache[:, 0], "seq", [(j, i) for i, j in up])
    cells = jnp.transpose(padded, (3, 0, 1, 2)).reshape(LAT_CH, -1)
    decoded_frames, feature_next = decode(
        live_frames, position, per_group - 1, cells, first_weight, first_bias, norm_gain,
        feature_cache, above, below, second_weight, second_bias,
    )
    feature_next = feature_next.reshape(2, ROWS_DEV, W, MID_CH)
    latent_next = lax.dynamic_slice_in_dim(first_input, live_frames, 2, 0).reshape(
        2, ROWS_DEV, W * LAT_CH
    )
    return (decoded_frames, latent_next, feature_next)


def solution(mesh):
    return jax.shard_map(
        body,
        mesh=mesh,
        in_specs=(
            P(None, ("rep", "seq")),
            P("rep", None),
            P("rep"),
            P("rep"),
            P(None, ("rep", "seq"), None),
            P(None, ("rep", "seq"), None, None),
            P(),
            P(),
            P(),
            P(),
            P(),
        ),
        out_specs=(
            P(None, ("rep", "seq"), None, None),
            P(None, ("rep", "seq"), None),
            P(None, ("rep", "seq"), None, None),
        ),
        check_vma=False,
    )
```

```python
import functools

import jax
import jax.numpy as jnp
from jax import lax
from jax.experimental import pallas as pl
from jax.experimental.pallas import tpu as pltpu
from jax.sharding import PartitionSpec as P

LAT_CH = 16
MID_CH = 384
OUT_CH = 192
REQS = 8
FMAX = 3
ROWS_DEV = 4
W = 64


def counted_before(marks, earlier):
    size = earlier.shape[0]
    carry = jnp.zeros((marks.shape[0], 1), jnp.float32)
    parts = []
    for start in range(0, marks.shape[1], size):
        block = marks[:, start : start + size]
        parts.append(jnp.dot(block.astype(jnp.bfloat16), earlier, preferred_element_type=jnp.float32) + carry)
        carry = carry + jnp.sum(block, axis=1, keepdims=True)
    return jnp.concatenate(parts, axis=1)


def gather_kernel(
    devices, assign_ref, layout_ref, latents_ref, cache_ref, features_ref,
    window_ref, above_ref, below_ref,
    send1_ref, recv1_ref, send2_ref, recv2_ref, table_ref, rim_out_ref, rim_in_ref,
    plane_ok, far_ok, s1, r1, s2, r2, sf, rf, sh, rh,
):
    f32, bf16, i32 = jnp.float32, jnp.bfloat16, jnp.int32
    per_group = devices // REQS
    plane = per_group // 2
    planes = devices // plane
    tile = ROWS_DEV * W
    tile_cells = FMAX * tile
    per_peer = tile_cells // devices
    rep, me = lax.axis_index("rep"), lax.axis_index("seq")
    z, p = me // plane, me % plane
    even = p % 2 == 0
    ahead, behind = (me + 1) % devices, (me + devices - 1) % devices
    first, final = p == 0, p == plane - 1

    def signal(semaphore, device):
        pl.semaphore_signal(semaphore, inc=1, device_id=(rep, device), device_id_type=pl.DeviceIdType.MESH)

    barrier = pltpu.get_barrier_semaphore()
    for q in range(0, plane, 2):
        @pl.when(p != q)
        def _():
            signal(barrier, z * plane + q)
    for i in range(1, planes):
        signal(barrier, ((z + i) % planes) * plane + (p // 2) * 2 + 1)

    @pl.when(final)
    def _():
        signal(barrier, ahead)

    @pl.when(first)
    def _():
        signal(barrier, behind)

    row_of = lax.broadcasted_iota(i32, (tile_cells // 3, tile_cells // 3), 0)
    lane_of = lax.broadcasted_iota(i32, (tile_cells // 3, tile_cells // 3), 1)
    earlier = (row_of < lane_of).astype(bf16)
    own = layout_ref[pl.ds(me, 1), :]
    request = ((own // (ROWS_DEV * per_group * W)) * 43) // 128
    group = jnp.zeros_like(own)
    for g in range(REQS):
        group = group + jnp.where(assign_ref[g] == request, g, 0)
    place = group * per_group + (own // tile) % per_group
    target = (place + devices - per_group // 2) % devices
    line = (target % plane) * planes + target // plane
    hit = lax.broadcasted_iota(i32, (devices, tile_cells), 0) == line
    marks = hit.astype(f32)
    order = counted_before(marks, earlier)
    latents = latents_ref[...]
    rows = []
    for k in range(per_peer):
        chosen = jnp.where(order == k, marks, 0.0).astype(bf16)
        rows.append(lax.dot_general(latents, chosen, (((1,), (1,)), ((), ())), preferred_element_type=f32))
    rows.append(jnp.zeros((devices - per_peer * LAT_CH, devices), f32))
    send1_ref[...] = jnp.transpose(jnp.concatenate(rows, axis=0)).astype(bf16).reshape(plane, planes, devices)

    @pl.when(even)
    def _():
        pl.semaphore_wait(barrier, plane - 1 + jnp.where(first, 1, 0))
        signal(plane_ok, me + 1)

    @pl.when(jnp.logical_not(even))
    def _():
        pl.semaphore_wait(plane_ok, 1)

    near = []
    for i in range(1, plane):
        q = (p + i) % plane
        near.append(pltpu.make_async_remote_copy(
            src_ref=send1_ref.at[q], dst_ref=recv1_ref.at[p], send_sem=s1.at[i], recv_sem=r1.at[i],
            device_id=(rep, z * plane + q), device_id_type=pl.DeviceIdType.MESH))
        near[-1].start()
    recv1_ref[p] = send1_ref[p]

    my_place = (me + per_group // 2) % devices
    my_group, position = my_place // per_group, my_place % per_group
    frame = ROWS_DEV * per_group * W
    offset = layout_ref[...] - (assign_ref[my_group] * (FMAX * frame) + position * tile)
    inside = jnp.logical_and(jnp.logical_and(offset >= 0, offset < FMAX * frame), (offset & (frame - tile)) == 0)
    within = ((offset // frame) * tile + (offset & (tile - 1))).astype(f32)
    marks = inside.astype(f32)
    order = counted_before(marks, earlier)
    spot = lax.broadcasted_iota(i32, (devices, tile_cells), 1).astype(f32)
    for k in range(per_peer):
        chosen = jnp.logical_and(order == k, inside)
        home = jnp.sum(jnp.where(chosen, within, 0.0), axis=1, keepdims=True)
        table_ref[k * devices : (k + 1) * devices, :] = (home == spot).astype(bf16)

    for copy in near:
        copy.wait()
    to = lax.broadcasted_iota(i32, (devices, devices), 0)
    source = lax.broadcasted_iota(i32, (devices, devices), 1)
    turn = (source == (to % plane) * planes + to // plane).astype(bf16)
    turned = jnp.dot(turn, recv1_ref[...].reshape(devices, devices), preferred_element_type=f32)
    send2_ref[...] = turned.reshape(planes, plane, devices).astype(bf16)

    @pl.when(jnp.logical_not(even))
    def _():
        pl.semaphore_wait(barrier, 2 * (planes - 1) + jnp.where(final, 1, 0))
        signal(far_ok, me - 1)

    @pl.when(even)
    def _():
        pl.semaphore_wait(far_ok, 1)

    far = []
    for i in range(1, planes):
        q = (z + i) % planes
        far.append(pltpu.make_async_remote_copy(
            src_ref=send2_ref.at[q], dst_ref=recv2_ref.at[z], send_sem=s2.at[i], recv_sem=r2.at[i],
            device_id=(rep, q * plane + p), device_id_type=pl.DeviceIdType.MESH))
        far[-1].start()
    recv2_ref[z] = send2_ref[z]
    sides = []
    for side in range(2):
        sides.append(pltpu.make_async_remote_copy(
            src_ref=features_ref.at[:, pl.ds((ROWS_DEV - 1) * W * (1 - side), W)],
            dst_ref=(above_ref, below_ref)[side],
            send_sem=sf.at[side], recv_sem=rf.at[side],
            device_id=(rep, (ahead, behind)[side]), device_id_type=pl.DeviceIdType.MESH))
        sides[-1].start()
    for copy in far:
        copy.wait()
    arrived = jnp.transpose(recv2_ref[...].astype(f32).reshape(devices, devices))
    arrived = jnp.concatenate([arrived[k * LAT_CH : (k + 1) * LAT_CH] for k in range(per_peer)], axis=1)
    cells = jnp.dot(arrived.astype(bf16), table_ref[...], preferred_element_type=f32).astype(bf16)
    frames = [cache_ref[:, f * tile : (f + 1) * tile] for f in range(2)]
    frames = frames + [cells[:, f * tile : (f + 1) * tile] for f in range(FMAX)]
    rim = 2 * W
    for f in range(2 + FMAX):
        rim_out_ref[0, f] = frames[f][:, tile - rim :]
        rim_out_ref[1, f] = frames[f][:, 0:rim]
    edges = []
    for side in range(2):
        edges.append(pltpu.make_async_remote_copy(
            src_ref=rim_out_ref.at[side], dst_ref=rim_in_ref.at[side],
            send_sem=sh.at[side], recv_sem=rh.at[side],
            device_id=(rep, (ahead, behind)[side]), device_id_type=pl.DeviceIdType.MESH))
        edges[-1].start()
    for copy in sides + edges:
        copy.wait()
    nothing = jnp.zeros((LAT_CH, rim), f32)
    for f in range(2 + FMAX):
        top = jnp.where(position == 0, nothing, rim_in_ref[0, f].astype(f32)).astype(bf16)
        bottom = jnp.where(position == per_group - 1, nothing, rim_in_ref[1, f].astype(f32)).astype(bf16)
        at = f * (tile + 2 * rim)
        window_ref[:, at : at + rim] = top
        window_ref[:, at + rim : at + rim + tile] = frames[f]
        window_ref[:, at + rim + tile : at + 2 * rim + tile] = bottom


def gather(devices, assign, layout, latents, latent_cache, feature_cache):
    plane = devices // REQS // 2
    planes = devices // plane
    cells = FMAX * ROWS_DEV * W
    vm = pl.BlockSpec(memory_space=pltpu.VMEM)
    bf16, dma = jnp.bfloat16, pltpu.SemaphoreType.DMA
    return pl.pallas_call(
        functools.partial(gather_kernel, devices),
        out_shape=(
            jax.ShapeDtypeStruct((LAT_CH, (2 + FMAX) * (ROWS_DEV + 4) * W), bf16),
            jax.ShapeDtypeStruct((2, W, MID_CH), bf16),
            jax.ShapeDtypeStruct((2, W, MID_CH), bf16),
        ),
        in_specs=[pl.BlockSpec(memory_space=pltpu.SMEM), vm, vm, vm, vm],
        out_specs=(vm, vm, vm),
        scratch_shapes=[
            pltpu.VMEM((plane, planes, devices), bf16),
            pltpu.VMEM((plane, planes, devices), bf16),
            pltpu.VMEM((planes, plane, devices), bf16),
            pltpu.VMEM((planes, plane, devices), bf16),
            pltpu.VMEM((cells, cells), bf16),
            pltpu.VMEM((2, 2 + FMAX, LAT_CH, 2 * W), bf16),
            pltpu.VMEM((2, 2 + FMAX, LAT_CH, 2 * W), bf16),
            pltpu.SemaphoreType.REGULAR,
            pltpu.SemaphoreType.REGULAR,
            dma((plane,)), dma((plane,)), dma((planes,)), dma((planes,)),
            dma((2,)), dma((2,)), dma((2,)), dma((2,)),
        ],
        compiler_params=pltpu.CompilerParams(collective_id=0, has_side_effects=True, vmem_limit_bytes=40 * 1024 * 1024),
        cost_estimate=pl.CostEstimate(flops=1_000_000_000, bytes_accessed=1_500_000, transcendentals=0),
    )(
        assign,
        layout,
        latents,
        jnp.transpose(latent_cache.reshape(2, ROWS_DEV, W, LAT_CH), (3, 0, 1, 2)).reshape(LAT_CH, 2 * ROWS_DEV * W),
        feature_cache.reshape(2, ROWS_DEV * W, MID_CH),
    )


def decode_kernel(
    live_ref, place_ref, xt_ref, w1_ref, b1_ref, gain_ref, fc_ref, top_ref, bot_ref, w2_hbm, b2_ref,
    out_ref, fn_ref, w2_ref, wc_ref, xs_ref, h_ref, sem,
):
    live = live_ref[0]
    place = place_ref[0]
    last = place_ref[1]
    load = pltpu.make_async_copy(w2_hbm, w2_ref, sem)
    load.start()
    f32, bf16 = jnp.float32, jnp.bfloat16
    rows, mid = ROWS_DEV + 2, MID_CH
    xt = xt_ref[...].astype(f32)
    lanes = xt.shape[1]
    column = lax.broadcasted_iota(jnp.int32, xt.shape, 1) % W
    shifted = (
        jnp.where(column == 0, 0.0, pltpu.roll(xt, 1, 1)),
        xt,
        jnp.where(column == W - 1, 0.0, pltpu.roll(xt, lanes - 1, 1)),
    )
    per_frame = (ROWS_DEV + 4) * W
    for e in range(3):
        odd = pltpu.roll(shifted[e], lanes - W, 1).astype(bf16)
        even = shifted[e].astype(bf16)
        for b in range(3):
            source, start = ((even, 0), (odd, 0), (even, 2 * W))[b]
            for a in range(3):
                k = ((a * 3 + b) * 3 + e) * LAT_CH
                for t in range(FMAX):
                    at = (t + a) * per_frame + start
                    xs_ref[k : k + LAT_CH, t * rows * W : (t + 1) * rows * W] = source[:, at : at + rows * W]
    cells = rows * W
    row = lax.broadcasted_iota(jnp.int32, (cells, mid), 0)
    first_column = (row % W) == 0
    last_column = (row % W) == W - 1
    outside = jnp.logical_or(
        jnp.logical_and(row < W, place == 0),
        jnp.logical_and(row >= cells - W, place == last),
    )

    def spread(frame, values):
        before = jnp.where(first_column, 0.0, pltpu.roll(values, 1, 0)).astype(bf16)
        after = jnp.where(last_column, 0.0, pltpu.roll(values, cells - 1, 0)).astype(bf16)
        here = values.astype(bf16)
        h_ref[0, frame, :, 0:mid] = before
        h_ref[0, frame, :, mid : 2 * mid] = here
        h_ref[1, frame, :, 0:mid] = here
        h_ref[1, frame, :, mid : 2 * mid] = after

    for frame in range(2):
        values = jnp.concatenate(
            [top_ref[frame], fc_ref[frame], bot_ref[frame]], axis=0
        ).astype(f32)
        spread(frame, jnp.where(outside, 0.0, values))
    bias = b1_ref[...]
    gain = gain_ref[...]
    for t in range(FMAX):
        pre = lax.dot_general(
            xs_ref[:, t * cells : (t + 1) * cells],
            w1_ref[...],
            (((0,), (0,)), ((), ())),
            preferred_element_type=f32,
        ) + bias
        inverse = lax.rsqrt(jnp.mean(pre * pre, axis=1, keepdims=True) + 1e-06)
        v = pre * inverse * gain
        half = 0.5 * v
        spread(2 + t, jnp.where(outside, 0.0, half + half * jnp.tanh(half)))
    own = slice(W, W + ROWS_DEV * W)
    for j in range(2):
        one = h_ref[1, 1 + j, own, 0:mid]
        two = h_ref[1, 2 + j, own, 0:mid]
        three = h_ref[1, 3 + j, own, 0:mid]
        fn_ref[j] = jnp.where(live == 1, one.astype(f32), jnp.where(live == 2, two.astype(f32), three.astype(f32))).astype(bf16)
    load.wait()
    near = (((0,), (1, 2)), ((0, 1), (2,)))

    @pl.loop(0, 3)
    def _(a):
        base = a * 9
        tap = [[w2_ref[base + b * 3 + e].astype(f32) for e in range(3)] for b in range(3)]
        for slot, (py, dy) in enumerate(((0, 0), (0, 1), (1, 0), (1, 1))):
            taps = [sum(tap[b][e] for b in near[py][dy]) for e in range(3)]
            for px in range(2):
                for dx in range(2):
                    total = sum(taps[e] for e in near[px][dx])
                    wc_ref[px, a, slot * OUT_CH : (slot + 1) * OUT_CH, dx * mid : (dx + 1) * mid] = total.astype(bf16)

    bias2 = b2_ref[...]
    block = ROWS_DEV * W
    source = lax.broadcasted_iota(jnp.int32, (block, block), 0)
    target = lax.broadcasted_iota(jnp.int32, (block, block), 1)
    parity, line, cell = source // (2 * W), source // W % 2, source % W
    weave = (target == line * 2 * W + cell * 2 + parity).astype(bf16)

    @pl.loop(0, FMAX)
    def _(t):
        kept = []
        for px in range(2):
            both = [None, None]
            for a in range(3):
                for r in range(3):
                    right = h_ref[px, t + a, r * W : r * W + block, :]
                    first, count = ((0, 1), (1, 2), (3, 1))[r]
                    left = wc_ref[px, a, first * OUT_CH : (first + count) * OUT_CH, :]
                    part = lax.dot_general(left, right, (((1,), (1,)), ((), ())), preferred_element_type=f32)
                    for i in range(count):
                        py = (first + i) // 2
                        piece = part[i * OUT_CH : (i + 1) * OUT_CH]
                        both[py] = piece if both[py] is None else both[py] + piece
            kept.append([jnp.where(t < live, b + bias2, 0.0).astype(bf16) for b in both])
        for py in range(2):
            for pair in range(ROWS_DEV // 2):
                lanes = slice(pair * 2 * W, (pair + 1) * 2 * W)
                joined = jnp.concatenate([kept[0][py][:, lanes], kept[1][py][:, lanes]], axis=1)
                woven = jnp.dot(joined, weave, preferred_element_type=f32).astype(bf16)
                for line in range(2):
                    out_ref[t, 2 * (2 * pair + line) + py] = woven[:, line * 2 * W : (line + 1) * 2 * W]


def decode(live, place, last, window, first_weight, first_bias, norm_gain, feature_cache, above, below, second_weight, second_bias):
    rows = ROWS_DEV + 2
    vm = pl.BlockSpec(memory_space=pltpu.VMEM)
    sm = pl.BlockSpec(memory_space=pltpu.SMEM)
    f32, bf16 = jnp.float32, jnp.bfloat16
    frames, features = pl.pallas_call(
        decode_kernel,
        out_shape=(
            jax.ShapeDtypeStruct((FMAX, 2 * ROWS_DEV, OUT_CH, 2 * W), bf16),
            jax.ShapeDtypeStruct((2, ROWS_DEV * W, MID_CH), bf16),
        ),
        in_specs=[sm, sm, vm, vm, vm, vm, vm, vm, vm, pl.BlockSpec(memory_space=pl.ANY), vm],
        out_specs=(vm, vm),
        scratch_shapes=[
            pltpu.VMEM((27, OUT_CH, MID_CH), bf16),
            pltpu.VMEM((2, 3, 4 * OUT_CH, 2 * MID_CH), bf16),
            pltpu.VMEM((27 * LAT_CH, FMAX * rows * W), bf16),
            pltpu.VMEM((2, 5, rows * W, 2 * MID_CH), bf16),
            pltpu.SemaphoreType.DMA,
        ],
        compiler_params=pltpu.CompilerParams(vmem_limit_bytes=60 * 1024 * 1024),
        cost_estimate=pl.CostEstimate(flops=6_200_000_000, bytes_accessed=7_000_000, transcendentals=442368),
    )(
        jnp.reshape(live, (1,)).astype(jnp.int32),
        jnp.stack([place, last]).astype(jnp.int32),
        window,
        first_weight.reshape(27 * LAT_CH, MID_CH),
        first_bias.reshape(1, MID_CH),
        norm_gain.reshape(1, MID_CH),
        feature_cache.reshape(2, ROWS_DEV * W, MID_CH),
        above.reshape(2, W, MID_CH),
        below.reshape(2, W, MID_CH),
        jnp.swapaxes(second_weight, 3, 4).reshape(27, OUT_CH, MID_CH),
        second_bias.reshape(OUT_CH, 1),
    )
    return jnp.swapaxes(frames, 2, 3), features


def body(
    latents,
    layout,
    assign,
    counts,
    latent_cache,
    feature_cache,
    first_weight,
    first_bias,
    norm_gain,
    second_weight,
    second_bias,
):
    devices = lax.axis_size("seq")
    per_group = devices // REQS
    place = (lax.axis_index("seq") + per_group // 2) % devices
    live = counts[assign[place // per_group]]
    window, above, below = gather(devices, assign, layout, latents, latent_cache, feature_cache)
    decoded_frames, feature_next = decode(
        live, place % per_group, per_group - 1, window, first_weight, first_bias, norm_gain,
        feature_cache, above, below, second_weight, second_bias,
    )
    own = window.reshape(LAT_CH, 2 + FMAX, ROWS_DEV + 4, W)[:, :, 2 : 2 + ROWS_DEV]
    latent_next = lax.dynamic_slice_in_dim(own, live, 2, 1)
    latent_next = jnp.transpose(latent_next, (1, 2, 3, 0)).reshape(2, ROWS_DEV, W * LAT_CH)
    return (decoded_frames, latent_next, feature_next.reshape(2, ROWS_DEV, W, MID_CH))


def solution(mesh):
    return jax.shard_map(
        body,
        mesh=mesh,
        in_specs=(
            P(None, ("rep", "seq")),
            P("rep", None),
            P("rep"),
            P("rep"),
            P(None, ("rep", "seq"), None),
            P(None, ("rep", "seq"), None, None),
            P(),
            P(),
            P(),
            P(),
            P(),
        ),
        out_specs=(
            P(None, ("rep", "seq"), None, None),
            P(None, ("rep", "seq"), None),
            P(None, ("rep", "seq"), None, None),
        ),
        check_vma=False,
    )
```

```python
import functools

import jax
import jax.numpy as jnp
from jax import lax
from jax.experimental import pallas as pl
from jax.experimental.pallas import tpu as pltpu
from jax.sharding import PartitionSpec as P

LAT_CH = 16
MID_CH = 384
OUT_CH = 192
REQS = 8
FMAX = 3
ROWS_DEV = 4
W = 64


def spread_of_cells():
    lane = lax.broadcasted_iota(jnp.int32, (W * LAT_CH, W), 0)
    cell = lax.broadcasted_iota(jnp.int32, (W * LAT_CH, W), 1)
    fold = (lane // LAT_CH == cell).astype(jnp.bfloat16)
    channel = lax.broadcasted_iota(jnp.int32, (LAT_CH, W * LAT_CH), 0)
    member = lax.broadcasted_iota(jnp.int32, (LAT_CH, W * LAT_CH), 1) % LAT_CH == channel
    return fold, member


def rows_outside(position, last):
    cells = (ROWS_DEV + 2) * W
    row = lax.broadcasted_iota(jnp.int32, (cells, MID_CH), 0)
    above = jnp.logical_and(row < W, position == 0)
    return jnp.logical_or(above, jnp.logical_and(row >= cells - W, position == last))


def lay_out(target, frame, values):
    cells = values.shape[0]
    column = lax.broadcasted_iota(jnp.int32, values.shape, 0) % W
    before = jnp.where(column == 0, 0.0, pltpu.roll(values, 1, 0)).astype(jnp.bfloat16)
    after = jnp.where(column == W - 1, 0.0, pltpu.roll(values, cells - 1, 0)).astype(jnp.bfloat16)
    here = values.astype(jnp.bfloat16)
    target[0, frame, :, 0:MID_CH] = before
    target[0, frame, :, MID_CH : 2 * MID_CH] = here
    target[1, frame, :, 0:MID_CH] = here
    target[1, frame, :, MID_CH : 2 * MID_CH] = after


def combine_taps(weight, upper, middle, lower):
    near = (((0,), (1, 2)), ((0, 1), (2,)))

    @pl.loop(0, 3)
    def _(a):
        base = a * 9
        tap = [[weight[base + b * 3 + e].astype(jnp.float32) for e in range(3)] for b in range(3)]
        for target, start, py, dy in ((upper, 0, 0, 0), (middle, 0, 0, 1), (middle, OUT_CH, 1, 0), (lower, 0, 1, 1)):
            taps = [sum(tap[b][e] for b in near[py][dy]) for e in range(3)]
            for px in range(2):
                for dx in range(2):
                    total = sum(taps[e] for e in near[px][dx]).astype(jnp.bfloat16)
                    target[px, a, start : start + OUT_CH, dx * MID_CH : (dx + 1) * MID_CH] = total


def add_products(sums, features, upper, middle, lower, px, frame, a, count, times, started):
    block = ROWS_DEV * W
    begun = set()
    for r, weights in enumerate((middle, upper, lower)):
        row = (1, 0, 2)[r]
        right = features[px, frame, row * W : row * W + block, :]
        left = weights[px, a : a + count]
        height = left.shape[1]
        part = lax.dot_general(
            left.reshape(count * height, left.shape[2]), right, (((1,), (1,)), ((), ())), preferred_element_type=jnp.float32
        )
        for i, t in enumerate(times):
            for py in ((0, 1), (0,), (1,))[r]:
                at = i * height + (py * OUT_CH if r == 0 else 0)
                piece = part[at : at + OUT_CH]
                if r == 0 and t not in started:
                    sums[t, px, py] = piece
                else:
                    sums[t, px, py] = sums[t, px, py] + piece


def counted_before(marks, earlier):
    size = earlier.shape[0]
    carry = jnp.zeros((marks.shape[0], 1), jnp.float32)
    parts = []
    for start in range(0, marks.shape[1], size):
        block = marks[:, start : start + size]
        parts.append(jnp.dot(block.astype(jnp.bfloat16), earlier, preferred_element_type=jnp.float32) + carry)
        carry = carry + jnp.sum(block, axis=1, keepdims=True)
    return jnp.concatenate(parts, axis=1)


def gather_kernel(
    devices, assign_ref, layout_hbm, latents_hbm, cache_hbm, features_hbm, weight_hbm,
    window_ref, upper_hbm, middle_hbm, lower_hbm, part_hbm,
    layout_ref, latents_ref, cache_ref, features_ref, weight_ref, above_ref, below_ref,
    upper_ref, middle_ref, lower_ref, small_ref, part_ref, load_sem, store_sem,
    send1_ref, recv1_ref, send2_ref, recv2_ref, table_ref, rim_out_ref, rim_in_ref,
    plane_ok, far_ok, s1, r1, s2, r2, sf, rf, sh, rh,
):
    f32, bf16, i32 = jnp.float32, jnp.bfloat16, jnp.int32
    per_group = devices // REQS
    plane = per_group // 2
    planes = devices // plane
    tile = ROWS_DEV * W
    tile_cells = FMAX * tile
    per_peer = tile_cells // devices
    rep, me = lax.axis_index("rep"), lax.axis_index("seq")
    z, p = me // plane, me % plane
    even = p % 2 == 0
    ahead, behind = (me + 1) % devices, (me + devices - 1) % devices
    first, final = p == 0, p == plane - 1

    def signal(semaphore, device):
        pl.semaphore_signal(semaphore, inc=1, device_id=(rep, device), device_id_type=pl.DeviceIdType.MESH)

    loads = [
        pltpu.make_async_copy(source, target, load_sem.at[i])
        for i, (source, target) in enumerate((
            (layout_hbm, layout_ref), (latents_hbm, latents_ref), (cache_hbm, cache_ref), (features_hbm, features_ref),
        ))
    ]
    loads = loads + [
        pltpu.make_async_copy(weight_hbm.at[3 * i : 3 * i + 3], weight_ref.at[3 * i : 3 * i + 3], load_sem.at[4 + i])
        for i in range(9)
    ]
    for copy in loads:
        copy.start()

    barrier = pltpu.get_barrier_semaphore()
    for q in range(0, plane, 2):
        @pl.when(p != q)
        def _():
            signal(barrier, z * plane + q)
    for i in range(1, planes):
        signal(barrier, ((z + i) % planes) * plane + (p // 2) * 2 + 1)

    @pl.when(final)
    def _():
        signal(barrier, ahead)

    @pl.when(first)
    def _():
        signal(barrier, behind)

    row_of = lax.broadcasted_iota(i32, (tile_cells // 3, tile_cells // 3), 0)
    lane_of = lax.broadcasted_iota(i32, (tile_cells // 3, tile_cells // 3), 1)
    earlier = (row_of < lane_of).astype(bf16)
    loads[0].wait()
    own = layout_ref[pl.ds(me, 1), :]
    request = ((own // (ROWS_DEV * per_group * W)) * 43) // 128
    group = jnp.zeros_like(own)
    for g in range(REQS):
        group = group + jnp.where(assign_ref[g] == request, g, 0)
    place = group * per_group + (own // tile) % per_group
    target = (place + devices - per_group // 2) % devices
    line = (target % plane) * planes + target // plane
    hit = lax.broadcasted_iota(i32, (devices, tile_cells), 0) == line
    marks = hit.astype(f32)
    order = counted_before(marks, earlier)
    loads[1].wait()
    latents = latents_ref[...]
    rows = []
    for k in range(per_peer):
        chosen = jnp.where(order == k, marks, 0.0).astype(bf16)
        rows.append(lax.dot_general(latents, chosen, (((1,), (1,)), ((), ())), preferred_element_type=f32))
    rows.append(jnp.zeros((devices - per_peer * LAT_CH, devices), f32))
    send1_ref[...] = jnp.transpose(jnp.concatenate(rows, axis=0)).astype(bf16).reshape(plane, planes, devices)

    @pl.when(even)
    def _():
        pl.semaphore_wait(barrier, plane - 1 + jnp.where(first, 1, 0))
        signal(plane_ok, me + 1)

    @pl.when(jnp.logical_not(even))
    def _():
        pl.semaphore_wait(plane_ok, 1)

    near = []
    for i in range(1, plane):
        q = (p + i) % plane
        near.append(pltpu.make_async_remote_copy(
            src_ref=send1_ref.at[q], dst_ref=recv1_ref.at[p], send_sem=s1.at[i], recv_sem=r1.at[i],
            device_id=(rep, z * plane + q), device_id_type=pl.DeviceIdType.MESH))
        near[-1].start()
    recv1_ref[p] = send1_ref[p]

    my_place = (me + per_group // 2) % devices
    my_group, position = my_place // per_group, my_place % per_group
    frame = ROWS_DEV * per_group * W
    offset = layout_ref[...] - (assign_ref[my_group] * (FMAX * frame) + position * tile)
    inside = jnp.logical_and(jnp.logical_and(offset >= 0, offset < FMAX * frame), (offset & (frame - tile)) == 0)
    within = ((offset // frame) * tile + (offset & (tile - 1))).astype(f32)
    marks = inside.astype(f32)
    order = counted_before(marks, earlier)
    spot = lax.broadcasted_iota(i32, (devices, tile_cells), 1).astype(f32)
    for k in range(per_peer):
        chosen = jnp.logical_and(order == k, inside)
        home = jnp.sum(jnp.where(chosen, within, 0.0), axis=1, keepdims=True)
        table_ref[k * devices : (k + 1) * devices, :] = (home == spot).astype(bf16)

    for copy in near:
        copy.wait()
    to = lax.broadcasted_iota(i32, (devices, devices), 0)
    source = lax.broadcasted_iota(i32, (devices, devices), 1)
    turn = (source == (to % plane) * planes + to // plane).astype(bf16)
    turned = jnp.dot(turn, recv1_ref[...].reshape(devices, devices), preferred_element_type=f32)
    send2_ref[...] = turned.reshape(planes, plane, devices).astype(bf16)

    @pl.when(jnp.logical_not(even))
    def _():
        pl.semaphore_wait(barrier, 2 * (planes - 1) + jnp.where(final, 1, 0))
        signal(far_ok, me - 1)

    @pl.when(even)
    def _():
        pl.semaphore_wait(far_ok, 1)

    far = []
    for i in range(1, planes):
        q = (z + i) % planes
        far.append(pltpu.make_async_remote_copy(
            src_ref=send2_ref.at[q], dst_ref=recv2_ref.at[z], send_sem=s2.at[i], recv_sem=r2.at[i],
            device_id=(rep, q * plane + p), device_id_type=pl.DeviceIdType.MESH))
        far[-1].start()
    recv2_ref[z] = send2_ref[z]
    loads[3].wait()
    sides = []
    for side in range(2):
        sides.append(pltpu.make_async_remote_copy(
            src_ref=features_ref.at[:, pl.ds((ROWS_DEV - 1) * W * (1 - side), W)],
            dst_ref=(above_ref, below_ref)[side],
            send_sem=sf.at[side], recv_sem=rf.at[side],
            device_id=(rep, (ahead, behind)[side]), device_id_type=pl.DeviceIdType.MESH))
        sides[-1].start()

    loads[2].wait()
    wide = cache_ref[...].astype(f32).reshape(2 * ROWS_DEV, W * LAT_CH)
    fold, member = spread_of_cells()
    stacked = jnp.concatenate([
        jnp.where(member, jnp.broadcast_to(wide[i : i + 1], member.shape), 0.0) for i in range(2 * ROWS_DEV)
    ], axis=0).astype(bf16)
    folded = jnp.dot(stacked, fold, preferred_element_type=f32)
    cached = jnp.concatenate([folded[i * LAT_CH : (i + 1) * LAT_CH] for i in range(2 * ROWS_DEV)], axis=1).astype(bf16)

    for copy in loads[4:]:
        copy.wait()
    combine_taps(weight_ref, upper_ref, middle_ref, lower_ref)
    stores = [
        pltpu.make_async_copy(source.at[px, a], target.at[px, a], store_sem.at[i, px, a])
        for i, (source, target) in enumerate(((upper_ref, upper_hbm), (middle_ref, middle_hbm), (lower_ref, lower_hbm)))
        for px in range(2)
        for a in range(3)
    ]
    for copy in stores:
        copy.start()

    for copy in sides:
        copy.wait()
    outside = rows_outside(position, per_group - 1)
    for f in range(2):
        values = jnp.concatenate([above_ref[f], features_ref[f], below_ref[f]], axis=0).astype(f32)
        lay_out(small_ref, f, jnp.where(outside, 0.0, values))
    for px in range(2):
        add_products(part_ref, small_ref, upper_ref, middle_ref, lower_ref, px, 1, 0, 2, (1, 0), {})
        add_products(part_ref, small_ref, upper_ref, middle_ref, lower_ref, px, 0, 0, 1, (0,), {0})
    saved = [pltpu.make_async_copy(part_ref.at[t], part_hbm.at[t], store_sem.at[3, 0, t]) for t in range(2)]
    for copy in saved:
        copy.start()
    for copy in far:
        copy.wait()
    arrived = jnp.transpose(recv2_ref[...].astype(f32).reshape(devices, devices))
    arrived = jnp.concatenate([arrived[k * LAT_CH : (k + 1) * LAT_CH] for k in range(per_peer)], axis=1)
    cells = jnp.dot(arrived.astype(bf16), table_ref[...], preferred_element_type=f32).astype(bf16)
    frames = [cached[:, f * tile : (f + 1) * tile] for f in range(2)]
    frames = frames + [cells[:, f * tile : (f + 1) * tile] for f in range(FMAX)]
    rim = 2 * W
    for f in range(2 + FMAX):
        rim_out_ref[0, f] = frames[f][:, tile - rim :]
        rim_out_ref[1, f] = frames[f][:, 0:rim]
    edges = []
    for side in range(2):
        edges.append(pltpu.make_async_remote_copy(
            src_ref=rim_out_ref.at[side], dst_ref=rim_in_ref.at[side],
            send_sem=sh.at[side], recv_sem=rh.at[side],
            device_id=(rep, (ahead, behind)[side]), device_id_type=pl.DeviceIdType.MESH))
        edges[-1].start()
    for copy in edges:
        copy.wait()
    nothing = jnp.zeros((LAT_CH, rim), f32)
    for f in range(2 + FMAX):
        top = jnp.where(position == 0, nothing, rim_in_ref[0, f].astype(f32)).astype(bf16)
        bottom = jnp.where(position == per_group - 1, nothing, rim_in_ref[1, f].astype(f32)).astype(bf16)
        at = f * (tile + 2 * rim)
        window_ref[:, at : at + rim] = top
        window_ref[:, at + rim : at + rim + tile] = frames[f]
        window_ref[:, at + rim + tile : at + 2 * rim + tile] = bottom
    for copy in stores + saved:
        copy.wait()


def gather(devices, assign, layout, latents, latent_cache, feature_cache, second_weight):
    plane = devices // REQS // 2
    planes = devices // plane
    cells = FMAX * ROWS_DEV * W
    vm, hbm = pl.BlockSpec(memory_space=pltpu.VMEM), pl.BlockSpec(memory_space=pl.ANY)
    bf16, dma = jnp.bfloat16, pltpu.SemaphoreType.DMA
    return pl.pallas_call(
        functools.partial(gather_kernel, devices),
        out_shape=(
            jax.ShapeDtypeStruct((LAT_CH, (2 + FMAX) * (ROWS_DEV + 4) * W), bf16),
            jax.ShapeDtypeStruct((2, 3, OUT_CH, 2 * MID_CH), bf16),
            jax.ShapeDtypeStruct((2, 3, 2 * OUT_CH, 2 * MID_CH), bf16),
            jax.ShapeDtypeStruct((2, 3, OUT_CH, 2 * MID_CH), bf16),
            jax.ShapeDtypeStruct((2, 2, 2, OUT_CH, ROWS_DEV * W), jnp.float32),
        ),
        in_specs=[pl.BlockSpec(memory_space=pltpu.SMEM), hbm, hbm, hbm, hbm, hbm],
        out_specs=(vm, hbm, hbm, hbm, hbm),
        scratch_shapes=[
            pltpu.VMEM((devices, cells), jnp.int32),
            pltpu.VMEM((LAT_CH, cells), bf16),
            pltpu.VMEM((2, ROWS_DEV, W * LAT_CH), bf16),
            pltpu.VMEM((2, ROWS_DEV * W, MID_CH), bf16),
            pltpu.VMEM((27, OUT_CH, MID_CH), bf16),
            pltpu.VMEM((2, W, MID_CH), bf16),
            pltpu.VMEM((2, W, MID_CH), bf16),
            pltpu.VMEM((2, 3, OUT_CH, 2 * MID_CH), bf16),
            pltpu.VMEM((2, 3, 2 * OUT_CH, 2 * MID_CH), bf16),
            pltpu.VMEM((2, 3, OUT_CH, 2 * MID_CH), bf16),
            pltpu.VMEM((2, 2, (ROWS_DEV + 2) * W, 2 * MID_CH), bf16),
            pltpu.VMEM((2, 2, 2, OUT_CH, ROWS_DEV * W), jnp.float32),
            dma((13,)),
            dma((4, 2, 3)),
            pltpu.VMEM((plane, planes, devices), bf16),
            pltpu.VMEM((plane, planes, devices), bf16),
            pltpu.VMEM((planes, plane, devices), bf16),
            pltpu.VMEM((planes, plane, devices), bf16),
            pltpu.VMEM((cells, cells), bf16),
            pltpu.VMEM((2, 2 + FMAX, LAT_CH, 2 * W), bf16),
            pltpu.VMEM((2, 2 + FMAX, LAT_CH, 2 * W), bf16),
            pltpu.SemaphoreType.REGULAR,
            pltpu.SemaphoreType.REGULAR,
            dma((plane,)), dma((plane,)), dma((planes,)), dma((planes,)),
            dma((2,)), dma((2,)), dma((2,)), dma((2,)),
        ],
        compiler_params=pltpu.CompilerParams(collective_id=0, has_side_effects=True, vmem_limit_bytes=56 * 1024 * 1024),
        cost_estimate=pl.CostEstimate(flops=3_000_000_000, bytes_accessed=13_000_000, transcendentals=0),
    )(
        assign,
        layout,
        latents,
        latent_cache,
        feature_cache.reshape(2, ROWS_DEV * W, MID_CH),
        jnp.swapaxes(second_weight, 3, 4).reshape(27, OUT_CH, MID_CH),
    )


def decode_kernel(
    per_group, place_axis, assign_ref, counts_ref, window_ref, w1_hbm, b1_hbm, gain_hbm, fc_hbm, upper_hbm, middle_hbm, lower_hbm,
    part_hbm, b2_hbm,
    out_hbm, ln_ref, fn_ref,
    w1_ref, b1_ref, gain_ref, fc_ref, upper_ref, middle_ref, lower_ref, sums_ref, b2_ref, xs_ref, h_ref, frames_ref,
    load_sem, out_sem,
):
    f32, bf16 = jnp.float32, jnp.bfloat16
    place = (lax.axis_index(place_axis) + per_group // 2) % (per_group * REQS)
    position = place % per_group
    live = counts_ref[assign_ref[place // per_group]]
    small = [
        pltpu.make_async_copy(source, target, load_sem.at[i])
        for i, (source, target) in enumerate((
            (w1_hbm, w1_ref), (b1_hbm, b1_ref), (gain_hbm, gain_ref), (b2_hbm, b2_ref), (fc_hbm, fc_ref),
        ))
    ]
    large = [pltpu.make_async_copy(part_hbm.at[t], sums_ref.at[t], load_sem.at[5 + t]) for t in range(2)]
    for i, (source, target) in enumerate(((middle_hbm, middle_ref), (upper_hbm, upper_ref), (lower_hbm, lower_ref))):
        for px in range(2):
            for a in range(3):
                large.append(pltpu.make_async_copy(source.at[px, a], target.at[px, a], load_sem.at[7 + i * 6 + px * 3 + a]))
    for copy in small + large:
        copy.start()
    rows = ROWS_DEV + 2
    cells, tile = rows * W, ROWS_DEV * W
    per_frame = (ROWS_DEV + 4) * W
    xt = window_ref[...].astype(f32)
    lanes = xt.shape[1]
    column = lax.broadcasted_iota(jnp.int32, xt.shape, 1) % W
    shifted = (
        jnp.where(column == 0, 0.0, pltpu.roll(xt, 1, 1)),
        xt,
        jnp.where(column == W - 1, 0.0, pltpu.roll(xt, lanes - 1, 1)),
    )
    for e in range(3):
        odd = pltpu.roll(shifted[e], lanes - W, 1).astype(bf16)
        even = shifted[e].astype(bf16)
        for b in range(3):
            source, start = ((even, 0), (odd, 0), (even, 2 * W))[b]
            for a in range(3):
                k = ((a * 3 + b) * 3 + e) * LAT_CH
                for t in range(FMAX):
                    at = (t + a) * per_frame + start
                    xs_ref[k : k + LAT_CH, t * cells : (t + 1) * cells] = source[:, at : at + cells]
    outside = rows_outside(position, per_group - 1)
    for copy in small:
        copy.wait()
    bias = b1_ref[...].reshape(1, MID_CH)
    gain = gain_ref[...].reshape(1, MID_CH)
    for t in range(FMAX):
        pre = lax.dot_general(
            xs_ref[:, t * cells : (t + 1) * cells], w1_ref[...], (((0,), (0,)), ((), ())), preferred_element_type=f32
        ) + bias
        inverse = lax.rsqrt(jnp.mean(pre * pre, axis=1, keepdims=True) + 1e-06)
        half = 0.5 * (pre * inverse * gain)
        lay_out(h_ref, t, jnp.where(outside, 0.0, half + half * jnp.tanh(half)))
    own = slice(W, W + tile)
    kept = [fc_ref[1].astype(f32)] + [h_ref[1, t, own, 0:MID_CH].astype(f32) for t in range(FMAX)]
    for j in range(2):
        fn_ref[j] = jnp.where(live == 1, kept[j], jnp.where(live == 2, kept[j + 1], kept[j + 2])).astype(bf16)
    fold, member = spread_of_cells()
    latest = []
    for j in range(2):
        frames = [xt[:, f * per_frame + 2 * W : f * per_frame + 2 * W + tile] for f in range(j + 1, j + 4)]
        chosen = jnp.where(live == 1, frames[0], jnp.where(live == 2, frames[1], frames[2]))
        latest = latest + [chosen[:, y * W : (y + 1) * W] for y in range(ROWS_DEV)]
    wide = lax.dot_general(
        jnp.concatenate(latest, axis=0).astype(bf16), fold, (((1,), (1,)), ((), ())), preferred_element_type=f32
    ).reshape(2 * ROWS_DEV, LAT_CH, W * LAT_CH)
    ln_ref[...] = jnp.sum(jnp.where(member[None], wide, 0.0), axis=1).reshape(2, ROWS_DEV, W * LAT_CH).astype(bf16)
    block = tile
    source = lax.broadcasted_iota(jnp.int32, (block, block), 0)
    target = lax.broadcasted_iota(jnp.int32, (block, block), 1)
    parity, line, cell = source // (2 * W), source // W % 2, source % W
    weave = (target == line * 2 * W + cell * 2 + parity).astype(bf16)
    bias2 = jnp.transpose(jnp.broadcast_to(b2_ref[...].reshape(1, OUT_CH), (8, OUT_CH)))[:, 0:1]
    for copy in large:
        copy.wait()
    started = {0, 1}
    done = []
    for frame in range(FMAX):
        for px in range(2):
            times = tuple(range(2, frame - 1, -1))
            add_products(sums_ref, h_ref, upper_ref, middle_ref, lower_ref, px, frame, frame, 3 - frame, times, started)
        started = {0, 1, 2}
        t = frame
        ready = [[jnp.where(t < live, sums_ref[t, px, py] + bias2, 0.0).astype(bf16) for py in range(2)] for px in range(2)]
        for py in range(2):
            for pair in range(ROWS_DEV // 2):
                part = slice(pair * 2 * W, (pair + 1) * 2 * W)
                joined = jnp.concatenate([ready[0][py][:, part], ready[1][py][:, part]], axis=1)
                woven = jnp.dot(joined, weave, preferred_element_type=f32).astype(bf16)
                for line in range(2):
                    frames_ref[t, 2 * (2 * pair + line) + py] = woven[:, line * 2 * W : (line + 1) * 2 * W]
        done.append(pltpu.make_async_copy(frames_ref.at[t], out_hbm.at[t], out_sem.at[t]))
        done[-1].start()
    for copy in done:
        copy.wait()


def decode(devices, assign, counts, gathered, first_weight, first_bias, norm_gain, feature_cache, second_bias):
    per_group = devices // REQS
    cells = (ROWS_DEV + 2) * W
    vm, hbm = pl.BlockSpec(memory_space=pltpu.VMEM), pl.BlockSpec(memory_space=pl.ANY)
    sm = pl.BlockSpec(memory_space=pltpu.SMEM)
    f32, bf16 = jnp.float32, jnp.bfloat16
    frames, latents, features = pl.pallas_call(
        functools.partial(decode_kernel, per_group, "seq"),
        out_shape=(
            jax.ShapeDtypeStruct((FMAX, 2 * ROWS_DEV, OUT_CH, 2 * W), bf16),
            jax.ShapeDtypeStruct((2, ROWS_DEV, W * LAT_CH), bf16),
            jax.ShapeDtypeStruct((2, ROWS_DEV * W, MID_CH), bf16),
        ),
        in_specs=[sm, sm, vm] + [hbm] * 9,
        out_specs=(hbm, vm, vm),
        scratch_shapes=[
            pltpu.VMEM((27 * LAT_CH, MID_CH), bf16),
            pltpu.VMEM((MID_CH,), f32),
            pltpu.VMEM((MID_CH,), f32),
            pltpu.VMEM((2, ROWS_DEV * W, MID_CH), bf16),
            pltpu.VMEM((2, 3, OUT_CH, 2 * MID_CH), bf16),
            pltpu.VMEM((2, 3, 2 * OUT_CH, 2 * MID_CH), bf16),
            pltpu.VMEM((2, 3, OUT_CH, 2 * MID_CH), bf16),
            pltpu.VMEM((FMAX, 2, 2, OUT_CH, ROWS_DEV * W), f32),
            pltpu.VMEM((OUT_CH,), f32),
            pltpu.VMEM((27 * LAT_CH, FMAX * cells), bf16),
            pltpu.VMEM((2, FMAX, cells, 2 * MID_CH), bf16),
            pltpu.VMEM((FMAX, 2 * ROWS_DEV, OUT_CH, 2 * W), bf16),
            pltpu.SemaphoreType.DMA((25,)),
            pltpu.SemaphoreType.DMA((FMAX,)),
        ],
        compiler_params=pltpu.CompilerParams(vmem_limit_bytes=56 * 1024 * 1024),
        cost_estimate=pl.CostEstimate(flops=4_500_000_000, bytes_accessed=11_000_000, transcendentals=442368),
    )(
        assign, counts, gathered[0], first_weight.reshape(27 * LAT_CH, MID_CH), first_bias, norm_gain,
        feature_cache.reshape(2, ROWS_DEV * W, MID_CH), *gathered[1:], second_bias,
    )
    return jnp.swapaxes(frames, 2, 3), latents, features.reshape(2, ROWS_DEV, W, MID_CH)


def body(
    latents,
    layout,
    assign,
    counts,
    latent_cache,
    feature_cache,
    first_weight,
    first_bias,
    norm_gain,
    second_weight,
    second_bias,
):
    devices = lax.axis_size("seq")
    gathered = gather(devices, assign, layout, latents, latent_cache, feature_cache, second_weight)
    return decode(devices, assign, counts, gathered, first_weight, first_bias, norm_gain, feature_cache, second_bias)


def solution(mesh):
    return jax.shard_map(
        body,
        mesh=mesh,
        in_specs=(
            P(None, ("rep", "seq")),
            P("rep", None),
            P("rep"),
            P("rep"),
            P(None, ("rep", "seq"), None),
            P(None, ("rep", "seq"), None, None),
            P(),
            P(),
            P(),
            P(),
            P(),
        ),
        out_specs=(
            P(None, ("rep", "seq"), None, None),
            P(None, ("rep", "seq"), None),
            P(None, ("rep", "seq"), None, None),
        ),
        check_vma=False,
    )
```

```python
import functools

import jax
import jax.numpy as jnp
from jax import lax
from jax.experimental import pallas as pl
from jax.experimental.pallas import tpu as pltpu
from jax.sharding import PartitionSpec as P

LAT_CH = 16
MID_CH = 384
OUT_CH = 192
REQS = 8
FMAX = 3
ROWS_DEV = 4
W = 64


def spread_of_cells():
    lane = lax.broadcasted_iota(jnp.int32, (W * LAT_CH, W), 0)
    cell = lax.broadcasted_iota(jnp.int32, (W * LAT_CH, W), 1)
    fold = (lane // LAT_CH == cell).astype(jnp.bfloat16)
    channel = lax.broadcasted_iota(jnp.int32, (LAT_CH, W * LAT_CH), 0)
    member = lax.broadcasted_iota(jnp.int32, (LAT_CH, W * LAT_CH), 1) % LAT_CH == channel
    return fold, member


def rows_outside(position, last):
    cells = (ROWS_DEV + 2) * W
    row = lax.broadcasted_iota(jnp.int32, (cells, MID_CH), 0)
    above = jnp.logical_and(row < W, position == 0)
    return jnp.logical_or(above, jnp.logical_and(row >= cells - W, position == last))


def lay_out(target, frame, values):
    cells = values.shape[0]
    column = lax.broadcasted_iota(jnp.int32, values.shape, 0) % W
    before = jnp.where(column == 0, 0.0, pltpu.roll(values, 1, 0)).astype(jnp.bfloat16)
    after = jnp.where(column == W - 1, 0.0, pltpu.roll(values, cells - 1, 0)).astype(jnp.bfloat16)
    here = values.astype(jnp.bfloat16)
    target[0, frame, :, 0:MID_CH] = before
    target[0, frame, :, MID_CH : 2 * MID_CH] = here
    target[1, frame, :, 0:MID_CH] = here
    target[1, frame, :, MID_CH : 2 * MID_CH] = after


def combine_taps(weight, upper, middle, lower):
    near = (((0,), (1, 2)), ((0, 1), (2,)))

    @pl.loop(0, 3)
    def _(a):
        base = a * 9
        tap = [[weight[base + b * 3 + e].astype(jnp.float32) for e in range(3)] for b in range(3)]
        for target, start, py, dy in ((upper, 0, 0, 0), (middle, 0, 0, 1), (middle, OUT_CH, 1, 0), (lower, 0, 1, 1)):
            taps = [sum(tap[b][e] for b in near[py][dy]) for e in range(3)]
            for px in range(2):
                for dx in range(2):
                    total = sum(taps[e] for e in near[px][dx]).astype(jnp.bfloat16)
                    target[px, a, start : start + OUT_CH, dx * MID_CH : (dx + 1) * MID_CH] = total


def add_products(sums, features, upper, middle, lower, px, frame, a, count, times, started):
    block = ROWS_DEV * W
    begun = set()
    for r, weights in enumerate((middle, upper, lower)):
        row = (1, 0, 2)[r]
        right = features[px, frame, row * W : row * W + block, :]
        left = weights[px, a : a + count]
        height = left.shape[1]
        part = lax.dot_general(
            left.reshape(count * height, left.shape[2]), right, (((1,), (1,)), ((), ())), preferred_element_type=jnp.float32
        )
        for i, t in enumerate(times):
            for py in ((0, 1), (0,), (1,))[r]:
                at = i * height + (py * OUT_CH if r == 0 else 0)
                piece = part[at : at + OUT_CH]
                if r == 0 and t not in started:
                    sums[t, px, py] = piece
                else:
                    sums[t, px, py] = sums[t, px, py] + piece


def counted_before(marks, earlier):
    size = earlier.shape[0]
    carry = jnp.zeros((marks.shape[0], 1), jnp.float32)
    parts = []
    for start in range(0, marks.shape[1], size):
        block = marks[:, start : start + size]
        parts.append(jnp.dot(block.astype(jnp.bfloat16), earlier, preferred_element_type=jnp.float32) + carry)
        carry = carry + jnp.sum(block, axis=1, keepdims=True)
    return jnp.concatenate(parts, axis=1)


def gather_kernel(
    devices, assign_ref, layout_hbm, latents_hbm, cache_hbm, features_hbm, weight_hbm,
    window_ref, upper_ref, middle_ref, lower_ref, part_ref,
    layout_ref, latents_ref, cache_ref, features_ref, weight_ref, above_ref, below_ref,
    small_ref, load_sem,
    send1_ref, recv1_ref, send2_ref, recv2_ref, upper_table, table_ref, lower_table, rim_out_ref, rim_in_ref,
    plane_ok, far_ok, s1, r1, s2, r2, sf, rf, sh, rh,
):
    f32, bf16, i32 = jnp.float32, jnp.bfloat16, jnp.int32
    per_group = devices // REQS
    plane = per_group // 2
    planes = devices // plane
    tile = ROWS_DEV * W
    tile_cells = FMAX * tile
    per_peer = tile_cells // devices
    rep, me = lax.axis_index("rep"), lax.axis_index("seq")
    z, p = me // plane, me % plane
    even = p % 2 == 0
    ahead, behind = (me + 1) % devices, (me + devices - 1) % devices
    first, final = p == 0, p == plane - 1

    def signal(semaphore, device):
        pl.semaphore_signal(semaphore, inc=1, device_id=(rep, device), device_id_type=pl.DeviceIdType.MESH)

    loads = [
        pltpu.make_async_copy(source, target, load_sem.at[i])
        for i, (source, target) in enumerate((
            (layout_hbm, layout_ref), (latents_hbm, latents_ref), (cache_hbm, cache_ref), (features_hbm, features_ref),
        ))
    ]
    loads = loads + [
        pltpu.make_async_copy(weight_hbm.at[3 * i : 3 * i + 3], weight_ref.at[3 * i : 3 * i + 3], load_sem.at[4 + i])
        for i in range(9)
    ]
    for copy in loads:
        copy.start()

    barrier = pltpu.get_barrier_semaphore()
    for q in range(0, plane, 2):
        @pl.when(p != q)
        def _():
            signal(barrier, z * plane + q)
    for i in range(1, planes):
        signal(barrier, ((z + i) % planes) * plane + (p // 2) * 2 + 1)

    @pl.when(final)
    def _():
        signal(barrier, ahead)

    @pl.when(first)
    def _():
        signal(barrier, behind)

    row_of = lax.broadcasted_iota(i32, (tile_cells // 3, tile_cells // 3), 0)
    lane_of = lax.broadcasted_iota(i32, (tile_cells // 3, tile_cells // 3), 1)
    earlier = (row_of < lane_of).astype(bf16)
    loads[0].wait()
    own = layout_ref[pl.ds(me, 1), :]
    request = ((own // (ROWS_DEV * per_group * W)) * 43) // 128
    group = jnp.zeros_like(own)
    for g in range(REQS):
        group = group + jnp.where(assign_ref[g] == request, g, 0)
    place = group * per_group + (own // tile) % per_group
    target = (place + devices - per_group // 2) % devices
    line = (target % plane) * planes + target // plane
    hit = lax.broadcasted_iota(i32, (devices, tile_cells), 0) == line
    marks = hit.astype(f32)
    order = counted_before(marks, earlier)
    loads[1].wait()
    latents = latents_ref[...]
    rows = []
    for k in range(per_peer):
        chosen = jnp.where(order == k, marks, 0.0).astype(bf16)
        rows.append(lax.dot_general(latents, chosen, (((1,), (1,)), ((), ())), preferred_element_type=f32))
    rows.append(jnp.zeros((devices - per_peer * LAT_CH, devices), f32))
    sent = jnp.transpose(jnp.concatenate(rows, axis=0)).reshape(plane, planes, devices)
    for q in range(plane):
        send1_ref[q, 0] = (sent[q - 1] if q > 0 else pltpu.roll(sent[plane - 1], 1, 0)).astype(bf16)
        send1_ref[q, 1] = sent[q].astype(bf16)
        send1_ref[q, 2] = (sent[q + 1] if q < plane - 1 else pltpu.roll(sent[0], planes - 1, 0)).astype(bf16)

    @pl.when(even)
    def _():
        pl.semaphore_wait(barrier, plane - 1 + jnp.where(first, 1, 0))
        signal(plane_ok, me + 1)

    @pl.when(jnp.logical_not(even))
    def _():
        pl.semaphore_wait(plane_ok, 1)

    near = []
    for i in range(1, plane):
        q = (p + i) % plane
        near.append(pltpu.make_async_remote_copy(
            src_ref=send1_ref.at[q], dst_ref=recv1_ref.at[p], send_sem=s1.at[i], recv_sem=r1.at[i],
            device_id=(rep, z * plane + q), device_id_type=pl.DeviceIdType.MESH))
        near[-1].start()
    recv1_ref[p] = send1_ref[p]

    my_place = (me + per_group // 2) % devices
    my_group, position = my_place // per_group, my_place % per_group
    frame = ROWS_DEV * per_group * W
    half = tile // 2
    for side, table in enumerate((upper_table, table_ref, lower_table)):
        other = (my_place + side - 1 + devices) % devices
        start = assign_ref[other // per_group] * (FMAX * frame) + (other % per_group) * tile
        offset = layout_ref[...] - start
        inside = jnp.logical_and(jnp.logical_and(offset >= 0, offset < FMAX * frame), (offset & (frame - tile)) == 0)
        inner = offset & (tile - 1)
        if side == 0:
            within = jnp.where(inner >= half, (offset // frame) * half + inner - half, -1)
        elif side == 1:
            within = (offset // frame) * tile + inner
        else:
            within = jnp.where(inner < half, (offset // frame) * half + inner, -1)
        within = within.astype(f32)
        order = counted_before(inside.astype(f32), earlier)
        spot = lax.broadcasted_iota(i32, (devices, table.shape[1]), 1).astype(f32)
        for k in range(per_peer):
            chosen = jnp.logical_and(order == k, inside)
            home = jnp.sum(jnp.where(chosen, within, 0.0), axis=1, keepdims=True)
            table[k * devices : (k + 1) * devices, :] = (home == spot).astype(bf16)

    for copy in near:
        copy.wait()
    to = lax.broadcasted_iota(i32, (devices, devices), 0)
    source = lax.broadcasted_iota(i32, (devices, devices), 1)
    turn = (source == (to % plane) * planes + to // plane).astype(bf16)
    for side in range(3):
        turned = jnp.dot(turn, recv1_ref[:, side].reshape(devices, devices), preferred_element_type=f32)
        send2_ref[:, side] = turned.reshape(planes, plane, devices).astype(bf16)

    @pl.when(jnp.logical_not(even))
    def _():
        pl.semaphore_wait(barrier, 2 * (planes - 1) + jnp.where(final, 1, 0))
        signal(far_ok, me - 1)

    @pl.when(even)
    def _():
        pl.semaphore_wait(far_ok, 1)

    far = []
    for i in range(1, planes):
        q = (z + i) % planes
        far.append(pltpu.make_async_remote_copy(
            src_ref=send2_ref.at[q], dst_ref=recv2_ref.at[z], send_sem=s2.at[i], recv_sem=r2.at[i],
            device_id=(rep, q * plane + p), device_id_type=pl.DeviceIdType.MESH))
        far[-1].start()
    recv2_ref[z] = send2_ref[z]
    loads[3].wait()
    sides = []
    for side in range(2):
        sides.append(pltpu.make_async_remote_copy(
            src_ref=features_ref.at[:, pl.ds((ROWS_DEV - 1) * W * (1 - side), W)],
            dst_ref=(above_ref, below_ref)[side],
            send_sem=sf.at[side], recv_sem=rf.at[side],
            device_id=(rep, (ahead, behind)[side]), device_id_type=pl.DeviceIdType.MESH))
        sides[-1].start()

    loads[2].wait()
    wide = cache_ref[...].astype(f32).reshape(2 * ROWS_DEV, W * LAT_CH)
    fold, member = spread_of_cells()
    stacked = jnp.concatenate([
        jnp.where(member, jnp.broadcast_to(wide[i : i + 1], member.shape), 0.0) for i in range(2 * ROWS_DEV)
    ], axis=0).astype(bf16)
    folded = jnp.dot(stacked, fold, preferred_element_type=f32)
    cached = jnp.concatenate([folded[i * LAT_CH : (i + 1) * LAT_CH] for i in range(2 * ROWS_DEV)], axis=1).astype(bf16)

    rim = 2 * W
    for f in range(2):
        rim_out_ref[0, f] = cached[:, (f + 1) * tile - rim : (f + 1) * tile]
        rim_out_ref[1, f] = cached[:, f * tile : f * tile + rim]
    edges = []
    for side in range(2):
        edges.append(pltpu.make_async_remote_copy(
            src_ref=rim_out_ref.at[side], dst_ref=rim_in_ref.at[side],
            send_sem=sh.at[side], recv_sem=rh.at[side],
            device_id=(rep, (ahead, behind)[side]), device_id_type=pl.DeviceIdType.MESH))
        edges[-1].start()

    for copy in loads[4:]:
        copy.wait()
    combine_taps(weight_ref, upper_ref, middle_ref, lower_ref)

    for copy in sides:
        copy.wait()
    for copy in edges:
        copy.wait_recv()
    outside = rows_outside(position, per_group - 1)
    for f in range(2):
        values = jnp.concatenate([above_ref[f], features_ref[f], below_ref[f]], axis=0).astype(f32)
        lay_out(small_ref, f, jnp.where(outside, 0.0, values))
    for px in range(2):
        add_products(part_ref, small_ref, upper_ref, middle_ref, lower_ref, px, 1, 0, 2, (1, 0), {})
        add_products(part_ref, small_ref, upper_ref, middle_ref, lower_ref, px, 0, 0, 1, (0,), {0})
    for copy in far:
        copy.wait()
    found = []
    for side, table in enumerate((upper_table, table_ref, lower_table)):
        arrived = jnp.transpose(recv2_ref[:, side].astype(f32).reshape(devices, devices))
        arrived = jnp.concatenate([arrived[k * LAT_CH : (k + 1) * LAT_CH] for k in range(per_peer)], axis=1)
        found.append(jnp.dot(arrived.astype(bf16), table[...], preferred_element_type=f32))
    nothing = jnp.zeros((LAT_CH, rim), f32)
    for f in range(2 + FMAX):
        if f < 2:
            top, here, bottom = rim_in_ref[0, f].astype(f32), cached[:, f * tile : (f + 1) * tile], rim_in_ref[1, f].astype(f32)
        else:
            t = f - 2
            top, bottom = (found[side][:, t * rim : (t + 1) * rim] for side in (0, 2))
            here = found[1][:, t * tile : (t + 1) * tile].astype(bf16)
        at = f * (tile + 2 * rim)
        window_ref[:, at : at + rim] = jnp.where(position == 0, nothing, top).astype(bf16)
        window_ref[:, at + rim : at + rim + tile] = here
        window_ref[:, at + rim + tile : at + 2 * rim + tile] = jnp.where(position == per_group - 1, nothing, bottom).astype(bf16)
    for copy in edges:
        copy.wait_send()


def gather(devices, assign, layout, latents, latent_cache, feature_cache, second_weight):
    plane = devices // REQS // 2
    planes = devices // plane
    cells = FMAX * ROWS_DEV * W
    vm, hbm = pl.BlockSpec(memory_space=pltpu.VMEM), pl.BlockSpec(memory_space=pltpu.HBM)
    bf16, dma = jnp.bfloat16, pltpu.SemaphoreType.DMA
    return pl.pallas_call(
        functools.partial(gather_kernel, devices),
        out_shape=(
            jax.ShapeDtypeStruct((LAT_CH, (2 + FMAX) * (ROWS_DEV + 4) * W), bf16),
            jax.ShapeDtypeStruct((2, 3, OUT_CH, 2 * MID_CH), bf16),
            jax.ShapeDtypeStruct((2, 3, 2 * OUT_CH, 2 * MID_CH), bf16),
            jax.ShapeDtypeStruct((2, 3, OUT_CH, 2 * MID_CH), bf16),
            jax.ShapeDtypeStruct((2, 2, 2, OUT_CH, ROWS_DEV * W), jnp.float32),
        ),
        in_specs=[pl.BlockSpec(memory_space=pltpu.SMEM), hbm, hbm, hbm, hbm, hbm],
        out_specs=(vm, vm, vm, vm, vm),
        scratch_shapes=[
            pltpu.VMEM((devices, cells), jnp.int32),
            pltpu.VMEM((LAT_CH, cells), bf16),
            pltpu.VMEM((2, ROWS_DEV, W * LAT_CH), bf16),
            pltpu.VMEM((2, ROWS_DEV * W, MID_CH), bf16),
            pltpu.VMEM((27, OUT_CH, MID_CH), bf16),
            pltpu.VMEM((2, W, MID_CH), bf16),
            pltpu.VMEM((2, W, MID_CH), bf16),
            pltpu.VMEM((2, 2, (ROWS_DEV + 2) * W, 2 * MID_CH), bf16),
            dma((13,)),
            pltpu.VMEM((plane, 3, planes, devices), bf16),
            pltpu.VMEM((plane, 3, planes, devices), bf16),
            pltpu.VMEM((planes, 3, plane, devices), bf16),
            pltpu.VMEM((planes, 3, plane, devices), bf16),
            pltpu.VMEM((cells, cells // 2), bf16),
            pltpu.VMEM((cells, cells), bf16),
            pltpu.VMEM((cells, cells // 2), bf16),
            pltpu.VMEM((2, 2, LAT_CH, 2 * W), bf16),
            pltpu.VMEM((2, 2, LAT_CH, 2 * W), bf16),
            pltpu.SemaphoreType.REGULAR,
            pltpu.SemaphoreType.REGULAR,
            dma((plane,)), dma((plane,)), dma((planes,)), dma((planes,)),
            dma((2,)), dma((2,)), dma((2,)), dma((2,)),
        ],
        compiler_params=pltpu.CompilerParams(collective_id=0, has_side_effects=True, vmem_limit_bytes=28 * 1024 * 1024),
        cost_estimate=pl.CostEstimate(flops=3_000_000_000, bytes_accessed=13_000_000, transcendentals=0),
    )(
        *(pltpu.with_memory_space_constraint(x, pltpu.HBM) for x in (
            assign,
            layout,
            latents,
            latent_cache,
            feature_cache.reshape(2, ROWS_DEV * W, MID_CH),
            jnp.swapaxes(second_weight, 3, 4).reshape(27, OUT_CH, MID_CH),
        )),
    )


def decode_kernel(
    per_group, place_axis, assign_ref, counts_ref, window_ref, w1_hbm, b1_hbm, gain_hbm, fc_hbm, upper_ref, middle_ref, lower_ref,
    part_ref, b2_hbm,
    out_hbm, ln_ref, fn_ref,
    w1_ref, b1_ref, gain_ref, fc_ref, sums_ref, b2_ref, xs_ref, h_ref, frames_ref,
    load_sem, out_sem,
):
    f32, bf16 = jnp.float32, jnp.bfloat16
    place = (lax.axis_index(place_axis) + per_group // 2) % (per_group * REQS)
    position = place % per_group
    live = counts_ref[assign_ref[place // per_group]]
    small = [
        pltpu.make_async_copy(source, target, load_sem.at[i])
        for i, (source, target) in enumerate((
            (w1_hbm, w1_ref), (b1_hbm, b1_ref), (gain_hbm, gain_ref), (b2_hbm, b2_ref), (fc_hbm, fc_ref),
        ))
    ]
    for copy in small:
        copy.start()
    rows = ROWS_DEV + 2
    cells, tile = rows * W, ROWS_DEV * W
    per_frame = (ROWS_DEV + 4) * W
    xt = window_ref[...].astype(f32)
    lanes = xt.shape[1]
    column = lax.broadcasted_iota(jnp.int32, xt.shape, 1) % W
    shifted = (
        jnp.where(column == 0, 0.0, pltpu.roll(xt, 1, 1)),
        xt,
        jnp.where(column == W - 1, 0.0, pltpu.roll(xt, lanes - 1, 1)),
    )
    for e in range(3):
        odd = pltpu.roll(shifted[e], lanes - W, 1).astype(bf16)
        even = shifted[e].astype(bf16)
        for b in range(3):
            source, start = ((even, 0), (odd, 0), (even, 2 * W))[b]
            for a in range(3):
                k = ((a * 3 + b) * 3 + e) * LAT_CH
                for t in range(FMAX):
                    at = (t + a) * per_frame + start
                    xs_ref[k : k + LAT_CH, t * cells : (t + 1) * cells] = source[:, at : at + cells]
    outside = rows_outside(position, per_group - 1)
    for copy in small:
        copy.wait()
    bias = b1_ref[...].reshape(1, MID_CH)
    gain = gain_ref[...].reshape(1, MID_CH)
    for t in range(FMAX):
        pre = lax.dot_general(
            xs_ref[:, t * cells : (t + 1) * cells], w1_ref[...], (((0,), (0,)), ((), ())), preferred_element_type=f32
        ) + bias
        inverse = lax.rsqrt(jnp.mean(pre * pre, axis=1, keepdims=True) + 1e-06)
        half = 0.5 * (pre * inverse * gain)
        lay_out(h_ref, t, jnp.where(outside, 0.0, half + half * jnp.tanh(half)))
    own = slice(W, W + tile)
    kept = [fc_ref[1].astype(f32)] + [h_ref[1, t, own, 0:MID_CH].astype(f32) for t in range(FMAX)]
    for j in range(2):
        fn_ref[j] = jnp.where(live == 1, kept[j], jnp.where(live == 2, kept[j + 1], kept[j + 2])).astype(bf16)
    fold, member = spread_of_cells()
    latest = []
    for j in range(2):
        frames = [xt[:, f * per_frame + 2 * W : f * per_frame + 2 * W + tile] for f in range(j + 1, j + 4)]
        chosen = jnp.where(live == 1, frames[0], jnp.where(live == 2, frames[1], frames[2]))
        latest = latest + [chosen[:, y * W : (y + 1) * W] for y in range(ROWS_DEV)]
    wide = lax.dot_general(
        jnp.concatenate(latest, axis=0).astype(bf16), fold, (((1,), (1,)), ((), ())), preferred_element_type=f32
    ).reshape(2 * ROWS_DEV, LAT_CH, W * LAT_CH)
    ln_ref[...] = jnp.sum(jnp.where(member[None], wide, 0.0), axis=1).reshape(2, ROWS_DEV, W * LAT_CH).astype(bf16)
    block = tile
    source = lax.broadcasted_iota(jnp.int32, (block, block), 0)
    target = lax.broadcasted_iota(jnp.int32, (block, block), 1)
    parity, line, cell = source // (2 * W), source // W % 2, source % W
    weave = (target == line * 2 * W + cell * 2 + parity).astype(bf16)
    bias2 = jnp.transpose(jnp.broadcast_to(b2_ref[...].reshape(1, OUT_CH), (8, OUT_CH)))[:, 0:1]
    started = set()
    done = []
    for frame in range(FMAX):
        for px in range(2):
            times = tuple(range(2, frame - 1, -1))
            add_products(sums_ref, h_ref, upper_ref, middle_ref, lower_ref, px, frame, frame, 3 - frame, times, started)
        started = {0, 1, 2}
        t = frame
        ready = []
        for px in range(2):
            total = [sums_ref[t, px, py] + (part_ref[t, px, py] if t < 2 else 0.0) + bias2 for py in range(2)]
            ready.append([jnp.where(t < live, one, 0.0).astype(bf16) for one in total])
        for py in range(2):
            for pair in range(ROWS_DEV // 2):
                part = slice(pair * 2 * W, (pair + 1) * 2 * W)
                joined = jnp.concatenate([ready[0][py][:, part], ready[1][py][:, part]], axis=1)
                woven = jnp.dot(joined, weave, preferred_element_type=f32).astype(bf16)
                for line in range(2):
                    frames_ref[t, 2 * (2 * pair + line) + py] = woven[:, line * 2 * W : (line + 1) * 2 * W]
        done.append(pltpu.make_async_copy(frames_ref.at[t], out_hbm.at[t], out_sem.at[t]))
        done[-1].start()
    for copy in done:
        copy.wait()


def decode(devices, assign, counts, gathered, first_weight, first_bias, norm_gain, feature_cache, second_bias):
    per_group = devices // REQS
    cells = (ROWS_DEV + 2) * W
    vm, hbm = pl.BlockSpec(memory_space=pltpu.VMEM), pl.BlockSpec(memory_space=pltpu.HBM)
    sm = pl.BlockSpec(memory_space=pltpu.SMEM)
    f32, bf16 = jnp.float32, jnp.bfloat16
    frames, latents, features = pl.pallas_call(
        functools.partial(decode_kernel, per_group, "seq"),
        out_shape=(
            jax.ShapeDtypeStruct((FMAX, 2 * ROWS_DEV, OUT_CH, 2 * W), bf16),
            jax.ShapeDtypeStruct((2, ROWS_DEV, W * LAT_CH), bf16),
            jax.ShapeDtypeStruct((2, ROWS_DEV * W, MID_CH), bf16),
        ),
        in_specs=[sm, sm, vm] + [hbm] * 4 + [vm] * 4 + [hbm],
        out_specs=(hbm, vm, vm),
        scratch_shapes=[
            pltpu.VMEM((27 * LAT_CH, MID_CH), bf16),
            pltpu.VMEM((MID_CH,), f32),
            pltpu.VMEM((MID_CH,), f32),
            pltpu.VMEM((2, ROWS_DEV * W, MID_CH), bf16),
            pltpu.VMEM((FMAX, 2, 2, OUT_CH, ROWS_DEV * W), f32),
            pltpu.VMEM((OUT_CH,), f32),
            pltpu.VMEM((27 * LAT_CH, FMAX * cells), bf16),
            pltpu.VMEM((2, FMAX, cells, 2 * MID_CH), bf16),
            pltpu.VMEM((FMAX, 2 * ROWS_DEV, OUT_CH, 2 * W), bf16),
            pltpu.SemaphoreType.DMA((5,)),
            pltpu.SemaphoreType.DMA((FMAX,)),
        ],
        compiler_params=pltpu.CompilerParams(vmem_limit_bytes=28 * 1024 * 1024),
        cost_estimate=pl.CostEstimate(flops=4_500_000_000, bytes_accessed=11_000_000, transcendentals=442368),
    )(
        assign, counts, gathered[0], first_weight.reshape(27 * LAT_CH, MID_CH), first_bias, norm_gain,
        feature_cache.reshape(2, ROWS_DEV * W, MID_CH), *gathered[1:], second_bias,
    )
    return jnp.swapaxes(frames, 2, 3), latents, features.reshape(2, ROWS_DEV, W, MID_CH)


def body(
    latents,
    layout,
    assign,
    counts,
    latent_cache,
    feature_cache,
    first_weight,
    first_bias,
    norm_gain,
    second_weight,
    second_bias,
):
    devices = lax.axis_size("seq")
    gathered = gather(devices, assign, layout, latents, latent_cache, feature_cache, second_weight)
    return decode(devices, assign, counts, gathered, first_weight, first_bias, norm_gain, feature_cache, second_bias)


def solution(mesh):
    return jax.shard_map(
        body,
        mesh=mesh,
        in_specs=(
            P(None, ("rep", "seq")),
            P("rep", None),
            P("rep"),
            P("rep"),
            P(None, ("rep", "seq"), None),
            P(None, ("rep", "seq"), None, None),
            P(),
            P(),
            P(),
            P(),
            P(),
        ),
        out_specs=(
            P(None, ("rep", "seq"), None, None),
            P(None, ("rep", "seq"), None),
            P(None, ("rep", "seq"), None, None),
        ),
        check_vma=False,
    )
```

```python
import functools

import jax
import jax.numpy as jnp
from jax import lax
from jax.experimental import pallas as pl
from jax.experimental.pallas import tpu as pltpu
from jax.sharding import PartitionSpec as P

LAT_CH = 16
MID_CH = 384
OUT_CH = 192
REQS = 8
FMAX = 3
ROWS_DEV = 4
W = 64


def spread_of_cells():
    lane = lax.broadcasted_iota(jnp.int32, (W * LAT_CH, W), 0)
    cell = lax.broadcasted_iota(jnp.int32, (W * LAT_CH, W), 1)
    fold = (lane // LAT_CH == cell).astype(jnp.bfloat16)
    channel = lax.broadcasted_iota(jnp.int32, (LAT_CH, W * LAT_CH), 0)
    member = lax.broadcasted_iota(jnp.int32, (LAT_CH, W * LAT_CH), 1) % LAT_CH == channel
    return fold, member


def rows_outside(position, last):
    cells = (ROWS_DEV + 2) * W
    row = lax.broadcasted_iota(jnp.int32, (cells, MID_CH), 0)
    above = jnp.logical_and(row < W, position == 0)
    return jnp.logical_or(above, jnp.logical_and(row >= cells - W, position == last))


def lay_out(target, frame, values):
    cells = values.shape[0]
    column = lax.broadcasted_iota(jnp.int32, values.shape, 0) % W
    before = jnp.where(column == 0, 0.0, pltpu.roll(values, 1, 0)).astype(jnp.bfloat16)
    after = jnp.where(column == W - 1, 0.0, pltpu.roll(values, cells - 1, 0)).astype(jnp.bfloat16)
    here = values.astype(jnp.bfloat16)
    target[0, frame, :, 0:MID_CH] = before
    target[0, frame, :, MID_CH : 2 * MID_CH] = here
    target[1, frame, :, 0:MID_CH] = here
    target[1, frame, :, MID_CH : 2 * MID_CH] = after


def combine_taps(weight, upper, middle, lower):
    near = (((0,), (1, 2)), ((0, 1), (2,)))

    @pl.loop(0, 3)
    def _(a):
        base = a * 9
        tap = [[weight[base + b * 3 + e].astype(jnp.float32) for e in range(3)] for b in range(3)]
        for target, start, py, dy in ((upper, 0, 0, 0), (middle, 0, 0, 1), (middle, OUT_CH, 1, 0), (lower, 0, 1, 1)):
            taps = [sum(tap[b][e] for b in near[py][dy]) for e in range(3)]
            for px in range(2):
                for dx in range(2):
                    total = sum(taps[e] for e in near[px][dx]).astype(jnp.bfloat16)
                    target[px, a, start : start + OUT_CH, dx * MID_CH : (dx + 1) * MID_CH] = total


def add_products(sums, features, upper, middle, lower, px, frame, a, count, times, started, parts=(0, 1, 2)):
    block = ROWS_DEV * W
    for r in parts:
        weights = (middle, upper, lower)[r]
        row = (1, 0, 2)[r]
        right = features[px, frame, row * W : row * W + block, :]
        left = weights[px, a : a + count]
        height = left.shape[1]
        part = lax.dot_general(
            left.reshape(count * height, left.shape[2]), right, (((1,), (1,)), ((), ())), preferred_element_type=jnp.float32
        )
        for i, t in enumerate(times):
            for py in ((0, 1), (0,), (1,))[r]:
                at = i * height + (py * OUT_CH if r == 0 else 0)
                piece = part[at : at + OUT_CH]
                if r == 0 and t not in started:
                    sums[t, px, py] = piece
                else:
                    sums[t, px, py] = sums[t, px, py] + piece


def counted_before(marks, earlier):
    size = earlier.shape[0]
    carry = jnp.zeros((marks.shape[0], 1), jnp.float32)
    parts = []
    for start in range(0, marks.shape[1], size):
        block = marks[:, start : start + size]
        parts.append(jnp.dot(block.astype(jnp.bfloat16), earlier, preferred_element_type=jnp.float32) + carry)
        carry = carry + jnp.sum(block, axis=1, keepdims=True)
    return jnp.concatenate(parts, axis=1)


def by_distance(ring):
    return sorted(range(1, ring), key=lambda i: (-min(i, ring - i), i))


def gather_kernel(
    devices, assign_hbm, layout_hbm, latents_hbm, cache_hbm, features_hbm, weight_hbm,
    window_ref, upper_ref, middle_ref, lower_ref, part_ref,
    assign_ref, layout_ref, latents_ref, cache_ref, features_ref, weight_ref, above_ref, below_ref,
    small_ref, load_sem,
    send1_ref, recv1_ref, send2_ref, recv2_ref, upper_table, table_ref, lower_table, rim_out_ref, rim_in_ref,
    plane_ok, far_ok, s1, r1, s2, r2, sf, rf, sh, rh,
):
    f32, bf16, i32 = jnp.float32, jnp.bfloat16, jnp.int32
    per_group = devices // REQS
    plane = per_group // 2
    planes = devices // plane
    tile = ROWS_DEV * W
    tile_cells = FMAX * tile
    per_peer = tile_cells // devices
    rep, me = lax.axis_index("rep"), lax.axis_index("seq")
    z, p = me // plane, me % plane
    even = p % 2 == 0
    ahead, behind = (me + 1) % devices, (me + devices - 1) % devices
    first, final = p == 0, p == plane - 1

    def signal(semaphore, device):
        pl.semaphore_signal(semaphore, inc=1, device_id=(rep, device), device_id_type=pl.DeviceIdType.MESH)

    loads = [
        pltpu.make_async_copy(source, target, load_sem.at[i])
        for i, (source, target) in enumerate((
            (layout_hbm, layout_ref), (assign_hbm, assign_ref), (latents_hbm, latents_ref), (cache_hbm, cache_ref), (features_hbm, features_ref),
        ))
    ]
    loads = loads + [
        pltpu.make_async_copy(weight_hbm.at[3 * i : 3 * i + 3], weight_ref.at[3 * i : 3 * i + 3], load_sem.at[5 + i])
        for i in range(9)
    ]
    for copy in loads:
        copy.start()

    barrier = pltpu.get_barrier_semaphore()
    for i in by_distance(planes):
        signal(barrier, ((z + i) % planes) * plane + (p // 2) * 2 + 1)
    for q in range(0, plane, 2):
        @pl.when(p != q)
        def _():
            signal(barrier, z * plane + q)

    @pl.when(final)
    def _():
        signal(barrier, ahead)

    @pl.when(first)
    def _():
        signal(barrier, behind)

    row_of = lax.broadcasted_iota(i32, (tile_cells // 3, tile_cells // 3), 0)
    lane_of = lax.broadcasted_iota(i32, (tile_cells // 3, tile_cells // 3), 1)
    earlier = (row_of < lane_of).astype(bf16)
    loads[0].wait()
    loads[1].wait()
    own = layout_ref[pl.ds(me, 1), :]
    request = ((own // (ROWS_DEV * per_group * W)) * 43) // 128
    group = jnp.zeros_like(own)
    for g in range(REQS):
        group = group + jnp.where(assign_ref[g] == request, g, 0)
    place = group * per_group + (own // tile) % per_group
    target = (place + devices - per_group // 2) % devices
    line = (target % plane) * planes + target // plane
    hit = lax.broadcasted_iota(i32, (devices, tile_cells), 0) == line
    marks = hit.astype(f32)
    order = counted_before(marks, earlier)
    loads[2].wait()
    latents = latents_ref[...]
    rows = []
    for k in range(per_peer):
        chosen = jnp.where(order == k, marks, 0.0).astype(bf16)
        rows.append(lax.dot_general(latents, chosen, (((1,), (1,)), ((), ())), preferred_element_type=f32))
    rows.append(jnp.zeros((devices - per_peer * LAT_CH, devices), f32))
    sent = jnp.transpose(jnp.concatenate(rows, axis=0)).reshape(plane, planes, devices)
    for q in range(plane):
        send1_ref[q, 0] = (sent[q - 1] if q > 0 else pltpu.roll(sent[plane - 1], 1, 0)).astype(bf16)
        send1_ref[q, 1] = sent[q].astype(bf16)
        send1_ref[q, 2] = (sent[q + 1] if q < plane - 1 else pltpu.roll(sent[0], planes - 1, 0)).astype(bf16)

    @pl.when(even)
    def _():
        pl.semaphore_wait(barrier, plane - 1 + jnp.where(first, 1, 0))
        signal(plane_ok, me + 1)

    @pl.when(jnp.logical_not(even))
    def _():
        pl.semaphore_wait(plane_ok, 1)

    near = []
    for i in range(1, plane):
        q = (p + i) % plane
        near.append(pltpu.make_async_remote_copy(
            src_ref=send1_ref.at[q], dst_ref=recv1_ref.at[p], send_sem=s1.at[i], recv_sem=r1.at[i],
            device_id=(rep, z * plane + q), device_id_type=pl.DeviceIdType.MESH))
        near[-1].start()
    recv1_ref[p] = send1_ref[p]

    my_place = (me + per_group // 2) % devices
    my_group, position = my_place // per_group, my_place % per_group
    frame = ROWS_DEV * per_group * W
    half = tile // 2
    for side, table in enumerate((upper_table, table_ref, lower_table)):
        other = (my_place + side - 1 + devices) % devices
        start = assign_ref[other // per_group] * (FMAX * frame) + (other % per_group) * tile
        offset = layout_ref[...] - start
        inside = jnp.logical_and(jnp.logical_and(offset >= 0, offset < FMAX * frame), (offset & (frame - tile)) == 0)
        inner = offset & (tile - 1)
        if side == 0:
            within = jnp.where(inner >= half, (offset // frame) * half + inner - half, -1)
        elif side == 1:
            within = (offset // frame) * tile + inner
        else:
            within = jnp.where(inner < half, (offset // frame) * half + inner, -1)
        within = within.astype(f32)
        order = counted_before(inside.astype(f32), earlier)
        spot = lax.broadcasted_iota(i32, (devices, table.shape[1]), 1).astype(f32)
        for k in range(per_peer):
            chosen = jnp.logical_and(order == k, inside)
            home = jnp.sum(jnp.where(chosen, within, 0.0), axis=1, keepdims=True)
            table[k * devices : (k + 1) * devices, :] = (home == spot).astype(bf16)

    for copy in near:
        copy.wait()
    to = lax.broadcasted_iota(i32, (devices, devices), 0)
    source = lax.broadcasted_iota(i32, (devices, devices), 1)
    turn = (source == (to % plane) * planes + to // plane).astype(bf16)
    for side in range(3):
        turned = jnp.dot(turn, recv1_ref[:, side].reshape(devices, devices), preferred_element_type=f32)
        send2_ref[:, side] = turned.reshape(planes, plane, devices).astype(bf16)

    @pl.when(jnp.logical_not(even))
    def _():
        pl.semaphore_wait(barrier, 2 * (planes - 1) + jnp.where(final, 1, 0))
        signal(far_ok, me - 1)

    @pl.when(even)
    def _():
        pl.semaphore_wait(far_ok, 1)

    far = []
    for i in by_distance(planes):
        q = (z + i) % planes
        far.append(pltpu.make_async_remote_copy(
            src_ref=send2_ref.at[q], dst_ref=recv2_ref.at[z], send_sem=s2.at[i], recv_sem=r2.at[i],
            device_id=(rep, q * plane + p), device_id_type=pl.DeviceIdType.MESH))
        far[-1].start()
    recv2_ref[z] = send2_ref[z]
    loads[4].wait()
    sides = []
    for side in range(2):
        sides.append(pltpu.make_async_remote_copy(
            src_ref=features_ref.at[:, pl.ds((ROWS_DEV - 1) * W * (1 - side), W)],
            dst_ref=(above_ref, below_ref)[side],
            send_sem=sf.at[side], recv_sem=rf.at[side],
            device_id=(rep, (ahead, behind)[side]), device_id_type=pl.DeviceIdType.MESH))
        sides[-1].start()

    loads[3].wait()
    wide = cache_ref[...].astype(f32).reshape(2 * ROWS_DEV, W * LAT_CH)
    fold, member = spread_of_cells()
    stacked = jnp.concatenate([
        jnp.where(member, jnp.broadcast_to(wide[i : i + 1], member.shape), 0.0) for i in range(2 * ROWS_DEV)
    ], axis=0).astype(bf16)
    folded = jnp.dot(stacked, fold, preferred_element_type=f32)
    cached = jnp.concatenate([folded[i * LAT_CH : (i + 1) * LAT_CH] for i in range(2 * ROWS_DEV)], axis=1).astype(bf16)

    rim = 2 * W
    for f in range(2):
        rim_out_ref[0, f] = cached[:, (f + 1) * tile - rim : (f + 1) * tile]
        rim_out_ref[1, f] = cached[:, f * tile : f * tile + rim]
    edges = []
    for side in range(2):
        edges.append(pltpu.make_async_remote_copy(
            src_ref=rim_out_ref.at[side], dst_ref=rim_in_ref.at[side],
            send_sem=sh.at[side], recv_sem=rh.at[side],
            device_id=(rep, (ahead, behind)[side]), device_id_type=pl.DeviceIdType.MESH))
        edges[-1].start()

    for copy in loads[5:]:
        copy.wait()
    combine_taps(weight_ref, upper_ref, middle_ref, lower_ref)

    for copy in sides:
        copy.wait()
    for copy in edges:
        copy.wait_recv()
    outside = rows_outside(position, per_group - 1)
    for f in range(2):
        values = jnp.concatenate([above_ref[f], features_ref[f], below_ref[f]], axis=0).astype(f32)
        lay_out(small_ref, f, jnp.where(outside, 0.0, values))
    for px in range(2):
        add_products(part_ref, small_ref, upper_ref, middle_ref, lower_ref, px, 1, 0, 2, (1, 0), {})
        add_products(part_ref, small_ref, upper_ref, middle_ref, lower_ref, px, 0, 0, 1, (0,), {0})
    for copy in far:
        copy.wait()
    found = []
    for side, table in enumerate((upper_table, table_ref, lower_table)):
        arrived = jnp.transpose(recv2_ref[:, side].astype(f32).reshape(devices, devices))
        arrived = jnp.concatenate([arrived[k * LAT_CH : (k + 1) * LAT_CH] for k in range(per_peer)], axis=1)
        found.append(jnp.dot(arrived.astype(bf16), table[...], preferred_element_type=f32))
    nothing = jnp.zeros((LAT_CH, rim), f32)
    for f in range(2 + FMAX):
        if f < 2:
            top, here, bottom = rim_in_ref[0, f].astype(f32), cached[:, f * tile : (f + 1) * tile], rim_in_ref[1, f].astype(f32)
        else:
            t = f - 2
            top, bottom = (found[side][:, t * rim : (t + 1) * rim] for side in (0, 2))
            here = found[1][:, t * tile : (t + 1) * tile].astype(bf16)
        at = f * (tile + 2 * rim)
        window_ref[:, at : at + rim] = jnp.where(position == 0, nothing, top).astype(bf16)
        window_ref[:, at + rim : at + rim + tile] = here
        window_ref[:, at + rim + tile : at + 2 * rim + tile] = jnp.where(position == per_group - 1, nothing, bottom).astype(bf16)
    for copy in edges:
        copy.wait_send()


def gather(devices, assign, layout, latents, latent_cache, feature_cache, second_weight):
    plane = devices // REQS // 2
    planes = devices // plane
    cells = FMAX * ROWS_DEV * W
    vm, hbm = pl.BlockSpec(memory_space=pltpu.VMEM), pl.BlockSpec(memory_space=pltpu.HBM)
    bf16, dma = jnp.bfloat16, pltpu.SemaphoreType.DMA
    return pl.pallas_call(
        functools.partial(gather_kernel, devices),
        out_shape=(
            jax.ShapeDtypeStruct((LAT_CH, (2 + FMAX) * (ROWS_DEV + 4) * W), bf16),
            jax.ShapeDtypeStruct((2, 3, OUT_CH, 2 * MID_CH), bf16),
            jax.ShapeDtypeStruct((2, 3, 2 * OUT_CH, 2 * MID_CH), bf16),
            jax.ShapeDtypeStruct((2, 3, OUT_CH, 2 * MID_CH), bf16),
            jax.ShapeDtypeStruct((2, 2, 2, OUT_CH, ROWS_DEV * W), jnp.float32),
        ),
        in_specs=[hbm] * 6,
        out_specs=(vm, vm, vm, vm, vm),
        scratch_shapes=[
            pltpu.SMEM((REQS,), jnp.int32),
            pltpu.VMEM((devices, cells), jnp.int32),
            pltpu.VMEM((LAT_CH, cells), bf16),
            pltpu.VMEM((2, ROWS_DEV, W * LAT_CH), bf16),
            pltpu.VMEM((2, ROWS_DEV * W, MID_CH), bf16),
            pltpu.VMEM((27, OUT_CH, MID_CH), bf16),
            pltpu.VMEM((2, W, MID_CH), bf16),
            pltpu.VMEM((2, W, MID_CH), bf16),
            pltpu.VMEM((2, 2, (ROWS_DEV + 2) * W, 2 * MID_CH), bf16),
            dma((14,)),
            pltpu.VMEM((plane, 3, planes, devices), bf16),
            pltpu.VMEM((plane, 3, planes, devices), bf16),
            pltpu.VMEM((planes, 3, plane, devices), bf16),
            pltpu.VMEM((planes, 3, plane, devices), bf16),
            pltpu.VMEM((cells, cells // 2), bf16),
            pltpu.VMEM((cells, cells), bf16),
            pltpu.VMEM((cells, cells // 2), bf16),
            pltpu.VMEM((2, 2, LAT_CH, 2 * W), bf16),
            pltpu.VMEM((2, 2, LAT_CH, 2 * W), bf16),
            pltpu.SemaphoreType.REGULAR,
            pltpu.SemaphoreType.REGULAR,
            dma((plane,)), dma((plane,)), dma((planes,)), dma((planes,)),
            dma((2,)), dma((2,)), dma((2,)), dma((2,)),
        ],
        compiler_params=pltpu.CompilerParams(collective_id=0, has_side_effects=True, vmem_limit_bytes=28 * 1024 * 1024),
        cost_estimate=pl.CostEstimate(flops=3_000_000_000, bytes_accessed=13_000_000, transcendentals=0),
    )(
        *(pltpu.with_memory_space_constraint(x, pltpu.HBM) for x in (
            assign,
            layout,
            latents,
            latent_cache,
            feature_cache.reshape(2, ROWS_DEV * W, MID_CH),
            jnp.swapaxes(second_weight, 3, 4).reshape(27, OUT_CH, MID_CH),
        )),
    )


def decode_kernel(
    per_group, place_axis, assign_hbm, counts_hbm, window_ref, w1_hbm, b1_hbm, gain_hbm, fc_hbm, upper_ref, middle_ref, lower_ref,
    part_ref, b2_hbm,
    out_hbm, ln_ref, fn_ref,
    assign_ref, counts_ref, w1_ref, b1_ref, gain_ref, fc_ref, sums_ref, b2_ref, xs_ref, pre_ref, h_ref, frames_ref,
    load_sem, out_sem,
):
    f32, bf16 = jnp.float32, jnp.bfloat16
    place = (lax.axis_index(place_axis) + per_group // 2) % (per_group * REQS)
    position = place % per_group
    small = [
        pltpu.make_async_copy(source, target, load_sem.at[i])
        for i, (source, target) in enumerate((
            (w1_hbm, w1_ref), (b1_hbm, b1_ref), (gain_hbm, gain_ref), (b2_hbm, b2_ref), (fc_hbm, fc_ref),
            (assign_hbm, assign_ref), (counts_hbm, counts_ref),
        ))
    ]
    for copy in small:
        copy.start()
    rows = ROWS_DEV + 2
    cells, tile = rows * W, ROWS_DEV * W
    per_frame = (ROWS_DEV + 4) * W
    xt = window_ref[...].astype(f32)
    lanes = xt.shape[1]
    column = lax.broadcasted_iota(jnp.int32, xt.shape, 1) % W
    shifted = (
        jnp.where(column == 0, 0.0, pltpu.roll(xt, 1, 1)),
        xt,
        jnp.where(column == W - 1, 0.0, pltpu.roll(xt, lanes - 1, 1)),
    )
    for e in range(3):
        odd = pltpu.roll(shifted[e], lanes - W, 1).astype(bf16)
        even = shifted[e].astype(bf16)
        for b in range(3):
            source, start = ((even, 0), (odd, 0), (even, 2 * W))[b]
            for a in range(3):
                k = ((a * 3 + b) * 3 + e) * LAT_CH
                for t in range(FMAX):
                    at = (t + a) * per_frame + start
                    xs_ref[k : k + LAT_CH, t * cells : (t + 1) * cells] = source[:, at : at + cells]
    for copy in small:
        copy.wait()
    live = counts_ref[assign_ref[place // per_group]]
    bias = b1_ref[...].reshape(1, MID_CH)
    gain = gain_ref[...].reshape(1, MID_CH)
    row = lax.broadcasted_iota(jnp.int32, (W, MID_CH), 0)

    def linear(t):
        pre_ref[t] = lax.dot_general(
            xs_ref[:, t * cells : (t + 1) * cells], w1_ref[...], (((0,), (0,)), ((), ())), preferred_element_type=f32
        )

    def activate(t, y):
        at = pl.ds(pl.multiple_of(y * W, W), W)
        pre = pre_ref[t, at, :] + bias
        inverse = lax.rsqrt(jnp.mean(pre * pre, axis=1, keepdims=True) + 1e-06)
        half = 0.5 * (pre * inverse * gain)
        above = jnp.logical_and(y == 0, position == 0)
        below = jnp.logical_and(y == rows - 1, position == per_group - 1)
        values = jnp.where(jnp.logical_or(above, below), 0.0, half + half * jnp.tanh(half))
        here = values.astype(bf16)
        h_ref[0, t, at, 0:MID_CH] = jnp.where(row == 0, 0.0, pltpu.roll(values, 1, 0)).astype(bf16)
        h_ref[0, t, at, MID_CH : 2 * MID_CH] = here
        h_ref[1, t, at, 0:MID_CH] = here
        h_ref[1, t, at, MID_CH : 2 * MID_CH] = jnp.where(row == W - 1, 0.0, pltpu.roll(values, W - 1, 0)).astype(bf16)

    def keep_last(j):
        own = slice(W, W + tile)
        fresh = h_ref[1, jnp.maximum(j + live - 2, 0), own, 0:MID_CH].astype(f32)
        fn_ref[j] = jnp.where(j + live == 1, fc_ref[1].astype(f32), fresh).astype(bf16)
        latest = window_ref[:, pl.ds(pl.multiple_of((j + live) * per_frame + 2 * W, 2 * W), tile)].astype(f32)
        latest = jnp.concatenate([latest[:, y * W : (y + 1) * W] for y in range(ROWS_DEV)], axis=0).astype(bf16)
        wide = lax.dot_general(latest, fold, (((1,), (1,)), ((), ())), preferred_element_type=f32)
        wide = jnp.where(member[None], wide.reshape(ROWS_DEV, LAT_CH, W * LAT_CH), 0.0)
        ln_ref[j] = jnp.sum(wide, axis=1).astype(bf16)

    def finish(t, py):
        ready = []
        for px in range(2):
            total = sums_ref[t, px, py] + (part_ref[t, px, py] if t < 2 else 0.0) + bias2
            ready.append(jnp.where(t < live, total, 0.0).astype(bf16))
        for pair in range(ROWS_DEV // 2):
            part = slice(pair * 2 * W, (pair + 1) * 2 * W)
            joined = jnp.concatenate([ready[0][:, part], ready[1][:, part]], axis=1)
            woven = jnp.dot(joined, weave, preferred_element_type=f32).astype(bf16)
            for line in range(2):
                frames_ref[t, 2 * (2 * pair + line) + py] = woven[:, line * 2 * W : (line + 1) * 2 * W]

    for t in range(FMAX):
        linear(t)
    for y in range(rows):
        activate(0, y)
    block = tile
    source = lax.broadcasted_iota(jnp.int32, (block, block), 0)
    target = lax.broadcasted_iota(jnp.int32, (block, block), 1)
    parity, line, cell = source // (2 * W), source // W % 2, source % W
    weave = (target == line * 2 * W + cell * 2 + parity).astype(bf16)
    bias2 = jnp.transpose(jnp.broadcast_to(b2_ref[...].reshape(1, OUT_CH), (8, OUT_CH)))[:, 0:1]
    fold, member = spread_of_cells()
    done = [pltpu.make_async_copy(frames_ref.at[t], out_hbm.at[t], out_sem.at[t]) for t in range(FMAX)]
    for frame in range(FMAX):
        times = tuple(range(2, frame - 1, -1))
        started = set() if frame == 0 else {0, 1, 2}

        @pl.loop(0, 2)
        def _(i):
            for r in range(3):
                add_products(sums_ref, h_ref, upper_ref, middle_ref, lower_ref, i, frame, frame, 3 - frame, times, started, (r,))
                if frame + 1 < FMAX:
                    activate(frame + 1, i * 3 + r)
            if frame > 0:
                finish(frame - 1, i)
            if frame == FMAX - 1:
                keep_last(i)

        if frame > 0:
            done[frame - 1].start()
    for py in range(2):
        finish(FMAX - 1, py)
    done[FMAX - 1].start()
    for copy in done:
        copy.wait()


def decode(devices, assign, counts, gathered, first_weight, first_bias, norm_gain, feature_cache, second_bias):
    per_group = devices // REQS
    cells = (ROWS_DEV + 2) * W
    vm, hbm = pl.BlockSpec(memory_space=pltpu.VMEM), pl.BlockSpec(memory_space=pltpu.HBM)
    f32, bf16 = jnp.float32, jnp.bfloat16
    frames, latents, features = pl.pallas_call(
        functools.partial(decode_kernel, per_group, "seq"),
        out_shape=(
            jax.ShapeDtypeStruct((FMAX, 2 * ROWS_DEV, OUT_CH, 2 * W), bf16),
            jax.ShapeDtypeStruct((2, ROWS_DEV, W * LAT_CH), bf16),
            jax.ShapeDtypeStruct((2, ROWS_DEV * W, MID_CH), bf16),
        ),
        in_specs=[hbm, hbm, vm] + [hbm] * 4 + [vm] * 4 + [hbm],
        out_specs=(hbm, vm, vm),
        scratch_shapes=[
            pltpu.SMEM((REQS,), jnp.int32),
            pltpu.SMEM((REQS,), jnp.int32),
            pltpu.VMEM((27 * LAT_CH, MID_CH), bf16),
            pltpu.VMEM((MID_CH,), f32),
            pltpu.VMEM((MID_CH,), f32),
            pltpu.VMEM((2, ROWS_DEV * W, MID_CH), bf16),
            pltpu.VMEM((FMAX, 2, 2, OUT_CH, ROWS_DEV * W), f32),
            pltpu.VMEM((OUT_CH,), f32),
            pltpu.VMEM((27 * LAT_CH, FMAX * cells), bf16),
            pltpu.VMEM((FMAX, cells, MID_CH), f32),
            pltpu.VMEM((2, FMAX, cells, 2 * MID_CH), bf16),
            pltpu.VMEM((FMAX, 2 * ROWS_DEV, OUT_CH, 2 * W), bf16),
            pltpu.SemaphoreType.DMA((7,)),
            pltpu.SemaphoreType.DMA((FMAX,)),
        ],
        compiler_params=pltpu.CompilerParams(vmem_limit_bytes=28 * 1024 * 1024),
        cost_estimate=pl.CostEstimate(flops=4_500_000_000, bytes_accessed=11_000_000, transcendentals=442368),
    )(
        assign, counts, gathered[0], first_weight.reshape(27 * LAT_CH, MID_CH), first_bias, norm_gain,
        feature_cache.reshape(2, ROWS_DEV * W, MID_CH), *gathered[1:], second_bias,
    )
    return jnp.swapaxes(frames, 2, 3), latents, features.reshape(2, ROWS_DEV, W, MID_CH)


def body(
    latents,
    layout,
    assign,
    counts,
    latent_cache,
    feature_cache,
    first_weight,
    first_bias,
    norm_gain,
    second_weight,
    second_bias,
):
    devices = lax.axis_size("seq")
    gathered = gather(devices, assign, layout, latents, latent_cache, feature_cache, second_weight)
    return decode(devices, assign, counts, gathered, first_weight, first_bias, norm_gain, feature_cache, second_bias)


def solution(mesh):
    return jax.shard_map(
        body,
        mesh=mesh,
        in_specs=(
            P(None, ("rep", "seq")),
            P("rep", None),
            P("rep"),
            P("rep"),
            P(None, ("rep", "seq"), None),
            P(None, ("rep", "seq"), None, None),
            P(),
            P(),
            P(),
            P(),
            P(),
        ),
        out_specs=(
            P(None, ("rep", "seq"), None, None),
            P(None, ("rep", "seq"), None),
            P(None, ("rep", "seq"), None, None),
        ),
        check_vma=False,
    )
```

```python
import functools

import jax
import jax.numpy as jnp
from jax import lax
from jax.experimental import pallas as pl
from jax.experimental.pallas import tpu as pltpu
from jax.sharding import PartitionSpec as P

LAT_CH = 16
MID_CH = 384
OUT_CH = 192
REQS = 8
FMAX = 3
ROWS_DEV = 4
W = 64


def spread_of_cells():
    lane = lax.broadcasted_iota(jnp.int32, (W * LAT_CH, W), 0)
    cell = lax.broadcasted_iota(jnp.int32, (W * LAT_CH, W), 1)
    fold = (lane // LAT_CH == cell).astype(jnp.bfloat16)
    channel = lax.broadcasted_iota(jnp.int32, (LAT_CH, W * LAT_CH), 0)
    member = lax.broadcasted_iota(jnp.int32, (LAT_CH, W * LAT_CH), 1) % LAT_CH == channel
    return fold, member


def rows_outside(position, last):
    cells = (ROWS_DEV + 2) * W
    row = lax.broadcasted_iota(jnp.int32, (cells, MID_CH), 0)
    above = jnp.logical_and(row < W, position == 0)
    return jnp.logical_or(above, jnp.logical_and(row >= cells - W, position == last))


def lay_out(target, frame, values):
    cells = values.shape[0]
    column = lax.broadcasted_iota(jnp.int32, values.shape, 0) % W
    before = jnp.where(column == 0, 0.0, pltpu.roll(values, 1, 0)).astype(jnp.bfloat16)
    after = jnp.where(column == W - 1, 0.0, pltpu.roll(values, cells - 1, 0)).astype(jnp.bfloat16)
    here = values.astype(jnp.bfloat16)
    target[0, frame, :, 0:MID_CH] = before
    target[0, frame, :, MID_CH : 2 * MID_CH] = here
    target[1, frame, :, 0:MID_CH] = here
    target[1, frame, :, MID_CH : 2 * MID_CH] = after


def combine_taps(weight, upper, middle, lower):
    near = (((0,), (1, 2)), ((0, 1), (2,)))

    @pl.loop(0, 3)
    def _(a):
        base = a * 9
        tap = [[weight[base + b * 3 + e].astype(jnp.float32) for e in range(3)] for b in range(3)]
        for target, start, py, dy in ((upper, 0, 0, 0), (middle, 0, 0, 1), (middle, OUT_CH, 1, 0), (lower, 0, 1, 1)):
            taps = [sum(tap[b][e] for b in near[py][dy]) for e in range(3)]
            for px in range(2):
                for dx in range(2):
                    total = sum(taps[e] for e in near[px][dx]).astype(jnp.bfloat16)
                    target[px, a, start : start + OUT_CH, dx * MID_CH : (dx + 1) * MID_CH] = total


def add_products(sums, features, upper, middle, lower, px, frame, a, count, times, started, parts=(0, 1, 2)):
    block = ROWS_DEV * W
    for r in parts:
        weights = (middle, upper, lower)[r]
        row = (1, 0, 2)[r]
        right = features[px, frame, row * W : row * W + block, :]
        left = weights[px, a : a + count]
        height = left.shape[1]
        part = lax.dot_general(
            left.reshape(count * height, left.shape[2]), right, (((1,), (1,)), ((), ())), preferred_element_type=jnp.float32
        )
        for i, t in enumerate(times):
            for py in ((0, 1), (0,), (1,))[r]:
                at = i * height + (py * OUT_CH if r == 0 else 0)
                piece = part[at : at + OUT_CH]
                if r == 0 and t not in started:
                    sums[t, px, py] = piece
                else:
                    sums[t, px, py] = sums[t, px, py] + piece


def counted_before(marks, earlier):
    size = earlier.shape[0]
    carry = jnp.zeros((marks.shape[0], 1), jnp.float32)
    parts = []
    for start in range(0, marks.shape[1], size):
        block = marks[:, start : start + size]
        parts.append(jnp.dot(block.astype(jnp.bfloat16), earlier, preferred_element_type=jnp.float32) + carry)
        carry = carry + jnp.sum(block, axis=1, keepdims=True)
    return jnp.concatenate(parts, axis=1)


def by_distance(ring):
    return sorted(range(1, ring), key=lambda i: (-min(i, ring - i), i))


def gather_kernel(
    devices, assign_hbm, layout_hbm, latents_hbm, cache_hbm, features_hbm, weight_hbm,
    window_ref, upper_ref, middle_ref, lower_ref, part_ref,
    assign_ref, layout_ref, latents_ref, cache_ref, features_ref, weight_ref, above_ref, below_ref,
    small_ref, load_sem,
    send1_ref, recv1_ref, send2_ref, recv2_ref, upper_table, table_ref, lower_table, rim_out_ref, rim_in_ref,
    plane_ok, far_ok, s1, r1, s2, r2, sf, rf, sh, rh,
):
    f32, bf16, i32 = jnp.float32, jnp.bfloat16, jnp.int32
    per_group = devices // REQS
    plane = per_group // 2
    planes = devices // plane
    tile = ROWS_DEV * W
    tile_cells = FMAX * tile
    per_peer = tile_cells // devices
    rep, me = lax.axis_index("rep"), lax.axis_index("seq")
    z, p = me // plane, me % plane
    even = p % 2 == 0
    ahead, behind = (me + 1) % devices, (me + devices - 1) % devices
    first, final = p == 0, p == plane - 1

    def signal(semaphore, device):
        pl.semaphore_signal(semaphore, inc=1, device_id=(rep, device), device_id_type=pl.DeviceIdType.MESH)

    loads = [
        pltpu.make_async_copy(source, target, load_sem.at[i])
        for i, (source, target) in enumerate((
            (layout_hbm, layout_ref), (assign_hbm, assign_ref), (latents_hbm, latents_ref), (cache_hbm, cache_ref), (features_hbm, features_ref),
        ))
    ]
    loads = loads + [
        pltpu.make_async_copy(weight_hbm.at[3 * i : 3 * i + 3], weight_ref.at[3 * i : 3 * i + 3], load_sem.at[5 + i])
        for i in range(9)
    ]
    for copy in loads:
        copy.start()

    barrier = pltpu.get_barrier_semaphore()
    for i in by_distance(planes):
        signal(barrier, ((z + i) % planes) * plane + (p // 2) * 2 + 1)
    for q in range(0, plane, 2):
        @pl.when(p != q)
        def _():
            signal(barrier, z * plane + q)

    @pl.when(final)
    def _():
        signal(barrier, ahead)

    @pl.when(first)
    def _():
        signal(barrier, behind)

    row_of = lax.broadcasted_iota(i32, (tile_cells // 3, tile_cells // 3), 0)
    lane_of = lax.broadcasted_iota(i32, (tile_cells // 3, tile_cells // 3), 1)
    earlier = (row_of < lane_of).astype(bf16)
    loads[0].wait()
    loads[1].wait()
    own = layout_ref[pl.ds(me, 1), :]
    request = ((own // (ROWS_DEV * per_group * W)) * 43) // 128
    group = jnp.zeros_like(own)
    for g in range(REQS):
        group = group + jnp.where(assign_ref[g] == request, g, 0)
    place = group * per_group + (own // tile) % per_group
    target = (place + devices - per_group // 2) % devices
    line = (target % plane) * planes + target // plane
    hit = lax.broadcasted_iota(i32, (devices, tile_cells), 0) == line
    marks = hit.astype(f32)
    order = counted_before(marks, earlier)
    loads[2].wait()
    latents = latents_ref[...]
    rows = []
    for k in range(per_peer):
        chosen = jnp.where(order == k, marks, 0.0).astype(bf16)
        rows.append(lax.dot_general(latents, chosen, (((1,), (1,)), ((), ())), preferred_element_type=f32))
    rows.append(jnp.zeros((devices - per_peer * LAT_CH, devices), f32))
    sent = jnp.transpose(jnp.concatenate(rows, axis=0)).reshape(plane, planes, devices)
    for q in range(plane):
        send1_ref[q, 0] = (sent[q - 1] if q > 0 else pltpu.roll(sent[plane - 1], 1, 0)).astype(bf16)
        send1_ref[q, 1] = sent[q].astype(bf16)
        send1_ref[q, 2] = (sent[q + 1] if q < plane - 1 else pltpu.roll(sent[0], planes - 1, 0)).astype(bf16)

    @pl.when(even)
    def _():
        pl.semaphore_wait(barrier, plane - 1 + jnp.where(first, 1, 0))
        signal(plane_ok, me + 1)

    @pl.when(jnp.logical_not(even))
    def _():
        pl.semaphore_wait(plane_ok, 1)

    near = []
    for i in range(1, plane):
        q = (p + i) % plane
        near.append(pltpu.make_async_remote_copy(
            src_ref=send1_ref.at[q], dst_ref=recv1_ref.at[p], send_sem=s1.at[i], recv_sem=r1.at[i],
            device_id=(rep, z * plane + q), device_id_type=pl.DeviceIdType.MESH))
        near[-1].start()
    recv1_ref[p] = send1_ref[p]

    my_place = (me + per_group // 2) % devices
    my_group, position = my_place // per_group, my_place % per_group
    frame = ROWS_DEV * per_group * W
    half = tile // 2
    for side, table in enumerate((upper_table, table_ref, lower_table)):
        other = (my_place + side - 1 + devices) % devices
        start = assign_ref[other // per_group] * (FMAX * frame) + (other % per_group) * tile
        offset = layout_ref[...] - start
        inside = jnp.logical_and(jnp.logical_and(offset >= 0, offset < FMAX * frame), (offset & (frame - tile)) == 0)
        inner = offset & (tile - 1)
        if side == 0:
            within = jnp.where(inner >= half, (offset // frame) * half + inner - half, -1)
        elif side == 1:
            within = (offset // frame) * tile + inner
        else:
            within = jnp.where(inner < half, (offset // frame) * half + inner, -1)
        within = within.astype(f32)
        order = counted_before(inside.astype(f32), earlier)
        spot = lax.broadcasted_iota(i32, (devices, table.shape[1]), 1).astype(f32)
        for k in range(per_peer):
            chosen = jnp.logical_and(order == k, inside)
            home = jnp.sum(jnp.where(chosen, within, 0.0), axis=1, keepdims=True)
            table[k * devices : (k + 1) * devices, :] = (home == spot).astype(bf16)

    for copy in near:
        copy.wait()
    to = lax.broadcasted_iota(i32, (devices, devices), 0)
    source = lax.broadcasted_iota(i32, (devices, devices), 1)
    turn = (source == (to % plane) * planes + to // plane).astype(bf16)
    for side in range(3):
        turned = jnp.dot(turn, recv1_ref[:, side].reshape(devices, devices), preferred_element_type=f32)
        send2_ref[:, side] = turned.reshape(planes, plane, devices).astype(bf16)

    @pl.when(jnp.logical_not(even))
    def _():
        pl.semaphore_wait(barrier, 2 * (planes - 1) + jnp.where(final, 1, 0))
        signal(far_ok, me - 1)

    @pl.when(even)
    def _():
        pl.semaphore_wait(far_ok, 1)

    far = []
    for i in by_distance(planes):
        q = (z + i) % planes
        far.append(pltpu.make_async_remote_copy(
            src_ref=send2_ref.at[q], dst_ref=recv2_ref.at[z], send_sem=s2.at[i], recv_sem=r2.at[i],
            device_id=(rep, q * plane + p), device_id_type=pl.DeviceIdType.MESH))
        far[-1].start()
    recv2_ref[z] = send2_ref[z]
    loads[4].wait()
    sides = []
    for side in range(2):
        sides.append(pltpu.make_async_remote_copy(
            src_ref=features_ref.at[:, pl.ds((ROWS_DEV - 1) * W * (1 - side), W)],
            dst_ref=(above_ref, below_ref)[side],
            send_sem=sf.at[side], recv_sem=rf.at[side],
            device_id=(rep, (ahead, behind)[side]), device_id_type=pl.DeviceIdType.MESH))
        sides[-1].start()

    loads[3].wait()
    wide = cache_ref[...].astype(f32).reshape(2 * ROWS_DEV, W * LAT_CH)
    fold, member = spread_of_cells()
    stacked = jnp.concatenate([
        jnp.where(member, jnp.broadcast_to(wide[i : i + 1], member.shape), 0.0) for i in range(2 * ROWS_DEV)
    ], axis=0).astype(bf16)
    folded = jnp.dot(stacked, fold, preferred_element_type=f32)
    cached = jnp.concatenate([folded[i * LAT_CH : (i + 1) * LAT_CH] for i in range(2 * ROWS_DEV)], axis=1).astype(bf16)

    rim = 2 * W
    for f in range(2):
        rim_out_ref[0, f] = cached[:, (f + 1) * tile - rim : (f + 1) * tile]
        rim_out_ref[1, f] = cached[:, f * tile : f * tile + rim]
    edges = []
    for side in range(2):
        edges.append(pltpu.make_async_remote_copy(
            src_ref=rim_out_ref.at[side], dst_ref=rim_in_ref.at[side],
            send_sem=sh.at[side], recv_sem=rh.at[side],
            device_id=(rep, (ahead, behind)[side]), device_id_type=pl.DeviceIdType.MESH))
        edges[-1].start()

    for copy in loads[5:]:
        copy.wait()
    combine_taps(weight_ref, upper_ref, middle_ref, lower_ref)

    for copy in sides:
        copy.wait()
    for copy in edges:
        copy.wait_recv()
    outside = rows_outside(position, per_group - 1)
    for f in range(2):
        values = jnp.concatenate([above_ref[f], features_ref[f], below_ref[f]], axis=0).astype(f32)
        lay_out(small_ref, f, jnp.where(outside, 0.0, values))
    for px in range(2):
        add_products(part_ref, small_ref, upper_ref, middle_ref, lower_ref, px, 1, 0, 2, (1, 0), {})
        add_products(part_ref, small_ref, upper_ref, middle_ref, lower_ref, px, 0, 0, 1, (0,), {0})
    for copy in far:
        copy.wait()
    found = []
    for side, table in enumerate((upper_table, table_ref, lower_table)):
        arrived = jnp.transpose(recv2_ref[:, side].astype(f32).reshape(devices, devices))
        arrived = jnp.concatenate([arrived[k * LAT_CH : (k + 1) * LAT_CH] for k in range(per_peer)], axis=1)
        found.append(jnp.dot(arrived.astype(bf16), table[...], preferred_element_type=f32))
    nothing = jnp.zeros((LAT_CH, rim), f32)
    for f in range(2 + FMAX):
        if f < 2:
            top, here, bottom = rim_in_ref[0, f].astype(f32), cached[:, f * tile : (f + 1) * tile], rim_in_ref[1, f].astype(f32)
        else:
            t = f - 2
            top, bottom = (found[side][:, t * rim : (t + 1) * rim] for side in (0, 2))
            here = found[1][:, t * tile : (t + 1) * tile].astype(bf16)
        at = f * (tile + 2 * rim)
        window_ref[:, at : at + rim] = jnp.where(position == 0, nothing, top).astype(bf16)
        window_ref[:, at + rim : at + rim + tile] = here
        window_ref[:, at + rim + tile : at + 2 * rim + tile] = jnp.where(position == per_group - 1, nothing, bottom).astype(bf16)
    for copy in edges:
        copy.wait_send()


def gather(devices, assign, layout, latents, latent_cache, feature_cache, second_weight):
    plane = devices // REQS // 2
    planes = devices // plane
    cells = FMAX * ROWS_DEV * W
    vm, hbm = pl.BlockSpec(memory_space=pltpu.VMEM), pl.BlockSpec(memory_space=pltpu.HBM)
    bf16, dma = jnp.bfloat16, pltpu.SemaphoreType.DMA
    return pl.pallas_call(
        functools.partial(gather_kernel, devices),
        out_shape=(
            jax.ShapeDtypeStruct((LAT_CH, (2 + FMAX) * (ROWS_DEV + 4) * W), bf16),
            jax.ShapeDtypeStruct((2, 3, OUT_CH, 2 * MID_CH), bf16),
            jax.ShapeDtypeStruct((2, 3, 2 * OUT_CH, 2 * MID_CH), bf16),
            jax.ShapeDtypeStruct((2, 3, OUT_CH, 2 * MID_CH), bf16),
            jax.ShapeDtypeStruct((2, 2, 2, OUT_CH, ROWS_DEV * W), jnp.float32),
        ),
        in_specs=[hbm] * 6,
        out_specs=(vm, vm, vm, vm, vm),
        scratch_shapes=[
            pltpu.SMEM((REQS,), jnp.int32),
            pltpu.VMEM((devices, cells), jnp.int32),
            pltpu.VMEM((LAT_CH, cells), bf16),
            pltpu.VMEM((2, ROWS_DEV, W * LAT_CH), bf16),
            pltpu.VMEM((2, ROWS_DEV * W, MID_CH), bf16),
            pltpu.VMEM((27, OUT_CH, MID_CH), bf16),
            pltpu.VMEM((2, W, MID_CH), bf16),
            pltpu.VMEM((2, W, MID_CH), bf16),
            pltpu.VMEM((2, 2, (ROWS_DEV + 2) * W, 2 * MID_CH), bf16),
            dma((14,)),
            pltpu.VMEM((plane, 3, planes, devices), bf16),
            pltpu.VMEM((plane, 3, planes, devices), bf16),
            pltpu.VMEM((planes, 3, plane, devices), bf16),
            pltpu.VMEM((planes, 3, plane, devices), bf16),
            pltpu.VMEM((cells, cells // 2), bf16),
            pltpu.VMEM((cells, cells), bf16),
            pltpu.VMEM((cells, cells // 2), bf16),
            pltpu.VMEM((2, 2, LAT_CH, 2 * W), bf16),
            pltpu.VMEM((2, 2, LAT_CH, 2 * W), bf16),
            pltpu.SemaphoreType.REGULAR,
            pltpu.SemaphoreType.REGULAR,
            dma((plane,)), dma((plane,)), dma((planes,)), dma((planes,)),
            dma((2,)), dma((2,)), dma((2,)), dma((2,)),
        ],
        compiler_params=pltpu.CompilerParams(collective_id=0, has_side_effects=True, vmem_limit_bytes=28 * 1024 * 1024),
        cost_estimate=pl.CostEstimate(flops=3_000_000_000, bytes_accessed=13_000_000, transcendentals=0),
    )(
        *(pltpu.with_memory_space_constraint(x, pltpu.HBM) for x in (
            assign,
            layout,
            latents,
            latent_cache,
            feature_cache.reshape(2, ROWS_DEV * W, MID_CH),
            jnp.swapaxes(second_weight, 3, 4).reshape(27, OUT_CH, MID_CH),
        )),
    )


def decode_kernel(
    per_group, place_axis, assign_hbm, counts_hbm, window_ref, w1_ref, b1_ref, gain_ref, fc_ref, upper_ref, middle_ref, lower_ref,
    part_ref, b2_ref,
    out_hbm, ln_hbm, fn_hbm,
    assign_ref, counts_ref, sums_ref, xs_ref, pre_ref, h_ref, frames_ref, ln_ref,
    load_sem, out_sem, last_sem, keep_sem,
):
    f32, bf16 = jnp.float32, jnp.bfloat16
    place = (lax.axis_index(place_axis) + per_group // 2) % (per_group * REQS)
    position = place % per_group
    small = [
        pltpu.make_async_copy(source, target, load_sem.at[i])
        for i, (source, target) in enumerate(((assign_hbm, assign_ref), (counts_hbm, counts_ref)))
    ]
    for copy in small:
        copy.start()
    rows = ROWS_DEV + 2
    cells, tile = rows * W, ROWS_DEV * W
    per_frame = (ROWS_DEV + 4) * W
    xt = window_ref[...].astype(f32)
    lanes = xt.shape[1]
    column = lax.broadcasted_iota(jnp.int32, xt.shape, 1) % W
    shifted = (
        jnp.where(column == 0, 0.0, pltpu.roll(xt, 1, 1)),
        xt,
        jnp.where(column == W - 1, 0.0, pltpu.roll(xt, lanes - 1, 1)),
    )
    evens = [one.astype(bf16) for one in shifted]
    odds = [pltpu.roll(one, lanes - W, 1).astype(bf16) for one in shifted]

    def patches(t):
        for e in range(3):
            for b in range(3):
                source, start = ((evens[e], 0), (odds[e], 0), (evens[e], 2 * W))[b]
                for a in range(3):
                    k = ((a * 3 + b) * 3 + e) * LAT_CH
                    at = (t + a) * per_frame + start
                    xs_ref[k : k + LAT_CH, t * cells : (t + 1) * cells] = source[:, at : at + cells]

    bias = b1_ref[...].reshape(1, MID_CH)
    gain = gain_ref[...].reshape(1, MID_CH)
    row = lax.broadcasted_iota(jnp.int32, (W, MID_CH), 0)

    def linear(t):
        pre_ref[t] = lax.dot_general(
            xs_ref[:, t * cells : (t + 1) * cells], w1_ref[...], (((0,), (0,)), ((), ())), preferred_element_type=f32
        )

    def activate(t, y):
        pre = pre_ref[t, y * W : (y + 1) * W, :] + bias
        inverse = lax.rsqrt(jnp.mean(pre * pre, axis=1, keepdims=True) + 1e-06)
        half = 0.5 * (pre * inverse * gain)
        values = half + half * jnp.tanh(half)
        if y == 0:
            values = jnp.where(position == 0, 0.0, values)
        if y == rows - 1:
            values = jnp.where(position == per_group - 1, 0.0, values)
        at = slice(y * W, (y + 1) * W)
        here = values.astype(bf16)
        h_ref[0, t, at, 0:MID_CH] = jnp.where(row == 0, 0.0, pltpu.roll(values, 1, 0)).astype(bf16)
        h_ref[0, t, at, MID_CH : 2 * MID_CH] = here
        h_ref[1, t, at, 0:MID_CH] = here
        h_ref[1, t, at, MID_CH : 2 * MID_CH] = jnp.where(row == W - 1, 0.0, pltpu.roll(values, W - 1, 0)).astype(bf16)

    for t in range(FMAX):
        patches(t)
        linear(t)
    for copy in small:
        copy.wait()
    live = counts_ref[assign_ref[place // per_group]]
    fold, member = spread_of_cells()
    for j in range(2):
        latest = window_ref[:, pl.ds(pl.multiple_of((j + live) * per_frame + 2 * W, 2 * W), tile)].astype(f32)
        latest = jnp.concatenate([latest[:, y * W : (y + 1) * W] for y in range(ROWS_DEV)], axis=0).astype(bf16)
        wide = lax.dot_general(latest, fold, (((1,), (1,)), ((), ())), preferred_element_type=f32)
        wide = jnp.where(member[None], wide.reshape(ROWS_DEV, LAT_CH, W * LAT_CH), 0.0)
        ln_ref[j] = jnp.sum(wide, axis=1).astype(bf16)
    kept = [pltpu.make_async_copy(ln_ref, ln_hbm, keep_sem.at[0])]
    kept[0].start()
    for y in range(rows):
        activate(0, y)
    block = tile
    source = lax.broadcasted_iota(jnp.int32, (block, block), 0)
    target = lax.broadcasted_iota(jnp.int32, (block, block), 1)
    parity, line, cell = source // (2 * W), source // W % 2, source % W
    weave = (target == line * 2 * W + cell * 2 + parity).astype(bf16)
    bias2 = jnp.transpose(jnp.broadcast_to(b2_ref[...].reshape(1, OUT_CH), (8, OUT_CH)))[:, 0:1]
    started = set()
    done = []
    own = slice(W, W + tile)
    for frame in range(FMAX):
        times = tuple(range(2, frame - 1, -1))
        for px in range(2):
            for r in range(3):
                add_products(sums_ref, h_ref, upper_ref, middle_ref, lower_ref, px, frame, frame, 3 - frame, times, started, (r,))
                if frame + 1 < FMAX:
                    activate(frame + 1, px * 3 + r)
        started = {0, 1, 2}
        t = frame
        for py in range(2):
            ready = []
            for px in range(2):
                total = sums_ref[t, px, py] + (part_ref[t, px, py] if t < 2 else 0.0) + bias2
                ready.append(jnp.where(t < live, total, 0.0).astype(bf16))
            for pair in range(ROWS_DEV // 2):
                part = slice(pair * 2 * W, (pair + 1) * 2 * W)
                joined = jnp.concatenate([ready[0][:, part], ready[1][:, part]], axis=1)
                woven = jnp.dot(joined, weave, preferred_element_type=f32).astype(bf16)
                for line in range(2):
                    at = 2 * (2 * pair + line) + py
                    frames_ref[t, at] = woven[:, line * 2 * W : (line + 1) * 2 * W]
                    if t == FMAX - 1:
                        done.append(pltpu.make_async_copy(frames_ref.at[t, at], out_hbm.at[t, at], last_sem.at[at]))
                        done[-1].start()
        if t < FMAX - 1:
            done.append(pltpu.make_async_copy(frames_ref.at[t], out_hbm.at[t], out_sem.at[t]))
            done[-1].start()
        if frame == FMAX - 2:
            @pl.when(live == 1)
            def _():
                pltpu.make_async_copy(fc_ref.at[1], fn_hbm.at[0], keep_sem.at[1]).start()

            @pl.when(live > 1)
            def _():
                pltpu.make_async_copy(h_ref.at[1, jnp.maximum(live - 2, 0), own, 0:MID_CH], fn_hbm.at[0], keep_sem.at[1]).start()

            kept.append(pltpu.make_async_copy(fc_ref.at[1], fn_hbm.at[0], keep_sem.at[1]))
            kept.append(pltpu.make_async_copy(h_ref.at[1, live - 1, own, 0:MID_CH], fn_hbm.at[1], keep_sem.at[2]))
            kept[-1].start()
    for copy in kept:
        copy.wait()
    for copy in done:
        copy.wait()


def decode(devices, assign, counts, gathered, first_weight, first_bias, norm_gain, feature_cache, second_bias):
    per_group = devices // REQS
    cells = (ROWS_DEV + 2) * W
    vm, hbm = pl.BlockSpec(memory_space=pltpu.VMEM), pl.BlockSpec(memory_space=pltpu.HBM)
    f32, bf16 = jnp.float32, jnp.bfloat16
    frames, latents, features = pl.pallas_call(
        functools.partial(decode_kernel, per_group, "seq"),
        out_shape=(
            jax.ShapeDtypeStruct((FMAX, 2 * ROWS_DEV, OUT_CH, 2 * W), bf16),
            jax.ShapeDtypeStruct((2, ROWS_DEV, W * LAT_CH), bf16),
            jax.ShapeDtypeStruct((2, ROWS_DEV * W, MID_CH), bf16),
        ),
        in_specs=[hbm, hbm] + [vm] * 10,
        out_specs=(hbm, hbm, hbm),
        scratch_shapes=[
            pltpu.SMEM((REQS,), jnp.int32),
            pltpu.SMEM((REQS,), jnp.int32),
            pltpu.VMEM((FMAX, 2, 2, OUT_CH, ROWS_DEV * W), f32),
            pltpu.VMEM((27 * LAT_CH, FMAX * cells), bf16),
            pltpu.VMEM((FMAX, cells, MID_CH), f32),
            pltpu.VMEM((2, FMAX, cells, 2 * MID_CH), bf16),
            pltpu.VMEM((FMAX, 2 * ROWS_DEV, OUT_CH, 2 * W), bf16),
            pltpu.VMEM((2, ROWS_DEV, W * LAT_CH), bf16),
            pltpu.SemaphoreType.DMA((2,)),
            pltpu.SemaphoreType.DMA((FMAX,)),
            pltpu.SemaphoreType.DMA((2 * ROWS_DEV,)),
            pltpu.SemaphoreType.DMA((3,)),
        ],
        compiler_params=pltpu.CompilerParams(vmem_limit_bytes=28 * 1024 * 1024),
        cost_estimate=pl.CostEstimate(flops=4_500_000_000, bytes_accessed=11_000_000, transcendentals=442368),
    )(
        assign, counts, gathered[0], first_weight.reshape(27 * LAT_CH, MID_CH), first_bias, norm_gain,
        feature_cache.reshape(2, ROWS_DEV * W, MID_CH), *gathered[1:], second_bias,
    )
    return jnp.swapaxes(frames, 2, 3), latents, features.reshape(2, ROWS_DEV, W, MID_CH)


def body(
    latents,
    layout,
    assign,
    counts,
    latent_cache,
    feature_cache,
    first_weight,
    first_bias,
    norm_gain,
    second_weight,
    second_bias,
):
    devices = lax.axis_size("seq")
    gathered = gather(devices, assign, layout, latents, latent_cache, feature_cache, second_weight)
    return decode(devices, assign, counts, gathered, first_weight, first_bias, norm_gain, feature_cache, second_bias)


def solution(mesh):
    return jax.shard_map(
        body,
        mesh=mesh,
        in_specs=(
            P(None, ("rep", "seq")),
            P("rep", None),
            P("rep"),
            P("rep"),
            P(None, ("rep", "seq"), None),
            P(None, ("rep", "seq"), None, None),
            P(),
            P(),
            P(),
            P(),
            P(),
        ),
        out_specs=(
            P(None, ("rep", "seq"), None, None),
            P(None, ("rep", "seq"), None),
            P(None, ("rep", "seq"), None, None),
        ),
        check_vma=False,
    )
```

```python
import functools

import jax
import jax.numpy as jnp
from jax import lax
from jax.experimental import pallas as pl
from jax.experimental.pallas import tpu as pltpu
from jax.sharding import PartitionSpec as P

LAT_CH = 16
MID_CH = 384
OUT_CH = 192
REQS = 8
FMAX = 3
ROWS_DEV = 4
W = 64


def spread_of_cells():
    lane = lax.broadcasted_iota(jnp.int32, (W * LAT_CH, W), 0)
    cell = lax.broadcasted_iota(jnp.int32, (W * LAT_CH, W), 1)
    fold = (lane // LAT_CH == cell).astype(jnp.bfloat16)
    channel = lax.broadcasted_iota(jnp.int32, (LAT_CH, W * LAT_CH), 0)
    member = lax.broadcasted_iota(jnp.int32, (LAT_CH, W * LAT_CH), 1) % LAT_CH == channel
    return fold, member


def rows_outside(position, last):
    cells = (ROWS_DEV + 2) * W
    row = lax.broadcasted_iota(jnp.int32, (cells, MID_CH), 0)
    above = jnp.logical_and(row < W, position == 0)
    return jnp.logical_or(above, jnp.logical_and(row >= cells - W, position == last))


def lay_out(target, frame, values):
    cells = values.shape[0]
    column = lax.broadcasted_iota(jnp.int32, values.shape, 0) % W
    before = jnp.where(column == 0, 0.0, pltpu.roll(values, 1, 0)).astype(jnp.bfloat16)
    after = jnp.where(column == W - 1, 0.0, pltpu.roll(values, cells - 1, 0)).astype(jnp.bfloat16)
    here = values.astype(jnp.bfloat16)
    target[0, frame, :, 0:MID_CH] = before
    target[0, frame, :, MID_CH : 2 * MID_CH] = here
    target[1, frame, :, 0:MID_CH] = here
    target[1, frame, :, MID_CH : 2 * MID_CH] = after


def combine_taps(weight, upper, middle, lower):
    near = (((0,), (1, 2)), ((0, 1), (2,)))

    @pl.loop(0, 3)
    def _(a):
        base = a * 9
        tap = [[weight[base + b * 3 + e].astype(jnp.float32) for e in range(3)] for b in range(3)]
        for target, start, py, dy in ((upper, 0, 0, 0), (middle, 0, 0, 1), (middle, OUT_CH, 1, 0), (lower, 0, 1, 1)):
            taps = [sum(tap[b][e] for b in near[py][dy]) for e in range(3)]
            for px in range(2):
                for dx in range(2):
                    total = sum(taps[e] for e in near[px][dx]).astype(jnp.bfloat16)
                    target[px, a, start : start + OUT_CH, dx * MID_CH : (dx + 1) * MID_CH] = total


def add_products(sums, features, upper, middle, lower, px, frame, a, count, times, started, parts=(0, 1, 2)):
    block = ROWS_DEV * W
    for r in parts:
        weights = (middle, upper, lower)[r]
        row = (1, 0, 2)[r]
        right = features[px, frame, row * W : row * W + block, :]
        left = weights[px, a : a + count]
        height = left.shape[1]
        part = lax.dot_general(
            left.reshape(count * height, left.shape[2]), right, (((1,), (1,)), ((), ())), preferred_element_type=jnp.float32
        )
        for i, t in enumerate(times):
            for py in ((0, 1), (0,), (1,))[r]:
                at = i * height + (py * OUT_CH if r == 0 else 0)
                piece = part[at : at + OUT_CH]
                if r == 0 and t not in started:
                    sums[t, px, py] = piece
                else:
                    sums[t, px, py] = sums[t, px, py] + piece


def counted_before(marks, earlier):
    size = earlier.shape[0]
    carry = jnp.zeros((marks.shape[0], 1), jnp.float32)
    parts = []
    for start in range(0, marks.shape[1], size):
        block = marks[:, start : start + size]
        parts.append(jnp.dot(block.astype(jnp.bfloat16), earlier, preferred_element_type=jnp.float32) + carry)
        carry = carry + jnp.sum(block, axis=1, keepdims=True)
    return jnp.concatenate(parts, axis=1)


def by_distance(ring):
    return sorted(range(1, ring), key=lambda i: (-min(i, ring - i), i))


def gather_kernel(
    devices, assign_hbm, layout_hbm, latents_hbm, cache_hbm, features_hbm, weight_hbm,
    window_ref, upper_ref, middle_ref, lower_ref, part_ref,
    assign_ref, layout_ref, latents_ref, cache_ref, features_ref, weight_ref, above_ref, below_ref,
    small_ref, load_sem,
    send1_ref, recv1_ref, send2_ref, recv2_ref, upper_table, table_ref, lower_table, rim_out_ref, rim_in_ref,
    plane_ok, far_ok, s1, r1, s2, r2, sf, rf, sh, rh,
):
    f32, bf16, i32 = jnp.float32, jnp.bfloat16, jnp.int32
    per_group = devices // REQS
    plane = per_group // 2
    planes = devices // plane
    tile = ROWS_DEV * W
    tile_cells = FMAX * tile
    per_peer = tile_cells // devices
    rep, me = lax.axis_index("rep"), lax.axis_index("seq")
    z, p = me // plane, me % plane
    even = p % 2 == 0
    ahead, behind = (me + 1) % devices, (me + devices - 1) % devices
    first, final = p == 0, p == plane - 1

    def signal(semaphore, device):
        pl.semaphore_signal(semaphore, inc=1, device_id=(rep, device), device_id_type=pl.DeviceIdType.MESH)

    loads = [
        pltpu.make_async_copy(source, target, load_sem.at[i])
        for i, (source, target) in enumerate((
            (layout_hbm, layout_ref), (assign_hbm, assign_ref), (latents_hbm, latents_ref), (cache_hbm, cache_ref), (features_hbm, features_ref),
        ))
    ]
    loads = loads + [
        pltpu.make_async_copy(weight_hbm.at[3 * i : 3 * i + 3], weight_ref.at[3 * i : 3 * i + 3], load_sem.at[5 + i])
        for i in range(9)
    ]
    for copy in loads:
        copy.start()

    barrier = pltpu.get_barrier_semaphore()
    for i in by_distance(planes):
        signal(barrier, ((z + i) % planes) * plane + (p // 2) * 2 + 1)
    for q in range(0, plane, 2):
        @pl.when(p != q)
        def _():
            signal(barrier, z * plane + q)

    @pl.when(final)
    def _():
        signal(barrier, ahead)

    @pl.when(first)
    def _():
        signal(barrier, (behind + devices - 1) % devices)

    row_of = lax.broadcasted_iota(i32, (tile_cells // 3, tile_cells // 3), 0)
    lane_of = lax.broadcasted_iota(i32, (tile_cells // 3, tile_cells // 3), 1)
    earlier = (row_of < lane_of).astype(bf16)
    loads[0].wait()
    loads[1].wait()
    own = layout_ref[pl.ds(me, 1), :]
    request = ((own // (ROWS_DEV * per_group * W)) * 43) // 128
    group = jnp.zeros_like(own)
    for g in range(REQS):
        group = group + jnp.where(assign_ref[g] == request, g, 0)
    place = group * per_group + (own // tile) % per_group
    target = (place + devices - per_group // 2) % devices
    line = (target % plane) * planes + target // plane
    hit = lax.broadcasted_iota(i32, (devices, tile_cells), 0) == line
    marks = hit.astype(f32)
    order = counted_before(marks, earlier)
    loads[2].wait()
    latents = latents_ref[...]
    rows = []
    for k in range(per_peer):
        chosen = jnp.where(order == k, marks, 0.0).astype(bf16)
        rows.append(lax.dot_general(latents, chosen, (((1,), (1,)), ((), ())), preferred_element_type=f32))
    rows.append(jnp.zeros((devices - per_peer * LAT_CH, devices), f32))
    sent = jnp.transpose(jnp.concatenate(rows, axis=0)).reshape(plane, planes, devices)
    for q in range(plane):
        send1_ref[q, 0] = (sent[q - 1] if q > 0 else pltpu.roll(sent[plane - 1], 1, 0)).astype(bf16)
        send1_ref[q, 1] = sent[q].astype(bf16)
        send1_ref[q, 2] = (sent[q + 1] if q < plane - 1 else pltpu.roll(sent[0], planes - 1, 0)).astype(bf16)

    @pl.when(even)
    def _():
        pl.semaphore_wait(barrier, plane - 1 + jnp.where(jnp.logical_or(first, p == plane - 2), 1, 0))
        signal(plane_ok, me + 1)

    @pl.when(jnp.logical_not(even))
    def _():
        pl.semaphore_wait(plane_ok, 1)

    near = []
    for i in range(1, plane):
        q = (p + i) % plane
        near.append(pltpu.make_async_remote_copy(
            src_ref=send1_ref.at[q], dst_ref=recv1_ref.at[p], send_sem=s1.at[i], recv_sem=r1.at[i],
            device_id=(rep, z * plane + q), device_id_type=pl.DeviceIdType.MESH))
        near[-1].start()
    recv1_ref[p] = send1_ref[p]

    loads[4].wait()
    sides = []
    for side in range(2):
        sides.append(pltpu.make_async_remote_copy(
            src_ref=features_ref.at[:, pl.ds((ROWS_DEV - 1) * W * (1 - side), W)],
            dst_ref=(above_ref, below_ref)[side],
            send_sem=sf.at[side], recv_sem=rf.at[side],
            device_id=(rep, (ahead, behind)[side]), device_id_type=pl.DeviceIdType.MESH))
        sides[-1].start()

    my_place = (me + per_group // 2) % devices
    my_group, position = my_place // per_group, my_place % per_group
    frame = ROWS_DEV * per_group * W
    half = tile // 2
    for side, table in enumerate((upper_table, table_ref, lower_table)):
        other = (my_place + side - 1 + devices) % devices
        start = assign_ref[other // per_group] * (FMAX * frame) + (other % per_group) * tile
        offset = layout_ref[...] - start
        inside = jnp.logical_and(jnp.logical_and(offset >= 0, offset < FMAX * frame), (offset & (frame - tile)) == 0)
        inner = offset & (tile - 1)
        if side == 0:
            within = jnp.where(inner >= half, (offset // frame) * half + inner - half, -1)
        elif side == 1:
            within = (offset // frame) * tile + inner
        else:
            within = jnp.where(inner < half, (offset // frame) * half + inner, -1)
        within = within.astype(f32)
        order = counted_before(inside.astype(f32), earlier)
        spot = lax.broadcasted_iota(i32, (devices, table.shape[1]), 1).astype(f32)
        for k in range(per_peer):
            chosen = jnp.logical_and(order == k, inside)
            home = jnp.sum(jnp.where(chosen, within, 0.0), axis=1, keepdims=True)
            table[k * devices : (k + 1) * devices, :] = (home == spot).astype(bf16)

    for copy in near:
        copy.wait()
    to = lax.broadcasted_iota(i32, (devices, devices), 0)
    source = lax.broadcasted_iota(i32, (devices, devices), 1)
    turn = (source == (to % plane) * planes + to // plane).astype(bf16)
    for side in range(3):
        turned = jnp.dot(turn, recv1_ref[:, side].reshape(devices, devices), preferred_element_type=f32)
        send2_ref[:, side] = turned.reshape(planes, plane, devices).astype(bf16)

    @pl.when(jnp.logical_not(even))
    def _():
        pl.semaphore_wait(barrier, 2 * (planes - 1))
        signal(far_ok, me - 1)

    @pl.when(even)
    def _():
        pl.semaphore_wait(far_ok, 1)

    far = []
    for i in by_distance(planes):
        q = (z + i) % planes
        far.append(pltpu.make_async_remote_copy(
            src_ref=send2_ref.at[q], dst_ref=recv2_ref.at[z], send_sem=s2.at[i], recv_sem=r2.at[i],
            device_id=(rep, q * plane + p), device_id_type=pl.DeviceIdType.MESH))
        far[-1].start()
    recv2_ref[z] = send2_ref[z]
    loads[3].wait()
    wide = cache_ref[...].astype(f32).reshape(2 * ROWS_DEV, W * LAT_CH)
    fold, member = spread_of_cells()
    stacked = jnp.concatenate([
        jnp.where(member, jnp.broadcast_to(wide[i : i + 1], member.shape), 0.0) for i in range(2 * ROWS_DEV)
    ], axis=0).astype(bf16)
    folded = jnp.dot(stacked, fold, preferred_element_type=f32)
    cached = jnp.concatenate([folded[i * LAT_CH : (i + 1) * LAT_CH] for i in range(2 * ROWS_DEV)], axis=1).astype(bf16)

    rim = 2 * W
    for f in range(2):
        rim_out_ref[0, f] = cached[:, (f + 1) * tile - rim : (f + 1) * tile]
        rim_out_ref[1, f] = cached[:, f * tile : f * tile + rim]
    edges = []
    for side in range(2):
        edges.append(pltpu.make_async_remote_copy(
            src_ref=rim_out_ref.at[side], dst_ref=rim_in_ref.at[side],
            send_sem=sh.at[side], recv_sem=rh.at[side],
            device_id=(rep, (ahead, behind)[side]), device_id_type=pl.DeviceIdType.MESH))
        edges[-1].start()

    for copy in loads[5:]:
        copy.wait()
    combine_taps(weight_ref, upper_ref, middle_ref, lower_ref)

    for copy in sides:
        copy.wait()
    for copy in edges:
        copy.wait_recv()
    outside = rows_outside(position, per_group - 1)
    for f in range(2):
        values = jnp.concatenate([above_ref[f], features_ref[f], below_ref[f]], axis=0).astype(f32)
        lay_out(small_ref, f, jnp.where(outside, 0.0, values))
    for px in range(2):
        add_products(part_ref, small_ref, upper_ref, middle_ref, lower_ref, px, 1, 0, 2, (1, 0), {})
        add_products(part_ref, small_ref, upper_ref, middle_ref, lower_ref, px, 0, 0, 1, (0,), {0})
    for copy in far:
        copy.wait()
    found = []
    for side, table in enumerate((upper_table, table_ref, lower_table)):
        arrived = jnp.transpose(recv2_ref[:, side].astype(f32).reshape(devices, devices))
        arrived = jnp.concatenate([arrived[k * LAT_CH : (k + 1) * LAT_CH] for k in range(per_peer)], axis=1)
        found.append(jnp.dot(arrived.astype(bf16), table[...], preferred_element_type=f32))
    nothing = jnp.zeros((LAT_CH, rim), f32)
    for f in range(2 + FMAX):
        if f < 2:
            top, here, bottom = rim_in_ref[0, f].astype(f32), cached[:, f * tile : (f + 1) * tile], rim_in_ref[1, f].astype(f32)
        else:
            t = f - 2
            top, bottom = (found[side][:, t * rim : (t + 1) * rim] for side in (0, 2))
            here = found[1][:, t * tile : (t + 1) * tile].astype(bf16)
        at = f * (tile + 2 * rim)
        window_ref[:, at : at + rim] = jnp.where(position == 0, nothing, top).astype(bf16)
        window_ref[:, at + rim : at + rim + tile] = here
        window_ref[:, at + rim + tile : at + 2 * rim + tile] = jnp.where(position == per_group - 1, nothing, bottom).astype(bf16)
    for copy in edges:
        copy.wait_send()


def gather(devices, assign, layout, latents, latent_cache, feature_cache, second_weight):
    plane = devices // REQS // 2
    planes = devices // plane
    cells = FMAX * ROWS_DEV * W
    vm, hbm = pl.BlockSpec(memory_space=pltpu.VMEM), pl.BlockSpec(memory_space=pltpu.HBM)
    bf16, dma = jnp.bfloat16, pltpu.SemaphoreType.DMA
    return pl.pallas_call(
        functools.partial(gather_kernel, devices),
        out_shape=(
            jax.ShapeDtypeStruct((LAT_CH, (2 + FMAX) * (ROWS_DEV + 4) * W), bf16),
            jax.ShapeDtypeStruct((2, 3, OUT_CH, 2 * MID_CH), bf16),
            jax.ShapeDtypeStruct((2, 3, 2 * OUT_CH, 2 * MID_CH), bf16),
            jax.ShapeDtypeStruct((2, 3, OUT_CH, 2 * MID_CH), bf16),
            jax.ShapeDtypeStruct((2, 2, 2, OUT_CH, ROWS_DEV * W), jnp.float32),
        ),
        in_specs=[hbm] * 6,
        out_specs=(vm, vm, vm, vm, vm),
        scratch_shapes=[
            pltpu.SMEM((REQS,), jnp.int32),
            pltpu.VMEM((devices, cells), jnp.int32),
            pltpu.VMEM((LAT_CH, cells), bf16),
            pltpu.VMEM((2, ROWS_DEV, W * LAT_CH), bf16),
            pltpu.VMEM((2, ROWS_DEV * W, MID_CH), bf16),
            pltpu.VMEM((27, OUT_CH, MID_CH), bf16),
            pltpu.VMEM((2, W, MID_CH), bf16),
            pltpu.VMEM((2, W, MID_CH), bf16),
            pltpu.VMEM((2, 2, (ROWS_DEV + 2) * W, 2 * MID_CH), bf16),
            dma((14,)),
            pltpu.VMEM((plane, 3, planes, devices), bf16),
            pltpu.VMEM((plane, 3, planes, devices), bf16),
            pltpu.VMEM((planes, 3, plane, devices), bf16),
            pltpu.VMEM((planes, 3, plane, devices), bf16),
            pltpu.VMEM((cells, cells // 2), bf16),
            pltpu.VMEM((cells, cells), bf16),
            pltpu.VMEM((cells, cells // 2), bf16),
            pltpu.VMEM((2, 2, LAT_CH, 2 * W), bf16),
            pltpu.VMEM((2, 2, LAT_CH, 2 * W), bf16),
            pltpu.SemaphoreType.REGULAR,
            pltpu.SemaphoreType.REGULAR,
            dma((plane,)), dma((plane,)), dma((planes,)), dma((planes,)),
            dma((2,)), dma((2,)), dma((2,)), dma((2,)),
        ],
        compiler_params=pltpu.CompilerParams(collective_id=0, has_side_effects=True, vmem_limit_bytes=28 * 1024 * 1024),
        cost_estimate=pl.CostEstimate(flops=3_000_000_000, bytes_accessed=13_000_000, transcendentals=0),
    )(
        *(pltpu.with_memory_space_constraint(x, pltpu.HBM) for x in (
            assign,
            layout,
            latents,
            latent_cache,
            feature_cache.reshape(2, ROWS_DEV * W, MID_CH),
            jnp.swapaxes(second_weight, 3, 4).reshape(27, OUT_CH, MID_CH),
        )),
    )


def decode_kernel(
    per_group, place_axis, assign_hbm, counts_hbm, window_ref, w1_ref, b1_ref, gain_ref, fc_ref, upper_ref, middle_ref, lower_ref,
    part_ref, b2_ref,
    out_hbm, ln_hbm, fn_hbm,
    assign_ref, counts_ref, sums_ref, xs_ref, pre_ref, h_ref, frames_ref, ln_ref,
    load_sem, out_sem, last_sem, keep_sem,
):
    f32, bf16 = jnp.float32, jnp.bfloat16
    place = (lax.axis_index(place_axis) + per_group // 2) % (per_group * REQS)
    position = place % per_group
    small = [
        pltpu.make_async_copy(source, target, load_sem.at[i])
        for i, (source, target) in enumerate(((assign_hbm, assign_ref), (counts_hbm, counts_ref)))
    ]
    for copy in small:
        copy.start()
    rows = ROWS_DEV + 2
    cells, tile = rows * W, ROWS_DEV * W
    per_frame = (ROWS_DEV + 4) * W
    xt = window_ref[...].astype(f32)
    lanes = xt.shape[1]
    column = lax.broadcasted_iota(jnp.int32, xt.shape, 1) % W
    shifted = (
        jnp.where(column == 0, 0.0, pltpu.roll(xt, 1, 1)),
        xt,
        jnp.where(column == W - 1, 0.0, pltpu.roll(xt, lanes - 1, 1)),
    )
    evens = [one.astype(bf16) for one in shifted]
    odds = [pltpu.roll(one, lanes - W, 1).astype(bf16) for one in shifted]

    def patches(t):
        for e in range(3):
            for b in range(3):
                source, start = ((evens[e], 0), (odds[e], 0), (evens[e], 2 * W))[b]
                for a in range(3):
                    k = ((a * 3 + b) * 3 + e) * LAT_CH
                    at = (t + a) * per_frame + start
                    xs_ref[k : k + LAT_CH, t * cells : (t + 1) * cells] = source[:, at : at + cells]

    bias = b1_ref[...].reshape(1, MID_CH)
    half_gain = 0.5 * gain_ref[...].reshape(1, MID_CH)
    row = lax.broadcasted_iota(jnp.int32, (W, MID_CH), 0)

    def linear(t):
        pre_ref[t] = lax.dot_general(
            xs_ref[:, t * cells : (t + 1) * cells], w1_ref[...], (((0,), (0,)), ((), ())), preferred_element_type=f32
        )

    def activate(t, y):
        pre = pre_ref[t, y * W : (y + 1) * W, :] + bias
        inverse = lax.rsqrt(jnp.mean(pre * pre, axis=1, keepdims=True) + 1e-06)
        half = pre * inverse * half_gain
        values = half + half * jnp.tanh(half)
        if y == 0:
            values = jnp.where(position == 0, 0.0, values)
        if y == rows - 1:
            values = jnp.where(position == per_group - 1, 0.0, values)
        at = slice(y * W, (y + 1) * W)
        here = values.astype(bf16)
        h_ref[0, t, at, 0:MID_CH] = jnp.where(row == 0, 0.0, pltpu.roll(values, 1, 0)).astype(bf16)
        h_ref[0, t, at, MID_CH : 2 * MID_CH] = here
        h_ref[1, t, at, 0:MID_CH] = here
        h_ref[1, t, at, MID_CH : 2 * MID_CH] = jnp.where(row == W - 1, 0.0, pltpu.roll(values, W - 1, 0)).astype(bf16)

    for t in range(FMAX):
        patches(t)
        linear(t)
    for copy in small:
        copy.wait()
    live = counts_ref[assign_ref[place // per_group]]
    fold, member = spread_of_cells()
    for j in range(2):
        latest = window_ref[:, pl.ds(pl.multiple_of((j + live) * per_frame + 2 * W, 2 * W), tile)].astype(f32)
        latest = jnp.concatenate([latest[:, y * W : (y + 1) * W] for y in range(ROWS_DEV)], axis=0).astype(bf16)
        wide = lax.dot_general(latest, fold, (((1,), (1,)), ((), ())), preferred_element_type=f32)
        wide = jnp.where(member[None], wide.reshape(ROWS_DEV, LAT_CH, W * LAT_CH), 0.0)
        ln_ref[j] = jnp.sum(wide, axis=1).astype(bf16)
    kept = [pltpu.make_async_copy(ln_ref, ln_hbm, keep_sem.at[0])]
    kept[0].start()
    for y in range(rows):
        activate(0, y)
    block = tile
    source = lax.broadcasted_iota(jnp.int32, (block, block), 0)
    target = lax.broadcasted_iota(jnp.int32, (block, block), 1)
    parity, line, cell = source // (2 * W), source // W % 2, source % W
    weave = (target == line * 2 * W + cell * 2 + parity).astype(bf16)
    bias2 = jnp.transpose(jnp.broadcast_to(b2_ref[...].reshape(1, OUT_CH), (8, OUT_CH)))[:, 0:1]
    started = set()
    done = []
    def finish(t, py):
        ready = []
        for px in range(2):
            total = sums_ref[t, px, py] + (part_ref[t, px, py] if t < 2 else 0.0) + bias2
            ready.append(jnp.where(t < live, total, 0.0).astype(bf16))
        for pair in range(ROWS_DEV // 2):
            part = slice(pair * 2 * W, (pair + 1) * 2 * W)
            joined = jnp.concatenate([ready[0][:, part], ready[1][:, part]], axis=1)
            woven = jnp.dot(joined, weave, preferred_element_type=f32).astype(bf16)
            for line in range(2):
                at = 2 * (2 * pair + line) + py
                frames_ref[t, at] = woven[:, line * 2 * W : (line + 1) * 2 * W]
                if t == FMAX - 1:
                    done.append(pltpu.make_async_copy(frames_ref.at[t, at], out_hbm.at[t, at], last_sem.at[at]))
                    done[-1].start()

    own = slice(W, W + tile)
    for frame in range(FMAX):
        times = tuple(range(2, frame - 1, -1))
        for r in range(3):
            for px in range(2):
                add_products(sums_ref, h_ref, upper_ref, middle_ref, lower_ref, px, frame, frame, 3 - frame, times, started, (r,))
                if frame + 1 < FMAX:
                    activate(frame + 1, r * 2 + px)
            if r > 0:
                finish(frame, r - 1)
        started = {0, 1, 2}
        t = frame
        if t < FMAX - 1:
            done.append(pltpu.make_async_copy(frames_ref.at[t], out_hbm.at[t], out_sem.at[t]))
            done[-1].start()
        if frame == FMAX - 2:
            @pl.when(live == 1)
            def _():
                pltpu.make_async_copy(fc_ref.at[1], fn_hbm.at[0], keep_sem.at[1]).start()

            @pl.when(live > 1)
            def _():
                pltpu.make_async_copy(h_ref.at[1, jnp.maximum(live - 2, 0), own, 0:MID_CH], fn_hbm.at[0], keep_sem.at[1]).start()

            kept.append(pltpu.make_async_copy(fc_ref.at[1], fn_hbm.at[0], keep_sem.at[1]))
            kept.append(pltpu.make_async_copy(h_ref.at[1, live - 1, own, 0:MID_CH], fn_hbm.at[1], keep_sem.at[2]))
            kept[-1].start()
    for copy in kept:
        copy.wait()
    for copy in done:
        copy.wait()


def decode(devices, assign, counts, gathered, first_weight, first_bias, norm_gain, feature_cache, second_bias):
    per_group = devices // REQS
    cells = (ROWS_DEV + 2) * W
    vm, hbm = pl.BlockSpec(memory_space=pltpu.VMEM), pl.BlockSpec(memory_space=pltpu.HBM)
    f32, bf16 = jnp.float32, jnp.bfloat16
    frames, latents, features = pl.pallas_call(
        functools.partial(decode_kernel, per_group, "seq"),
        out_shape=(
            jax.ShapeDtypeStruct((FMAX, 2 * ROWS_DEV, OUT_CH, 2 * W), bf16),
            jax.ShapeDtypeStruct((2, ROWS_DEV, W * LAT_CH), bf16),
            jax.ShapeDtypeStruct((2, ROWS_DEV * W, MID_CH), bf16),
        ),
        in_specs=[hbm, hbm] + [vm] * 10,
        out_specs=(hbm, hbm, hbm),
        scratch_shapes=[
            pltpu.SMEM((REQS,), jnp.int32),
            pltpu.SMEM((REQS,), jnp.int32),
            pltpu.VMEM((FMAX, 2, 2, OUT_CH, ROWS_DEV * W), f32),
            pltpu.VMEM((27 * LAT_CH, FMAX * cells), bf16),
            pltpu.VMEM((FMAX, cells, MID_CH), f32),
            pltpu.VMEM((2, FMAX, cells, 2 * MID_CH), bf16),
            pltpu.VMEM((FMAX, 2 * ROWS_DEV, OUT_CH, 2 * W), bf16),
            pltpu.VMEM((2, ROWS_DEV, W * LAT_CH), bf16),
            pltpu.SemaphoreType.DMA((2,)),
            pltpu.SemaphoreType.DMA((FMAX,)),
            pltpu.SemaphoreType.DMA((2 * ROWS_DEV,)),
            pltpu.SemaphoreType.DMA((3,)),
        ],
        compiler_params=pltpu.CompilerParams(vmem_limit_bytes=28 * 1024 * 1024),
        cost_estimate=pl.CostEstimate(flops=4_500_000_000, bytes_accessed=11_000_000, transcendentals=442368),
    )(
        assign, counts, gathered[0], first_weight.reshape(27 * LAT_CH, MID_CH), first_bias, norm_gain,
        feature_cache.reshape(2, ROWS_DEV * W, MID_CH), *gathered[1:], second_bias,
    )
    return jnp.swapaxes(frames, 2, 3), latents, features.reshape(2, ROWS_DEV, W, MID_CH)


def body(
    latents,
    layout,
    assign,
    counts,
    latent_cache,
    feature_cache,
    first_weight,
    first_bias,
    norm_gain,
    second_weight,
    second_bias,
):
    devices = lax.axis_size("seq")
    gathered = gather(devices, assign, layout, latents, latent_cache, feature_cache, second_weight)
    return decode(devices, assign, counts, gathered, first_weight, first_bias, norm_gain, feature_cache, second_bias)


def solution(mesh):
    return jax.shard_map(
        body,
        mesh=mesh,
        in_specs=(
            P(None, ("rep", "seq")),
            P("rep", None),
            P("rep"),
            P("rep"),
            P(None, ("rep", "seq"), None),
            P(None, ("rep", "seq"), None, None),
            P(),
            P(),
            P(),
            P(),
            P(),
        ),
        out_specs=(
            P(None, ("rep", "seq"), None, None),
            P(None, ("rep", "seq"), None),
            P(None, ("rep", "seq"), None, None),
        ),
        check_vma=False,
    )
```

```python
import functools

import jax
import jax.numpy as jnp
from jax import lax
from jax.experimental import pallas as pl
from jax.experimental.pallas import tpu as pltpu
from jax.sharding import PartitionSpec as P

LAT_CH = 16
MID_CH = 384
OUT_CH = 192
REQS = 8
FMAX = 3
ROWS_DEV = 4
W = 64


def spread_of_cells():
    lane = lax.broadcasted_iota(jnp.int32, (W * LAT_CH, W), 0)
    cell = lax.broadcasted_iota(jnp.int32, (W * LAT_CH, W), 1)
    fold = (lane // LAT_CH == cell).astype(jnp.bfloat16)
    channel = lax.broadcasted_iota(jnp.int32, (LAT_CH, W * LAT_CH), 0)
    member = lax.broadcasted_iota(jnp.int32, (LAT_CH, W * LAT_CH), 1) % LAT_CH == channel
    return fold, member


def rows_outside(position, last):
    cells = (ROWS_DEV + 2) * W
    row = lax.broadcasted_iota(jnp.int32, (cells, MID_CH), 0)
    above = jnp.logical_and(row < W, position == 0)
    return jnp.logical_or(above, jnp.logical_and(row >= cells - W, position == last))


def lay_out(target, frame, values):
    cells = values.shape[0]
    column = lax.broadcasted_iota(jnp.int32, values.shape, 0) % W
    before = jnp.where(column == 0, 0.0, pltpu.roll(values, 1, 0)).astype(jnp.bfloat16)
    after = jnp.where(column == W - 1, 0.0, pltpu.roll(values, cells - 1, 0)).astype(jnp.bfloat16)
    here = values.astype(jnp.bfloat16)
    target[0, frame, :, 0:MID_CH] = before
    target[0, frame, :, MID_CH : 2 * MID_CH] = here
    target[1, frame, :, 0:MID_CH] = here
    target[1, frame, :, MID_CH : 2 * MID_CH] = after


def combine_taps(weight, upper, middle, lower):
    near = (((0,), (1, 2)), ((0, 1), (2,)))

    @pl.loop(0, 3)
    def _(a):
        base = a * 9
        tap = [[weight[base + b * 3 + e].astype(jnp.float32) for e in range(3)] for b in range(3)]
        for target, start, py, dy in ((upper, 0, 0, 0), (middle, 0, 0, 1), (middle, OUT_CH, 1, 0), (lower, 0, 1, 1)):
            taps = [sum(tap[b][e] for b in near[py][dy]) for e in range(3)]
            for px in range(2):
                for dx in range(2):
                    total = sum(taps[e] for e in near[px][dx]).astype(jnp.bfloat16)
                    target[px, a, start : start + OUT_CH, dx * MID_CH : (dx + 1) * MID_CH] = total


def add_products(sums, features, upper, middle, lower, px, frame, a, count, times, started, parts=(0, 1, 2)):
    block = ROWS_DEV * W
    for r in parts:
        weights = (middle, upper, lower)[r]
        row = (1, 0, 2)[r]
        right = features[px, frame, row * W : row * W + block, :]
        left = weights[px, a : a + count]
        height = left.shape[1]
        part = lax.dot_general(
            left.reshape(count * height, left.shape[2]), right, (((1,), (1,)), ((), ())), preferred_element_type=jnp.float32
        )
        for i, t in enumerate(times):
            for py in ((0, 1), (0,), (1,))[r]:
                at = i * height + (py * OUT_CH if r == 0 else 0)
                piece = part[at : at + OUT_CH]
                if r == 0 and t not in started:
                    sums[t, px, py] = piece
                else:
                    sums[t, px, py] = sums[t, px, py] + piece


def counted_before(marks, earlier):
    size = earlier.shape[0]
    carry = jnp.zeros((marks.shape[0], 1), jnp.float32)
    parts = []
    for start in range(0, marks.shape[1], size):
        block = marks[:, start : start + size]
        parts.append(jnp.dot(block.astype(jnp.bfloat16), earlier, preferred_element_type=jnp.float32) + carry)
        carry = carry + jnp.sum(block, axis=1, keepdims=True)
    return jnp.concatenate(parts, axis=1)


def by_distance(ring):
    return sorted(range(1, ring), key=lambda i: (-min(i, ring - i), i))


def gather_kernel(
    devices, assign_hbm, layout_hbm, latents_hbm, cache_hbm, features_hbm, weight_hbm,
    window_ref, upper_ref, middle_ref, lower_ref, part_ref,
    assign_ref, layout_ref, latents_ref, cache_ref, features_ref, weight_ref, above_ref, below_ref,
    small_ref, load_sem,
    send1_ref, recv1_ref, send2_ref, recv2_ref, upper_table, table_ref, lower_table, rim_out_ref, rim_in_ref,
    plane_ok, far_ok, s1, r1, s2, r2, sf, rf, sh, rh,
):
    f32, bf16, i32 = jnp.float32, jnp.bfloat16, jnp.int32
    per_group = devices // REQS
    plane = per_group // 2
    planes = devices // plane
    tile = ROWS_DEV * W
    tile_cells = FMAX * tile
    per_peer = tile_cells // devices
    rep, me = lax.axis_index("rep"), lax.axis_index("seq")
    z, p = me // plane, me % plane
    even = p % 2 == 0
    ahead, behind = (me + 1) % devices, (me + devices - 1) % devices
    first, final = p == 0, p == plane - 1

    def signal(semaphore, device):
        pl.semaphore_signal(semaphore, inc=1, device_id=(rep, device), device_id_type=pl.DeviceIdType.MESH)

    loads = [
        pltpu.make_async_copy(source, target, load_sem.at[i])
        for i, (source, target) in enumerate((
            (layout_hbm, layout_ref), (assign_hbm, assign_ref), (latents_hbm, latents_ref), (cache_hbm, cache_ref), (features_hbm, features_ref),
        ))
    ]
    loads = loads + [
        pltpu.make_async_copy(weight_hbm.at[3 * i : 3 * i + 3], weight_ref.at[3 * i : 3 * i + 3], load_sem.at[5 + i])
        for i in range(9)
    ]
    for copy in loads:
        copy.start()

    barrier = pltpu.get_barrier_semaphore()
    for i in by_distance(planes):
        signal(barrier, ((z + i) % planes) * plane + (p // 2) * 2 + 1)
    for q in range(0, plane, 2):
        @pl.when(p != q)
        def _():
            signal(barrier, z * plane + q)

    @pl.when(final)
    def _():
        signal(barrier, ahead)

    @pl.when(first)
    def _():
        signal(barrier, (behind + devices - 1) % devices)

    row_of = lax.broadcasted_iota(i32, (tile_cells // 3, tile_cells // 3), 0)
    lane_of = lax.broadcasted_iota(i32, (tile_cells // 3, tile_cells // 3), 1)
    earlier = (row_of < lane_of).astype(bf16)
    loads[0].wait()
    loads[1].wait()
    own = layout_ref[pl.ds(me, 1), :]
    request = ((own // (ROWS_DEV * per_group * W)) * 43) // 128
    group = jnp.zeros_like(own)
    for g in range(REQS):
        group = group + jnp.where(assign_ref[g] == request, g, 0)
    place = group * per_group + (own // tile) % per_group
    target = (place + devices - per_group // 2) % devices
    line = (target % plane) * planes + target // plane
    hit = lax.broadcasted_iota(i32, (devices, tile_cells), 0) == line
    marks = hit.astype(f32)
    order = counted_before(marks, earlier)
    loads[2].wait()
    latents = latents_ref[...]
    rows = []
    for k in range(per_peer):
        chosen = jnp.where(order == k, marks, 0.0).astype(bf16)
        rows.append(lax.dot_general(latents, chosen, (((1,), (1,)), ((), ())), preferred_element_type=f32))
    rows.append(jnp.zeros((devices - per_peer * LAT_CH, devices), f32))
    sent = jnp.transpose(jnp.concatenate(rows, axis=0)).reshape(plane, planes, devices)
    for q in range(plane):
        send1_ref[q, 0] = (sent[q - 1] if q > 0 else pltpu.roll(sent[plane - 1], 1, 0)).astype(bf16)
        send1_ref[q, 1] = sent[q].astype(bf16)
        send1_ref[q, 2] = (sent[q + 1] if q < plane - 1 else pltpu.roll(sent[0], planes - 1, 0)).astype(bf16)

    @pl.when(even)
    def _():
        pl.semaphore_wait(barrier, plane - 1 + jnp.where(jnp.logical_or(first, p == plane - 2), 1, 0))
        signal(plane_ok, me + 1)

    @pl.when(jnp.logical_not(even))
    def _():
        pl.semaphore_wait(plane_ok, 1)

    near = []
    for i in range(1, plane):
        q = (p + i) % plane
        near.append(pltpu.make_async_remote_copy(
            src_ref=send1_ref.at[q], dst_ref=recv1_ref.at[p], send_sem=s1.at[i], recv_sem=r1.at[i],
            device_id=(rep, z * plane + q), device_id_type=pl.DeviceIdType.MESH))
        near[-1].start()
    recv1_ref[p] = send1_ref[p]

    loads[4].wait()
    sides = []
    for side in range(2):
        sides.append(pltpu.make_async_remote_copy(
            src_ref=features_ref.at[:, pl.ds((ROWS_DEV - 1) * W * (1 - side), W)],
            dst_ref=(above_ref, below_ref)[side],
            send_sem=sf.at[side], recv_sem=rf.at[side],
            device_id=(rep, (ahead, behind)[side]), device_id_type=pl.DeviceIdType.MESH))
        sides[-1].start()

    my_place = (me + per_group // 2) % devices
    my_group, position = my_place // per_group, my_place % per_group
    frame = ROWS_DEV * per_group * W
    half = tile // 2
    for side, table in enumerate((upper_table, table_ref, lower_table)):
        other = (my_place + side - 1 + devices) % devices
        start = assign_ref[other // per_group] * (FMAX * frame) + (other % per_group) * tile
        offset = layout_ref[...] - start
        inside = jnp.logical_and(jnp.logical_and(offset >= 0, offset < FMAX * frame), (offset & (frame - tile)) == 0)
        inner = offset & (tile - 1)
        if side == 0:
            within = jnp.where(inner >= half, (offset // frame) * half + inner - half, -1)
        elif side == 1:
            within = (offset // frame) * tile + inner
        else:
            within = jnp.where(inner < half, (offset // frame) * half + inner, -1)
        within = within.astype(f32)
        order = counted_before(inside.astype(f32), earlier)
        spot = lax.broadcasted_iota(i32, (devices, table.shape[1]), 1).astype(f32)
        for k in range(per_peer):
            chosen = jnp.logical_and(order == k, inside)
            home = jnp.sum(jnp.where(chosen, within, 0.0), axis=1, keepdims=True)
            table[k * devices : (k + 1) * devices, :] = (home == spot).astype(bf16)

    for copy in near:
        copy.wait()
    to = lax.broadcasted_iota(i32, (devices, devices), 0)
    source = lax.broadcasted_iota(i32, (devices, devices), 1)
    turn = (source == (to % plane) * planes + to // plane).astype(bf16)
    for side in range(3):
        turned = jnp.dot(turn, recv1_ref[:, side].reshape(devices, devices), preferred_element_type=f32)
        send2_ref[:, side] = turned.reshape(planes, plane, devices).astype(bf16)

    @pl.when(jnp.logical_not(even))
    def _():
        pl.semaphore_wait(barrier, 2 * (planes - 1))
        signal(far_ok, me - 1)

    @pl.when(even)
    def _():
        pl.semaphore_wait(far_ok, 1)

    far = []
    for i in by_distance(planes):
        q = (z + i) % planes
        far.append(pltpu.make_async_remote_copy(
            src_ref=send2_ref.at[q], dst_ref=recv2_ref.at[z], send_sem=s2.at[i], recv_sem=r2.at[i],
            device_id=(rep, q * plane + p), device_id_type=pl.DeviceIdType.MESH))
        far[-1].start()
    recv2_ref[z] = send2_ref[z]
    loads[3].wait()
    wide = cache_ref[...].astype(f32).reshape(2 * ROWS_DEV, W * LAT_CH)
    fold, member = spread_of_cells()
    stacked = jnp.concatenate([
        jnp.where(member, jnp.broadcast_to(wide[i : i + 1], member.shape), 0.0) for i in range(2 * ROWS_DEV)
    ], axis=0).astype(bf16)
    folded = jnp.dot(stacked, fold, preferred_element_type=f32)
    cached = jnp.concatenate([folded[i * LAT_CH : (i + 1) * LAT_CH] for i in range(2 * ROWS_DEV)], axis=1).astype(bf16)

    rim = 2 * W
    for f in range(2):
        rim_out_ref[0, f] = cached[:, (f + 1) * tile - rim : (f + 1) * tile]
        rim_out_ref[1, f] = cached[:, f * tile : f * tile + rim]
    edges = []
    for side in range(2):
        edges.append(pltpu.make_async_remote_copy(
            src_ref=rim_out_ref.at[side], dst_ref=rim_in_ref.at[side],
            send_sem=sh.at[side], recv_sem=rh.at[side],
            device_id=(rep, (ahead, behind)[side]), device_id_type=pl.DeviceIdType.MESH))
        edges[-1].start()

    for copy in loads[5:]:
        copy.wait()
    combine_taps(weight_ref, upper_ref, middle_ref, lower_ref)

    for copy in sides:
        copy.wait()
    for copy in edges:
        copy.wait_recv()
    outside = rows_outside(position, per_group - 1)
    for f in range(2):
        values = jnp.concatenate([above_ref[f], features_ref[f], below_ref[f]], axis=0).astype(f32)
        lay_out(small_ref, f, jnp.where(outside, 0.0, values))
    for px in range(2):
        add_products(part_ref, small_ref, upper_ref, middle_ref, lower_ref, px, 1, 0, 2, (1, 0), {})
        add_products(part_ref, small_ref, upper_ref, middle_ref, lower_ref, px, 0, 0, 1, (0,), {0})
    for copy in far:
        copy.wait()
    found = []
    for side, table in enumerate((upper_table, table_ref, lower_table)):
        arrived = jnp.transpose(recv2_ref[:, side].astype(f32).reshape(devices, devices))
        arrived = jnp.concatenate([arrived[k * LAT_CH : (k + 1) * LAT_CH] for k in range(per_peer)], axis=1)
        found.append(jnp.dot(arrived.astype(bf16), table[...], preferred_element_type=f32))
    nothing = jnp.zeros((LAT_CH, rim), f32)
    for f in range(2 + FMAX):
        if f < 2:
            top, here, bottom = rim_in_ref[0, f].astype(f32), cached[:, f * tile : (f + 1) * tile], rim_in_ref[1, f].astype(f32)
        else:
            t = f - 2
            top, bottom = (found[side][:, t * rim : (t + 1) * rim] for side in (0, 2))
            here = found[1][:, t * tile : (t + 1) * tile].astype(bf16)
        at = f * (tile + 2 * rim)
        window_ref[:, at : at + rim] = jnp.where(position == 0, nothing, top).astype(bf16)
        window_ref[:, at + rim : at + rim + tile] = here
        window_ref[:, at + rim + tile : at + 2 * rim + tile] = jnp.where(position == per_group - 1, nothing, bottom).astype(bf16)
    for copy in edges:
        copy.wait_send()


def gather(devices, assign, layout, latents, latent_cache, feature_cache, second_weight):
    plane = devices // REQS // 2
    planes = devices // plane
    cells = FMAX * ROWS_DEV * W
    vm, hbm = pl.BlockSpec(memory_space=pltpu.VMEM), pl.BlockSpec(memory_space=pltpu.HBM)
    bf16, dma = jnp.bfloat16, pltpu.SemaphoreType.DMA
    return pl.pallas_call(
        functools.partial(gather_kernel, devices),
        out_shape=(
            jax.ShapeDtypeStruct((LAT_CH, (2 + FMAX) * (ROWS_DEV + 4) * W), bf16),
            jax.ShapeDtypeStruct((2, 3, OUT_CH, 2 * MID_CH), bf16),
            jax.ShapeDtypeStruct((2, 3, 2 * OUT_CH, 2 * MID_CH), bf16),
            jax.ShapeDtypeStruct((2, 3, OUT_CH, 2 * MID_CH), bf16),
            jax.ShapeDtypeStruct((2, 2, 2, OUT_CH, ROWS_DEV * W), jnp.float32),
        ),
        in_specs=[hbm] * 6,
        out_specs=(vm, vm, vm, vm, vm),
        scratch_shapes=[
            pltpu.SMEM((REQS,), jnp.int32),
            pltpu.VMEM((devices, cells), jnp.int32),
            pltpu.VMEM((LAT_CH, cells), bf16),
            pltpu.VMEM((2, ROWS_DEV, W * LAT_CH), bf16),
            pltpu.VMEM((2, ROWS_DEV * W, MID_CH), bf16),
            pltpu.VMEM((27, OUT_CH, MID_CH), bf16),
            pltpu.VMEM((2, W, MID_CH), bf16),
            pltpu.VMEM((2, W, MID_CH), bf16),
            pltpu.VMEM((2, 2, (ROWS_DEV + 2) * W, 2 * MID_CH), bf16),
            dma((14,)),
            pltpu.VMEM((plane, 3, planes, devices), bf16),
            pltpu.VMEM((plane, 3, planes, devices), bf16),
            pltpu.VMEM((planes, 3, plane, devices), bf16),
            pltpu.VMEM((planes, 3, plane, devices), bf16),
            pltpu.VMEM((cells, cells // 2), bf16),
            pltpu.VMEM((cells, cells), bf16),
            pltpu.VMEM((cells, cells // 2), bf16),
            pltpu.VMEM((2, 2, LAT_CH, 2 * W), bf16),
            pltpu.VMEM((2, 2, LAT_CH, 2 * W), bf16),
            pltpu.SemaphoreType.REGULAR,
            pltpu.SemaphoreType.REGULAR,
            dma((plane,)), dma((plane,)), dma((planes,)), dma((planes,)),
            dma((2,)), dma((2,)), dma((2,)), dma((2,)),
        ],
        compiler_params=pltpu.CompilerParams(collective_id=0, has_side_effects=True, vmem_limit_bytes=28 * 1024 * 1024),
        cost_estimate=pl.CostEstimate(flops=3_000_000_000, bytes_accessed=13_000_000, transcendentals=0),
    )(
        *(pltpu.with_memory_space_constraint(x, pltpu.HBM) for x in (
            assign,
            layout,
            latents,
            latent_cache,
            feature_cache.reshape(2, ROWS_DEV * W, MID_CH),
            jnp.swapaxes(second_weight, 3, 4).reshape(27, OUT_CH, MID_CH),
        )),
    )


def decode_kernel(
    per_group, place_axis, assign_hbm, counts_hbm, window_ref, w1_ref, b1_ref, gain_ref, fc_ref, upper_ref, middle_ref, lower_ref,
    part_ref, b2_ref,
    out_hbm, ln_hbm, fn_hbm,
    assign_ref, counts_ref, sums_ref, xs_ref, pre_ref, h_ref, frames_ref, ln_ref,
    load_sem, out_sem, last_sem, keep_sem,
):
    f32, bf16 = jnp.float32, jnp.bfloat16
    place = (lax.axis_index(place_axis) + per_group // 2) % (per_group * REQS)
    position = place % per_group
    small = [
        pltpu.make_async_copy(source, target, load_sem.at[i])
        for i, (source, target) in enumerate(((assign_hbm, assign_ref), (counts_hbm, counts_ref)))
    ]
    for copy in small:
        copy.start()
    rows = ROWS_DEV + 2
    cells, tile = rows * W, ROWS_DEV * W
    per_frame = (ROWS_DEV + 4) * W
    xt = window_ref[...].astype(f32)
    lanes = xt.shape[1]
    column = lax.broadcasted_iota(jnp.int32, xt.shape, 1) % W
    shifted = (
        jnp.where(column == 0, 0.0, pltpu.roll(xt, 1, 1)),
        xt,
        jnp.where(column == W - 1, 0.0, pltpu.roll(xt, lanes - 1, 1)),
    )
    evens = [one.astype(bf16) for one in shifted]
    odds = [pltpu.roll(one, lanes - W, 1).astype(bf16) for one in shifted]

    def patches(t):
        for e in range(3):
            for b in range(3):
                source, start = ((evens[e], 0), (odds[e], 0), (evens[e], 2 * W))[b]
                for a in range(3):
                    k = ((a * 3 + b) * 3 + e) * LAT_CH
                    at = (t + a) * per_frame + start
                    xs_ref[k : k + LAT_CH, t * cells : (t + 1) * cells] = source[:, at : at + cells]

    bias = b1_ref[...].reshape(1, MID_CH)
    gain = gain_ref[...].reshape(1, MID_CH)
    row = lax.broadcasted_iota(jnp.int32, (W, MID_CH), 0)

    def linear(t):
        pre_ref[t] = lax.dot_general(
            xs_ref[:, t * cells : (t + 1) * cells], w1_ref[...], (((0,), (0,)), ((), ())), preferred_element_type=f32
        )

    def activate(t, y):
        pre = pre_ref[t, y * W : (y + 1) * W, :] + bias
        inverse = lax.rsqrt(jnp.mean(pre * pre, axis=1, keepdims=True) + 1e-06)
        half = 0.5 * (pre * inverse * gain)
        values = half + half * jnp.tanh(half)
        if y == 0:
            values = jnp.where(position == 0, 0.0, values)
        if y == rows - 1:
            values = jnp.where(position == per_group - 1, 0.0, values)
        at = slice(y * W, (y + 1) * W)
        here = values.astype(bf16)
        h_ref[0, t, at, 0:MID_CH] = jnp.where(row == 0, 0.0, pltpu.roll(values, 1, 0)).astype(bf16)
        h_ref[0, t, at, MID_CH : 2 * MID_CH] = here
        h_ref[1, t, at, 0:MID_CH] = here
        h_ref[1, t, at, MID_CH : 2 * MID_CH] = jnp.where(row == W - 1, 0.0, pltpu.roll(values, W - 1, 0)).astype(bf16)

    for t in range(FMAX):
        patches(t)
        linear(t)
    for copy in small:
        copy.wait()
    live = counts_ref[assign_ref[place // per_group]]
    fold, member = spread_of_cells()
    for j in range(2):
        latest = window_ref[:, pl.ds(pl.multiple_of((j + live) * per_frame + 2 * W, 2 * W), tile)].astype(f32)
        latest = jnp.concatenate([latest[:, y * W : (y + 1) * W] for y in range(ROWS_DEV)], axis=0).astype(bf16)
        wide = lax.dot_general(latest, fold, (((1,), (1,)), ((), ())), preferred_element_type=f32)
        wide = jnp.where(member[None], wide.reshape(ROWS_DEV, LAT_CH, W * LAT_CH), 0.0)
        ln_ref[j] = jnp.sum(wide, axis=1).astype(bf16)
    kept = [pltpu.make_async_copy(ln_ref, ln_hbm, keep_sem.at[0])]
    kept[0].start()
    for y in range(rows):
        activate(0, y)
    block = tile
    source = lax.broadcasted_iota(jnp.int32, (block, block), 0)
    target = lax.broadcasted_iota(jnp.int32, (block, block), 1)
    parity, line, cell = source // (2 * W), source // W % 2, source % W
    weave = (target == line * 2 * W + cell * 2 + parity).astype(bf16)
    bias2 = jnp.transpose(jnp.broadcast_to(b2_ref[...].reshape(1, OUT_CH), (8, OUT_CH)))[:, 0:1]
    started = set()
    done = []
    own = slice(W, W + tile)
    for frame in range(FMAX):
        times = tuple(range(2, frame - 1, -1))
        for px in range(2):
            for r in range(3):
                add_products(sums_ref, h_ref, upper_ref, middle_ref, lower_ref, px, frame, frame, 3 - frame, times, started, (r,))
                if frame + 1 < FMAX:
                    activate(frame + 1, px * 3 + r)
        started = {0, 1, 2}
        t = frame
        for py in range(2):
            ready = []
            for px in range(2):
                total = sums_ref[t, px, py] + (part_ref[t, px, py] if t < 2 else 0.0) + bias2
                ready.append(jnp.where(t < live, total, 0.0).astype(bf16))
            for pair in range(ROWS_DEV // 2):
                part = slice(pair * 2 * W, (pair + 1) * 2 * W)
                joined = jnp.concatenate([ready[0][:, part], ready[1][:, part]], axis=1)
                woven = jnp.dot(joined, weave, preferred_element_type=f32).astype(bf16)
                for line in range(2):
                    at = 2 * (2 * pair + line) + py
                    frames_ref[t, at] = woven[:, line * 2 * W : (line + 1) * 2 * W]
                    if t == FMAX - 1:
                        done.append(pltpu.make_async_copy(frames_ref.at[t, at], out_hbm.at[t, at], last_sem.at[at]))
                        done[-1].start()
        if t < FMAX - 1:
            done.append(pltpu.make_async_copy(frames_ref.at[t], out_hbm.at[t], out_sem.at[t]))
            done[-1].start()
        if frame == FMAX - 2:
            @pl.when(live == 1)
            def _():
                pltpu.make_async_copy(fc_ref.at[1], fn_hbm.at[0], keep_sem.at[1]).start()

            @pl.when(live > 1)
            def _():
                pltpu.make_async_copy(h_ref.at[1, jnp.maximum(live - 2, 0), own, 0:MID_CH], fn_hbm.at[0], keep_sem.at[1]).start()

            kept.append(pltpu.make_async_copy(fc_ref.at[1], fn_hbm.at[0], keep_sem.at[1]))
            kept.append(pltpu.make_async_copy(h_ref.at[1, live - 1, own, 0:MID_CH], fn_hbm.at[1], keep_sem.at[2]))
            kept[-1].start()
    for copy in kept:
        copy.wait()
    for copy in done:
        copy.wait()


def decode(devices, assign, counts, gathered, first_weight, first_bias, norm_gain, feature_cache, second_bias):
    per_group = devices // REQS
    cells = (ROWS_DEV + 2) * W
    vm, hbm = pl.BlockSpec(memory_space=pltpu.VMEM), pl.BlockSpec(memory_space=pltpu.HBM)
    f32, bf16 = jnp.float32, jnp.bfloat16
    frames, latents, features = pl.pallas_call(
        functools.partial(decode_kernel, per_group, "seq"),
        out_shape=(
            jax.ShapeDtypeStruct((FMAX, 2 * ROWS_DEV, OUT_CH, 2 * W), bf16),
            jax.ShapeDtypeStruct((2, ROWS_DEV, W * LAT_CH), bf16),
            jax.ShapeDtypeStruct((2, ROWS_DEV * W, MID_CH), bf16),
        ),
        in_specs=[hbm, hbm] + [vm] * 10,
        out_specs=(hbm, hbm, hbm),
        scratch_shapes=[
            pltpu.SMEM((REQS,), jnp.int32),
            pltpu.SMEM((REQS,), jnp.int32),
            pltpu.VMEM((FMAX, 2, 2, OUT_CH, ROWS_DEV * W), f32),
            pltpu.VMEM((27 * LAT_CH, FMAX * cells), bf16),
            pltpu.VMEM((FMAX, cells, MID_CH), f32),
            pltpu.VMEM((2, FMAX, cells, 2 * MID_CH), bf16),
            pltpu.VMEM((FMAX, 2 * ROWS_DEV, OUT_CH, 2 * W), bf16),
            pltpu.VMEM((2, ROWS_DEV, W * LAT_CH), bf16),
            pltpu.SemaphoreType.DMA((2,)),
            pltpu.SemaphoreType.DMA((FMAX,)),
            pltpu.SemaphoreType.DMA((2 * ROWS_DEV,)),
            pltpu.SemaphoreType.DMA((3,)),
        ],
        compiler_params=pltpu.CompilerParams(vmem_limit_bytes=28 * 1024 * 1024),
        cost_estimate=pl.CostEstimate(flops=4_500_000_000, bytes_accessed=11_000_000, transcendentals=442368),
    )(
        assign, counts, gathered[0], first_weight.reshape(27 * LAT_CH, MID_CH), first_bias, norm_gain,
        feature_cache.reshape(2, ROWS_DEV * W, MID_CH), *gathered[1:], second_bias,
    )
    return jnp.swapaxes(frames, 2, 3), latents, features.reshape(2, ROWS_DEV, W, MID_CH)


def body(
    latents,
    layout,
    assign,
    counts,
    latent_cache,
    feature_cache,
    first_weight,
    first_bias,
    norm_gain,
    second_weight,
    second_bias,
):
    devices = lax.axis_size("seq")
    gathered = gather(devices, assign, layout, latents, latent_cache, feature_cache, second_weight)
    return decode(devices, assign, counts, gathered, first_weight, first_bias, norm_gain, feature_cache, second_bias)


def solution(mesh):
    return jax.shard_map(
        body,
        mesh=mesh,
        in_specs=(
            P(None, ("rep", "seq")),
            P("rep", None),
            P("rep"),
            P("rep"),
            P(None, ("rep", "seq"), None),
            P(None, ("rep", "seq"), None, None),
            P(),
            P(),
            P(),
            P(),
            P(),
        ),
        out_specs=(
            P(None, ("rep", "seq"), None, None),
            P(None, ("rep", "seq"), None),
            P(None, ("rep", "seq"), None, None),
        ),
        check_vma=False,
    )
```
